16 devices in a mesh: model: 2 (over z), data: 8 (over y, x, core).
Axes of the slice: x: 2, y: 2, z: 2, core: 2. Of those that a mesh axis runs over, the one named last changes fastest.
Arguments:
- local_grads: bfloat16 [8, 12, 2359296], P('data', None, 'model')
- master: float32 [12, 2359296], P(None, ('model', 'data'))
- moment_one: float32 [12, 2359296], P(None, ('model', 'data'))
- moment_two: float32 [12, 2359296], P(None, ('model', 'data'))
Outputs:
- output 1: bfloat16 [12, 2359296], P(None, 'model')
- output 2: float32 [12, 2359296], P(None, ('model', 'data'))
- output 3: float32 [12, 2359296], P(None, ('model', 'data'))
- output 4: float32 [12, 2359296], P(None, ('model', 'data'))
All inputs are finite; a program needn't handle non-finite values.
Results may differ from the reference program's by a relative error of at most 0.001.
Values are sent between devices in bfloat16 or wider.
A program may use at most 1 GiB of HBM per device.

```python
import jax
import jax.numpy as jnp
from jax import lax

D = 1536
LAYERS = 1
DATA = 8
STEP = 4
BLOCKS = 12 * LAYERS
BLOCK_SIZE = D * D
LEARN_RATE = 0.08
BETA_ONE = 0.9
BETA_TWO = 0.999
EPSILON = 1e-6
WEIGHT_DECAY = 0.01
MAX_NORM = 1.0
CORR_ONE = 1.0 - BETA_ONE ** STEP
CORR_TWO = 1.0 - BETA_TWO ** STEP


def tensor_sums(block_values):
    return jnp.stack([block_values[..., 0:3].sum(axis=-1), block_values[..., 3], block_values[..., 4:8].sum(axis=-1), block_values[..., 8:12].sum(axis=-1)], axis=-1)


def spread_tensors(tensor_values):
    lead_shape = tensor_values.shape[:-1]
    pieces = [jnp.broadcast_to(tensor_values[..., tensor_pos:tensor_pos + 1], lead_shape + (block_count,)) for tensor_pos, block_count in enumerate((3, 1, 4, 4))]
    return jnp.concatenate(pieces, axis=-1)


def setup_inputs(seed: int = 0) -> dict:
    key_list = jax.random.split(jax.random.key(seed), 8)
    fan_scale = jnp.concatenate([jnp.full((8,), D ** -0.5, jnp.float32), jnp.full((4,), (4 * D) ** -0.5, jnp.float32)])
    weight_factor = jnp.exp(jax.random.uniform(key_list[0], (LAYERS, 4), jnp.float32, minval=-0.8, maxval=0.8))
    weight_scale = (spread_tensors(weight_factor) * fan_scale).reshape(BLOCKS, 1)
    weight_slope = spread_tensors(jax.random.uniform(key_list[1], (LAYERS, 4), jnp.float32, minval=1.5, maxval=2.5)).reshape(BLOCKS, 1)
    position = jnp.arange(BLOCK_SIZE, dtype=jnp.float32) / BLOCK_SIZE - 0.5
    grad_factor = spread_tensors(jnp.exp(jax.random.uniform(key_list[2], (LAYERS, 4), jnp.float32, minval=-1.0, maxval=1.0))).reshape(BLOCKS, 1)
    grad_sigma = grad_factor * (3.0 * MAX_NORM) / jnp.sqrt(BLOCK_SIZE * jnp.sum(grad_factor * grad_factor))
    unit_scale = grad_sigma / jnp.sqrt(2.0)
    shared = jax.random.normal(key_list[3], (BLOCKS, BLOCK_SIZE), jnp.float32)

    def one_replica(replica):
        replica_noise = jax.random.normal(jax.random.fold_in(key_list[4], replica), (BLOCKS, BLOCK_SIZE), jnp.float32)
        return (unit_scale * (shared + DATA ** 0.5 * replica_noise)).astype(jnp.bfloat16)

    local_grads = lax.map(one_replica, jnp.arange(DATA))
    step_sigma = grad_sigma / 3.0
    master = weight_scale * jnp.exp(weight_slope * position) * jax.random.normal(key_list[5], (BLOCKS, BLOCK_SIZE), jnp.float32)
    moment_one = 0.1 * step_sigma * jax.random.normal(key_list[6], (BLOCKS, BLOCK_SIZE), jnp.float32)
    moment_two = 0.003 * step_sigma * step_sigma * jax.random.uniform(key_list[7], (BLOCKS, BLOCK_SIZE), jnp.float32, minval=0.5, maxval=1.5)
    return {'local_grads': local_grads, 'master': master, 'moment_one': moment_one, 'moment_two': moment_two}


def reference(local_grads, master, moment_one, moment_two):
    grad_mean = jnp.sum(local_grads, axis=0, dtype=jnp.float32) / DATA
    clip_scale = jnp.minimum(1.0, MAX_NORM / jnp.sqrt(jnp.sum(grad_mean * grad_mean)))
    scaled = clip_scale * grad_mean
    new_one = BETA_ONE * moment_one + (1.0 - BETA_ONE) * scaled
    new_two = BETA_TWO * moment_two + (1.0 - BETA_TWO) * scaled * scaled
    direction = (new_one / CORR_ONE) / (jnp.sqrt(new_two / CORR_TWO) + EPSILON) + WEIGHT_DECAY * master
    norm_sq = jnp.stack([jnp.sum(master * master, axis=1), jnp.sum(direction * direction, axis=1)])
    tensor_norms = jnp.sqrt(tensor_sums(norm_sq.reshape(2, LAYERS, 12)))
    block_ratio = spread_tensors(tensor_norms[0] / tensor_norms[1]).reshape(BLOCKS, 1)
    new_master = master - LEARN_RATE * block_ratio * direction
    return new_master.astype(jnp.bfloat16), new_master, new_one, new_two
```

```python
import functools

import jax
import jax.numpy as jnp
from jax import lax
from jax.experimental import pallas as pl
from jax.experimental.pallas import tpu as pltpu
from jax.sharding import PartitionSpec as P

STEP = 4
LEARN_RATE = 0.08
BETA_ONE = 0.9
BETA_TWO = 0.999
EPSILON = 1e-6
WEIGHT_DECAY = 0.01
MAX_NORM = 1.0
CORR_ONE = 1.0 - BETA_ONE ** STEP
CORR_TWO = 1.0 - BETA_TWO ** STEP

MESH = pl.DeviceIdType.MESH
F32 = jnp.float32
BF16 = jnp.bfloat16

SHARD = 147456
COLS = 12288
TOP_ROUTE = SHARD // 2
BOT_ROUTE = SHARD // 4
N_TOP = TOP_ROUTE // COLS
N_BOT = BOT_ROUTE // COLS
N_CHUNK = N_TOP + N_BOT
STRIP = 512


def flip(value):
    return 1 - value


def my_place():
    data_pos = lax.axis_index('data')
    return data_pos // 4, lax.rem(data_pos // 2, 2), lax.rem(data_pos, 2)


def data_index(pos_y, pos_x, core):
    return (pos_y * 2 + pos_x) * 2 + core


def others():
    mine = lax.axis_index('model') * 8 + lax.axis_index('data')
    for step in range(1, 16):
        other = lax.rem(mine + step, 16)
        yield other // 8, lax.rem(other, 8)


def enter_all():
    barrier = pltpu.get_barrier_semaphore()
    for device in others():
        pl.semaphore_signal(barrier, inc=1, device_id=device, device_id_type=MESH)
    pl.semaphore_wait(barrier, 15)


def drain(ref, sem):
    pltpu.make_async_copy(ref, ref, sem).wait()


def share_all(box, send_sem, recv_sem):
    mine = lax.axis_index('model') * 8 + lax.axis_index('data')
    for device in others():
        pltpu.make_async_remote_copy(src_ref=box.at[mine], dst_ref=box.at[mine], send_sem=send_sem, recv_sem=recv_sem, device_id=device, device_id_type=MESH).start()
    drain(box.at[pl.ds(0, 15)], send_sem)
    drain(box.at[pl.ds(0, 15)], recv_sem)


def chunk_views(array, shard, route, chunk, block, top):
    if top:
        start = pl.multiple_of(shard * SHARD + route * TOP_ROUTE + chunk * COLS, COLS)
        return [(array.at[pl.ds(0, 8), pl.ds(start, COLS)], block)]
    views = []
    for half in range(2):
        start = pl.multiple_of(shard * SHARD + half * TOP_ROUTE + route * BOT_ROUTE + (chunk - N_TOP) * COLS, COLS)
        views.append((array.at[pl.ds(8, 4), pl.ds(start, COLS)], block.at[pl.ds(4 * half, 4)]))
    return views


def reduce_kernel(grads, mean_out, total_out, first, sent, got, kept, box, first_send, first_recv, second_send, second_recv, out_sem, box_send, box_recv):
    pos_y, pos_x, core = my_place()
    model_pos = lax.axis_index('model')
    grad = grads.at[0]

    def local(chunk, top):
        for route in range(2):
            for far in range(2):
                row, col = ((lax.rem(pos_y + far, 2), pos_x), (pos_y, lax.rem(pos_x + far, 2)))[route]
                shard = data_index(row, col, core)
                for src, dst in chunk_views(grad, shard, route, chunk, first.at[route, chunk, 0, far], top):
                    pltpu.make_async_copy(src, dst, first_recv.at[route, chunk]).start()

    def remote(chunk, top):
        for far in range(2):
            for other in range(2):
                for route in range(2):
                    side = (pos_y, flip(pos_x)) if route == 0 else (flip(pos_y), pos_x)
                    to_core = lax.rem(core + other, 2)
                    row, col = (lax.rem(side[0] + far, 2), side[1]) if route == 0 else (side[0], lax.rem(side[1] + far, 2))
                    for src, dst in chunk_views(grad, data_index(row, col, to_core), route, chunk, first.at[route, chunk, 2 + other, far], top):
                        pltpu.make_async_remote_copy(src_ref=src, dst_ref=dst, send_sem=first_send.at[route, chunk], recv_sem=first_recv.at[route, chunk], device_id=(model_pos, data_index(side[0], side[1], to_core)), device_id_type=MESH).start()
            for route in range(2):
                row, col = ((lax.rem(pos_y + far, 2), pos_x), (pos_y, lax.rem(pos_x + far, 2)))[route]
                for src, dst in chunk_views(grad, data_index(row, col, flip(core)), route, chunk, first.at[route, chunk, 1, far], top):
                    pltpu.make_async_remote_copy(src_ref=src, dst_ref=dst, send_sem=first_send.at[route, chunk], recv_sem=first_recv.at[route, chunk], device_id=(model_pos, data_index(pos_y, pos_x, flip(core))), device_id_type=MESH).start()

    def over_chunks(body):
        pl.loop(0, N_TOP)(functools.partial(body, top=True))
        pl.loop(N_TOP, N_CHUNK)(functools.partial(body, top=False))

    over_chunks(local)
    enter_all()
    over_chunks(remote)

    def second(route, chunk):
        side = data_index(flip(pos_y), pos_x, core) if route == 0 else data_index(pos_y, flip(pos_x), core)
        return pltpu.make_async_remote_copy(src_ref=sent.at[route, chunk], dst_ref=got.at[route, chunk], send_sem=second_send.at[route, chunk], recv_sem=second_recv.at[route, chunk], device_id=(model_pos, side), device_id_type=MESH)

    def add_four(route, chunk):
        drain(first.at[route, chunk], first_recv.at[route, chunk])

        @pl.loop(0, COLS // STRIP)
        def _(strip):
            cols = pl.ds(pl.multiple_of(strip * STRIP, STRIP), STRIP)
            for far, target in ((0, kept), (1, sent)):
                parts = [first[route, chunk, source, far, :, cols].astype(F32) for source in range(4)]
                target[route, chunk, :, cols] = (parts[0] + parts[1]) + (parts[2] + parts[3])

    @pl.loop(0, N_CHUNK)
    def _(chunk):
        add_four(0, chunk)

        @pl.when(chunk > 0)
        def _():
            second(1, chunk - 1).start()

        add_four(1, chunk)
        second(0, chunk).start()

    second(1, N_CHUNK - 1).start()

    def writes(route, chunk, top):
        return [pltpu.make_async_copy(block, view, out_sem.at[route, chunk]) for view, block in chunk_views(mean_out, 0, route, chunk, kept.at[route, chunk], top)]

    def finish(chunk, squares, top):
        for route in range(2):
            drain(got.at[route, chunk], second_recv.at[route, chunk])

            def strip_body(strip, total):
                cols = pl.ds(pl.multiple_of(strip * STRIP, STRIP), STRIP)
                mean = (kept[route, chunk, :, cols] + got[route, chunk, :, cols]) * 0.125
                kept[route, chunk, :, cols] = mean
                square = mean * mean
                for tile in range(STRIP // 128):
                    total = total + square[:, tile * 128:(tile + 1) * 128]
                return total

            squares = lax.fori_loop(0, COLS // STRIP, strip_body, squares)
            for copy in writes(route, chunk, top):
                copy.start()
        return squares

    squares = lax.fori_loop(0, N_TOP, functools.partial(finish, top=True), jnp.zeros((8, 128), F32))
    squares = lax.fori_loop(N_TOP, N_CHUNK, functools.partial(finish, top=False), squares)
    box[model_pos * 8 + lax.axis_index('data')] = squares
    share_all(box, box_send, box_recv)
    total_out[...] = jnp.sum(box[...], axis=0)

    @pl.loop(0, N_CHUNK)
    def _(chunk):
        for route in range(2):
            drain(first.at[route, chunk, pl.ds(1, 3)], first_send.at[route, chunk])
            drain(sent.at[route, chunk], second_send.at[route, chunk])
            drain(kept.at[route, chunk], out_sem.at[route, chunk])


def reduce_grads(local_grads):
    sems = pltpu.SemaphoreType.DMA((2, N_CHUNK))
    return pl.pallas_call(
        reduce_kernel,
        out_shape=(jax.ShapeDtypeStruct((12, SHARD), F32), jax.ShapeDtypeStruct((8, 128), F32)),
        in_specs=[pl.BlockSpec(memory_space=pltpu.HBM)],
        out_specs=(pl.BlockSpec(memory_space=pltpu.HBM), pl.BlockSpec(memory_space=pltpu.VMEM)),
        scratch_shapes=[
            pltpu.VMEM((2, N_CHUNK, 4, 2, 8, COLS), BF16),
            pltpu.VMEM((2, N_CHUNK, 8, COLS), F32),
            pltpu.VMEM((2, N_CHUNK, 8, COLS), F32),
            pltpu.VMEM((2, N_CHUNK, 8, COLS), F32),
            pltpu.VMEM((16, 8, 128), F32),
            sems, sems, sems, sems, sems,
            pltpu.SemaphoreType.DMA, pltpu.SemaphoreType.DMA,
        ],
        compiler_params=pltpu.CompilerParams(collective_id=0, has_side_effects=True, vmem_limit_bytes=60 * 1024 * 1024),
        name='reduce_grads',
    )(local_grads)


def tensor_sums(block_values):
    return jnp.stack([block_values[..., 0:3].sum(axis=-1), block_values[..., 3], block_values[..., 4:8].sum(axis=-1), block_values[..., 8:12].sum(axis=-1)], axis=-1)


def spread_tensors(tensor_values):
    lead_shape = tensor_values.shape[:-1]
    pieces = [jnp.broadcast_to(tensor_values[..., tensor_pos:tensor_pos + 1], lead_shape + (block_count,)) for tensor_pos, block_count in enumerate((3, 1, 4, 4))]
    return jnp.concatenate(pieces, axis=-1)


def adam_direction(grad_mean, clip_scale, master, moment_one, moment_two):
    scaled = clip_scale * grad_mean
    new_one = BETA_ONE * moment_one + (1.0 - BETA_ONE) * scaled
    new_two = BETA_TWO * moment_two + (1.0 - BETA_TWO) * scaled * scaled
    direction = (new_one / CORR_ONE) / (jnp.sqrt(new_two / CORR_TWO) + EPSILON) + WEIGHT_DECAY * master
    return new_one, new_two, direction


def block_ratio(norm_sq):
    tensor_norms = jnp.sqrt(tensor_sums(norm_sq.reshape(2, -1, 12)))
    return spread_tensors(tensor_norms[0] / tensor_norms[1]).reshape(-1, 1)


def solution(mesh):
    both_axes = ('model', 'data')
    state_spec = P(None, both_axes)

    def device_step(local_grads, master, moment_one, moment_two):
        grad_mean, total = reduce_grads(local_grads)
        clip_scale = jnp.minimum(1.0, MAX_NORM / jnp.sqrt(jnp.sum(total)))
        new_one, new_two, direction = adam_direction(grad_mean, clip_scale, master, moment_one, moment_two)
        norm_sq = lax.psum(jnp.stack([jnp.sum(master * master, axis=1), jnp.sum(direction * direction, axis=1)]), both_axes)
        new_master = master - LEARN_RATE * block_ratio(norm_sq) * direction
        params = lax.all_gather(new_master.astype(jnp.bfloat16), 'data', axis=1, tiled=True)
        return params, new_master, new_one, new_two

    return jax.shard_map(device_step, mesh=mesh, in_specs=(P('data', None, 'model'), state_spec, state_spec, state_spec), out_specs=(P(None, 'model'), state_spec, state_spec, state_spec), check_vma=False)
```

```python
import functools

import jax
import jax.numpy as jnp
from jax import lax
from jax.experimental import pallas as pl
from jax.experimental.pallas import tpu as pltpu
from jax.sharding import PartitionSpec as P

STEP = 4
LEARN_RATE = 0.08
BETA_ONE = 0.9
BETA_TWO = 0.999
EPSILON = 1e-6
WEIGHT_DECAY = 0.01
MAX_NORM = 1.0
CORR_ONE = 1.0 - BETA_ONE ** STEP
CORR_TWO = 1.0 - BETA_TWO ** STEP

MESH = pl.DeviceIdType.MESH
F32 = jnp.float32
BF16 = jnp.bfloat16

SHARD = 147456
COLS = 12288
TOP_ROUTE = SHARD // 2
BOT_ROUTE = SHARD // 4
N_TOP = TOP_ROUTE // COLS
N_BOT = BOT_ROUTE // COLS
N_CHUNK = N_TOP + N_BOT
STRIP = 512

MIB = 1024 * 1024
STEP_LIMIT = 9 * MIB
WRITE_LIMIT = STEP_LIMIT


def flip(value):
    return 1 - value


def my_place():
    data_pos = lax.axis_index('data')
    return data_pos // 4, lax.rem(data_pos // 2, 2), lax.rem(data_pos, 2)


def data_index(pos_y, pos_x, core):
    return (pos_y * 2 + pos_x) * 2 + core


def others():
    mine = lax.axis_index('model') * 8 + lax.axis_index('data')
    for step in range(1, 16):
        other = lax.rem(mine + step, 16)
        yield other // 8, lax.rem(other, 8)


def enter_all():
    barrier = pltpu.get_barrier_semaphore()
    for device in others():
        pl.semaphore_signal(barrier, inc=1, device_id=device, device_id_type=MESH)
    pl.semaphore_wait(barrier, 15)


def drain(ref, sem):
    pltpu.make_async_copy(ref, ref, sem).wait()


def row_views(array, shard, route, chunk, block, top):
    if top:
        start = shard * SHARD + route * TOP_ROUTE + chunk * COLS
        return [(array.at[pl.ds(0, 8), pl.ds(pl.multiple_of(start, COLS), COLS)], block)]
    views = []
    for half in range(2):
        start = shard * SHARD + half * TOP_ROUTE + route * BOT_ROUTE + (chunk - N_TOP) * COLS
        views.append((array.at[pl.ds(8, 4), pl.ds(pl.multiple_of(start, COLS), COLS)], block.at[pl.ds(4 * half, 4)]))
    return views


def sweep(body, carry=0):
    carry = lax.fori_loop(0, N_TOP, functools.partial(body, top=True), carry)
    return lax.fori_loop(N_TOP, N_CHUNK, functools.partial(body, top=False), carry)


def strips(body, carry=0):
    def step(strip, carry):
        return body(pl.ds(pl.multiple_of(strip * STRIP, STRIP), STRIP), carry)

    return lax.fori_loop(0, COLS // STRIP, step, carry)


def fold(total, values):
    for tile in range(STRIP // 128):
        total = total + values[:, tile * 128:(tile + 1) * 128]
    return total


def step_kernel(
    grads, master_in, one_in, two_in,
    top_out, bot_out, master, one, two,
    mean, total_box, norm_box,
    first_send, first_recv, second_send, second_recv, load_sem,
    side_send, side_recv, forward_send, corner_recv, partner_send, partner_recv, box_sem,
):
    pos_y, pos_x, core = my_place()
    model_pos = lax.axis_index('model')
    mine = model_pos * 8 + lax.axis_index('data')
    grad = grads.at[0]
    sent, got = master, two
    chips = ((pos_y, pos_x), (pos_y, flip(pos_x)), (flip(pos_y), pos_x), (flip(pos_y), flip(pos_x)))
    places = [data_index(row, col, core) for row, col in chips]
    partner = data_index(pos_y, pos_x, flip(core))

    def copy_to(src, dst, place, send_sem, recv_sem):
        pltpu.make_async_remote_copy(src_ref=src, dst_ref=dst, send_sem=send_sem, recv_sem=recv_sem, device_id=(model_pos, place), device_id_type=MESH).start()

    def landing(route, chunk, block, count, top):
        if top:
            start = ((route * N_TOP + chunk) * 8 + block) * COLS
        else:
            start = ((route * N_BOT + chunk - N_TOP) * 8 + block) * COLS
        return (top_out if top else bot_out).at[:, pl.ds(pl.multiple_of(start, COLS), count * COLS)]

    def wanted(route, row, col, far):
        return (lax.rem(row + far, 2), col) if route == 0 else (row, lax.rem(col + far, 2))

    def local(chunk, carry, top):
        for route in range(2):
            for far in range(2):
                shard = data_index(*wanted(route, pos_y, pos_x, far), core)
                for src, dst in row_views(grad, shard, route, chunk, landing(route, chunk, far, 1, top), top):
                    pltpu.make_async_copy(src, dst, first_recv.at[route, chunk]).start()
        return carry

    def remote(chunk, carry, top):
        for far in range(2):
            for other in range(2):
                for route in range(2):
                    row, col = chips[1 + route]
                    to_core = lax.rem(core + other, 2)
                    shard = data_index(*wanted(route, row, col, far), to_core)
                    for src, dst in row_views(grad, shard, route, chunk, landing(route, chunk, 4 + 2 * other + far, 1, top), top):
                        copy_to(src, dst, data_index(row, col, to_core), first_send.at[route, chunk], first_recv.at[route, chunk])
            for route in range(2):
                shard = data_index(*wanted(route, pos_y, pos_x, far), flip(core))
                for src, dst in row_views(grad, shard, route, chunk, landing(route, chunk, 2 + far, 1, top), top):
                    copy_to(src, dst, partner, first_send.at[route, chunk], first_recv.at[route, chunk])
        return carry

    def load(which, array, block, route, chunk, top):
        for src, dst in row_views(array, 0, route, chunk, block.at[route, chunk], top):
            pltpu.make_async_copy(src, dst, load_sem.at[which, route, chunk]).start()

    sweep(local)
    enter_all()
    sweep(remote)

    def load_one(chunk, carry, top):
        for route in range(2):
            load(1, one_in, one, route, chunk, top)
        return carry

    sweep(load_one)

    def second(route, chunk):
        copy_to(sent.at[route, chunk], got.at[route, chunk], places[2 - route], second_send.at[route, chunk], second_recv.at[route, chunk])

    def add_four(route, chunk, top):
        drain(landing(route, chunk, 0, 8, top), first_recv.at[route, chunk])

        def body(cols, carry):
            for far, target in ((0, mean), (1, sent)):
                parts = [landing(route, chunk, 2 * source + far, 1, top)[:, cols].astype(F32) for source in range(4)]
                target[route, chunk, :, cols] = (parts[0] + parts[1]) + (parts[2] + parts[3])
            return carry

        strips(body)

    def first_sums(chunk, carry, top):
        add_four(0, chunk, top)

        @pl.when(chunk > 0)
        def _():
            second(1, chunk - 1)

        add_four(1, chunk, top)
        second(0, chunk)
        return carry

    sweep(first_sums)
    second(1, N_CHUNK - 1)

    def finish(chunk, squares, top):
        for route in range(2):
            drain(got.at[route, chunk], second_recv.at[route, chunk])

            def body(cols, total):
                value = (mean[route, chunk, :, cols] + got[route, chunk, :, cols]) * 0.125
                mean[route, chunk, :, cols] = value
                return fold(total, value * value)

            squares = strips(body, squares)
            load(2, two_in, two, route, chunk, top)
            drain(sent.at[route, chunk], second_send.at[route, chunk])
            load(0, master_in, master, route, chunk, top)
        return squares

    def share_all(box, send_sem, recv_sem):
        for device in others():
            pltpu.make_async_remote_copy(src_ref=box.at[mine], dst_ref=box.at[mine], send_sem=send_sem, recv_sem=recv_sem, device_id=device, device_id_type=MESH).start()
        drain(box.at[pl.ds(0, 15)], recv_sem)

    total_box[mine] = sweep(finish, jnp.zeros((8, 128), F32))
    share_all(total_box, box_sem.at[0], box_sem.at[1])
    total = jnp.sum(jnp.sum(total_box[...], axis=0), keepdims=True)
    clip = jnp.minimum(1.0, MAX_NORM / jnp.sqrt(total))

    def update(route, chunk, carry):
        for which, block in enumerate((master, one, two)):
            drain(block.at[route, chunk], load_sem.at[which, route, chunk])

        def body(cols, carry):
            place = (route, chunk, slice(None), cols)
            weight = master[place]
            scaled = clip * mean[place]
            new_one = BETA_ONE * one[place] + (1.0 - BETA_ONE) * scaled
            new_two = BETA_TWO * two[place] + (1.0 - BETA_TWO) * scaled * scaled
            direction = (new_one * (1.0 / CORR_ONE)) / (jnp.sqrt(new_two * (1.0 / CORR_TWO)) + EPSILON) + WEIGHT_DECAY * weight
            one[place] = new_one
            two[place] = new_two
            mean[place] = direction
            return fold(carry[0], weight * weight), fold(carry[1], direction * direction)

        return strips(body, carry)

    for index, (low, high) in enumerate(((0, N_TOP), (N_TOP, N_CHUNK))):
        zero = jnp.zeros((8, 128), F32)
        weight_sq, direction_sq = lax.fori_loop(low, high, lambda chunk, carry: update(1, chunk, update(0, chunk, carry)), (zero, zero))
        norm_box[mine, index] = weight_sq
        norm_box[mine, 2 + index] = direction_sq
    share_all(norm_box, box_sem.at[2], box_sem.at[3])
    sums = jnp.sum(jnp.sum(norm_box[...], axis=0), axis=2, keepdims=True)
    row = lax.broadcasted_iota(jnp.int32, (8, 1), 0)

    def norms(top_rows, bot_rows):
        pieces = [jnp.sum(jnp.where(mask, top_rows, 0.0), axis=0, keepdims=True) for mask in (row < 3, row == 3, row > 3)]
        top_all = jnp.where(row < 3, pieces[0], jnp.where(row == 3, pieces[1], pieces[2]))
        return jnp.sqrt(top_all), jnp.sqrt(jnp.sum(bot_rows, axis=0, keepdims=True) + jnp.zeros_like(top_all))

    weight_norms, direction_norms = norms(sums[0], sums[1]), norms(sums[2], sums[3])
    bot_rate, top_rate = [LEARN_RATE * (weight_norms[index] / direction_norms[index]) for index in (1, 0)]

    def piece(place, route, chunk, top):
        if top:
            start = place * SHARD + route * TOP_ROUTE + chunk * COLS
        else:
            start = place * (SHARD // 2) + route * BOT_ROUTE + (chunk - N_TOP) * COLS
        return (top_out if top else bot_out).at[:, pl.ds(pl.multiple_of(start, COLS), COLS)]

    def part(place, top, share=1):
        size = SHARD if top else SHARD // 2
        return (top_out if top else bot_out).at[:, pl.ds(pl.multiple_of(place * size, size), size // share)]

    def weights(route, chunk, top):
        rate = top_rate if top else bot_rate
        view = piece(places[0], route, chunk, top)

        def body(cols, carry):
            place = (route, chunk, slice(None), cols)
            value = master[place] - rate * mean[place]
            master[place] = value
            view[:, cols] = value.astype(BF16)
            return carry

        strips(body)

    def send(route, chunk, top):
        view = piece(places[0], route, chunk, top)
        kind = int(top)
        for axis in range(2):
            copy_to(view, view, places[1 + axis], side_send.at[axis, kind], side_recv.at[axis, route, chunk])
        copy_to(view, view, partner, partner_send.at[0, kind], partner_recv.at[0, kind])

    def own(chunk, carry, top):
        weights(0, chunk, top)

        @pl.when(chunk > (0 if top else N_TOP))
        def _():
            send(1, chunk - 1, top)

        weights(1, chunk, top)
        send(0, chunk, top)

        @pl.when(chunk == (N_TOP - 1 if top else N_CHUNK - 1))
        def _():
            send(1, chunk, top)

        return carry

    def hand_on(chunk, carry, top):
        kind = int(top)
        for route in range(2):
            for axis in range(2):
                view = piece(places[1 + axis], route, chunk, top)
                drain(view, side_recv.at[axis, route, chunk])
                if axis == route:
                    copy_to(view, view, places[2 - axis], forward_send.at[route, kind], corner_recv.at[route, chunk])
                copy_to(view, view, partner, partner_send.at[1 + axis, kind], partner_recv.at[1 + axis, kind])
        return carry

    def corner(chunk, carry, top):
        for route in range(2):
            view = piece(places[3], route, chunk, top)
            drain(view, corner_recv.at[route, chunk])
            copy_to(view, view, partner, partner_send.at[3, int(top)], partner_recv.at[3, int(top)])
        return carry

    sweep(own)
    sweep(hand_on)
    sweep(corner)

    for top in (True, False):
        kind = int(top)
        for axis in range(2):
            drain(part(places[0], top), side_send.at[axis, kind])
            drain(part(places[0], top, 2), forward_send.at[axis, kind])
        for chip, (row_pos, col_pos) in enumerate(chips):
            drain(part(places[chip], top), partner_send.at[chip, kind])
            drain(part(data_index(row_pos, col_pos, flip(core)), top), partner_recv.at[chip, kind])
    drain(total_box.at[pl.ds(0, 15)], box_sem.at[0])
    drain(norm_box.at[pl.ds(0, 15)], box_sem.at[2])

    def first_sent(chunk, carry, top):
        for route in range(2):
            drain(landing(route, chunk, 2, 6, top), first_send.at[route, chunk])
        return carry

    sweep(first_sent)


def in_hbm(array):
    return pltpu.with_memory_space_constraint(array, pltpu.HBM)


def run_step(local_grads, master, moment_one, moment_two):
    dma = pltpu.SemaphoreType.DMA
    block = pltpu.VMEM((2, N_CHUNK, 8, COLS), F32)
    each = dma((2, N_CHUNK))
    return pl.pallas_call(
        step_kernel,
        out_shape=(pltpu.VMEM((8, 8 * SHARD), BF16), pltpu.VMEM((8, 4 * SHARD), BF16), block, block, block),
        in_specs=[pl.BlockSpec(memory_space=pltpu.HBM)] * 4,
        out_specs=(pl.BlockSpec(memory_space=pltpu.VMEM),) * 5,
        scratch_shapes=[
            block,
            pltpu.VMEM((16, 8, 128), F32),
            pltpu.VMEM((16, 4, 8, 128), F32),
            each, each, each, each, dma((3, 2, N_CHUNK)),
            dma((2, 2)), dma((2, 2, N_CHUNK)), dma((2, 2)), each, dma((4, 2)), dma((4, 2)), dma((4,)),
        ],
        compiler_params=pltpu.CompilerParams(collective_id=0, has_side_effects=True, vmem_limit_bytes=STEP_LIMIT),
        name='lamb_step',
    )(in_hbm(local_grads), in_hbm(master), in_hbm(moment_one), in_hbm(moment_two))


def write_kernel(top, bot, master, one, two, params_out, master_out, one_out, two_out, sem):
    copies = []
    for place in range(8):
        copies.append((top.at[:, pl.ds(place * SHARD, SHARD)], params_out.at[pl.ds(0, 8), pl.ds(place * SHARD, SHARD)]))
        for half in range(2):
            copies.append((bot.at[pl.ds(4 * half, 4), pl.ds(place * TOP_ROUTE, TOP_ROUTE)], params_out.at[pl.ds(8, 4), pl.ds(place * SHARD + half * TOP_ROUTE, TOP_ROUTE)]))
    for block, array in ((master, master_out), (one, one_out), (two, two_out)):
        for route in range(2):
            for chunk in range(N_CHUNK):
                copies += [(src, dst) for dst, src in row_views(array, 0, route, chunk, block.at[route, chunk], chunk < N_TOP)]
    for index, (src, dst) in enumerate(copies):
        pltpu.make_async_copy(src, dst, sem.at[index]).start()
    for index, (src, dst) in enumerate(copies):
        pltpu.make_async_copy(src, dst, sem.at[index]).wait()


def write_out(*blocks):
    state = jax.ShapeDtypeStruct((12, SHARD), F32)
    return pl.pallas_call(
        write_kernel,
        out_shape=(jax.ShapeDtypeStruct((12, 8 * SHARD), BF16), state, state, state),
        in_specs=[pl.BlockSpec(memory_space=pltpu.VMEM)] * 5,
        out_specs=(pl.BlockSpec(memory_space=pltpu.HBM),) * 4,
        scratch_shapes=[pltpu.SemaphoreType.DMA((24 + 6 * (N_TOP + 2 * N_BOT),))],
        compiler_params=pltpu.CompilerParams(vmem_limit_bytes=WRITE_LIMIT),
        name='write_out',
    )(*[pltpu.with_memory_space_constraint(block, pltpu.VMEM) for block in blocks])


def solution(mesh):
    state_spec = P(None, ('model', 'data'))

    def device_step(local_grads, master, moment_one, moment_two):
        return write_out(*run_step(local_grads, master, moment_one, moment_two))

    return jax.shard_map(device_step, mesh=mesh, in_specs=(P('data', None, 'model'), state_spec, state_spec, state_spec), out_specs=(P(None, 'model'), state_spec, state_spec, state_spec), check_vma=False)
```

```python
import functools

import jax
import jax.numpy as jnp
from jax import lax
from jax.experimental import pallas as pl
from jax.experimental.pallas import tpu as pltpu
from jax.sharding import PartitionSpec as P

STEP = 4
LEARN_RATE = 0.08
BETA_ONE = 0.9
BETA_TWO = 0.999
EPSILON = 1e-6
WEIGHT_DECAY = 0.01
MAX_NORM = 1.0
CORR_ONE = 1.0 - BETA_ONE ** STEP
CORR_TWO = 1.0 - BETA_TWO ** STEP

MESH = pl.DeviceIdType.MESH
F32 = jnp.float32
BF16 = jnp.bfloat16

SHARD = 147456
COLS = 12288
TOP_ROUTE = SHARD // 2
BOT_ROUTE = SHARD // 4
N_TOP = TOP_ROUTE // COLS
N_BOT = BOT_ROUTE // COLS
N_CHUNK = N_TOP + N_BOT
STRIP = 1024

TINY = 1.2e-38
MIB = 1024 * 1024
STEP_LIMIT = 9 * MIB
WRITE_LIMIT = STEP_LIMIT


def flip(value):
    return 1 - value


def my_place():
    data_pos = lax.axis_index('data')
    return data_pos // 4, lax.rem(data_pos // 2, 2), lax.rem(data_pos, 2)


def data_index(pos_y, pos_x, core):
    return (pos_y * 2 + pos_x) * 2 + core


def others():
    mine = lax.axis_index('model') * 8 + lax.axis_index('data')
    for step in range(1, 16):
        other = lax.rem(mine + step, 16)
        yield other // 8, lax.rem(other, 8)


def enter_all():
    barrier = pltpu.get_barrier_semaphore()
    for device in others():
        pl.semaphore_signal(barrier, inc=1, device_id=device, device_id_type=MESH)
    pl.semaphore_wait(barrier, 15)


def drain(ref, sem):
    pltpu.make_async_copy(ref, ref, sem).wait()


def row_views(array, shard, route, chunk, block, top):
    if top:
        start = shard * SHARD + route * TOP_ROUTE + chunk * COLS
        return [(array.at[pl.ds(0, 8), pl.ds(pl.multiple_of(start, COLS), COLS)], block)]
    views = []
    for half in range(2):
        start = shard * SHARD + half * TOP_ROUTE + route * BOT_ROUTE + (chunk - N_TOP) * COLS
        views.append((array.at[pl.ds(8, 4), pl.ds(pl.multiple_of(start, COLS), COLS)], block.at[pl.ds(4 * half, 4)]))
    return views


def sweep(body, carry=0):
    carry = lax.fori_loop(0, N_TOP, functools.partial(body, top=True), carry)
    return lax.fori_loop(N_TOP, N_CHUNK, functools.partial(body, top=False), carry)


def strips(body, carry=0):
    def step(strip, carry):
        return body(pl.ds(pl.multiple_of(strip * STRIP, STRIP), STRIP), carry)

    return lax.fori_loop(0, COLS // STRIP, step, carry)


def fold(total, values):
    for tile in range(STRIP // 128):
        total = total + values[:, tile * 128:(tile + 1) * 128]
    return total


def step_kernel(
    grads, master_in, one_in, two_in,
    top_out, bot_out, master, one, two,
    mean, total_box, norm_box,
    first_send, first_recv, second_send, second_recv, load_sem,
    side_send, side_recv, forward_send, corner_recv, partner_send, partner_recv, box_sem,
):
    pos_y, pos_x, core = my_place()
    model_pos = lax.axis_index('model')
    mine = model_pos * 8 + lax.axis_index('data')
    grad = grads.at[0]
    sent, got = master, two
    chips = ((pos_y, pos_x), (pos_y, flip(pos_x)), (flip(pos_y), pos_x), (flip(pos_y), flip(pos_x)))
    places = [data_index(row, col, core) for row, col in chips]
    partner = data_index(pos_y, pos_x, flip(core))

    def copy_to(src, dst, place, send_sem, recv_sem):
        pltpu.make_async_remote_copy(src_ref=src, dst_ref=dst, send_sem=send_sem, recv_sem=recv_sem, device_id=(model_pos, place), device_id_type=MESH).start()

    def landing(route, chunk, block, count, top):
        if top:
            start = ((route * N_TOP + chunk) * 8 + block) * COLS
        else:
            start = ((route * N_BOT + chunk - N_TOP) * 8 + block) * COLS
        return (top_out if top else bot_out).at[:, pl.ds(pl.multiple_of(start, COLS), count * COLS)]

    def wanted(route, row, col, far):
        return (lax.rem(row + far, 2), col) if route == 0 else (row, lax.rem(col + far, 2))

    def local(chunk, carry, top):
        for route in range(2):
            for far in range(2):
                shard = data_index(*wanted(route, pos_y, pos_x, far), core)
                for src, dst in row_views(grad, shard, route, chunk, landing(route, chunk, far, 1, top), top):
                    pltpu.make_async_copy(src, dst, first_recv.at[route, chunk]).start()
        return carry

    def remote(chunk, carry, top):
        for far in range(2):
            for other in range(2):
                for route in range(2):
                    row, col = chips[1 + route]
                    to_core = lax.rem(core + other, 2)
                    shard = data_index(*wanted(route, row, col, far), to_core)
                    for src, dst in row_views(grad, shard, route, chunk, landing(route, chunk, 4 + 2 * other + far, 1, top), top):
                        copy_to(src, dst, data_index(row, col, to_core), first_send.at[route, chunk], first_recv.at[route, chunk])
            for route in range(2):
                shard = data_index(*wanted(route, pos_y, pos_x, far), flip(core))
                for src, dst in row_views(grad, shard, route, chunk, landing(route, chunk, 2 + far, 1, top), top):
                    copy_to(src, dst, partner, first_send.at[route, chunk], first_recv.at[route, chunk])
        return carry

    def load(which, array, block, route, chunk, top):
        for src, dst in row_views(array, 0, route, chunk, block.at[route, chunk], top):
            pltpu.make_async_copy(src, dst, load_sem.at[which, route, chunk]).start()

    sweep(local)
    enter_all()
    sweep(remote)

    def load_one(chunk, carry, top):
        for route in range(2):
            load(1, one_in, one, route, chunk, top)
        return carry

    sweep(load_one)

    def second(route, chunk):
        copy_to(sent.at[route, chunk], got.at[route, chunk], places[2 - route], second_send.at[route, chunk], second_recv.at[route, chunk])

    def add_four(route, chunk, top):
        drain(landing(route, chunk, 0, 8, top), first_recv.at[route, chunk])

        def body(cols, carry):
            for far, target in ((0, mean), (1, sent)):
                parts = [landing(route, chunk, 2 * source + far, 1, top)[:, cols].astype(F32) for source in range(4)]
                target[route, chunk, :, cols] = (parts[0] + parts[1]) + (parts[2] + parts[3])
            return carry

        strips(body)

    def first_sums(chunk, carry, top):
        add_four(0, chunk, top)

        @pl.when(chunk > 0)
        def _():
            second(1, chunk - 1)

        add_four(1, chunk, top)
        second(0, chunk)
        return carry

    sweep(first_sums)
    second(1, N_CHUNK - 1)

    def finish(chunk, squares, top):
        for route in range(2):
            drain(got.at[route, chunk], second_recv.at[route, chunk])

            def body(cols, total):
                value = (mean[route, chunk, :, cols] + got[route, chunk, :, cols]) * 0.125
                mean[route, chunk, :, cols] = value
                return fold(total, value * value)

            squares = strips(body, squares)
            load(2, two_in, two, route, chunk, top)
            drain(sent.at[route, chunk], second_send.at[route, chunk])
            load(0, master_in, master, route, chunk, top)
        return squares

    def share_all(box, send_sem, recv_sem):
        for device in others():
            pltpu.make_async_remote_copy(src_ref=box.at[mine], dst_ref=box.at[mine], send_sem=send_sem, recv_sem=recv_sem, device_id=device, device_id_type=MESH).start()

    total_box[mine] = sweep(finish, jnp.zeros((8, 128), F32))
    share_all(total_box, box_sem.at[0], box_sem.at[1])
    drain(total_box.at[pl.ds(0, 15)], box_sem.at[1])
    total = jnp.sum(jnp.sum(total_box[...], axis=0), keepdims=True)
    clip = jnp.minimum(1.0, MAX_NORM / jnp.sqrt(total))
    one_scale, two_scale = clip * (1.0 - BETA_ONE), clip * (1.0 - BETA_TWO) ** 0.5

    def update(route, chunk, carry):
        for which, block in enumerate((master, one, two)):
            drain(block.at[route, chunk], load_sem.at[which, route, chunk])

        def body(cols, carry):
            place = (route, chunk, slice(None), cols)
            weight = master[place]
            value = mean[place]
            new_one = BETA_ONE * one[place] + one_scale * value
            change = two_scale * value
            new_two = BETA_TWO * two[place] + change * change
            one[place] = new_one
            two[place] = new_two
            floor = jnp.maximum(new_two, TINY)
            root = floor * lax.rsqrt(floor)
            direction = (new_one * (CORR_TWO ** 0.5 / CORR_ONE)) / (root + EPSILON * CORR_TWO ** 0.5) + WEIGHT_DECAY * weight
            mean[place] = direction
            return fold(carry[0], weight * weight), fold(carry[1], direction * direction)

        return strips(body, carry)

    def update_rows(index, low, high):
        zero = jnp.zeros((8, 128), F32)
        weight_sq, direction_sq = lax.fori_loop(low, high, lambda chunk, carry: update(1, chunk, update(0, chunk, carry)), (zero, zero))
        box = norm_box.at[index]
        box[mine, 0] = weight_sq
        box[mine, 1] = direction_sq
        share_all(box, box_sem.at[2 + index], box_sem.at[4 + index])

    def row_sums(index):
        box = norm_box.at[index]
        drain(box.at[pl.ds(0, 15)], box_sem.at[4 + index])
        return jnp.sum(jnp.sum(box[...], axis=0), axis=2, keepdims=True)

    def bot_rate():
        sums = jnp.sqrt(jnp.sum(row_sums(0), axis=1, keepdims=True))
        return LEARN_RATE * (sums[0] / sums[1]) + jnp.zeros((8, 1), F32)

    def top_rate():
        sums = row_sums(1)
        row = lax.broadcasted_iota(jnp.int32, (8, 1), 0)

        def norms(values):
            pieces = [jnp.sum(jnp.where(mask, values, 0.0), axis=0, keepdims=True) for mask in (row < 3, row == 3, row > 3)]
            return jnp.sqrt(jnp.where(row < 3, pieces[0], jnp.where(row == 3, pieces[1], pieces[2])))

        return LEARN_RATE * (norms(sums[0]) / norms(sums[1]))

    update_rows(0, N_TOP, N_CHUNK)
    update_rows(1, 0, N_TOP)

    def piece(place, route, chunk, top):
        if top:
            start = place * SHARD + route * TOP_ROUTE + chunk * COLS
        else:
            start = place * (SHARD // 2) + route * BOT_ROUTE + (chunk - N_TOP) * COLS
        return (top_out if top else bot_out).at[:, pl.ds(pl.multiple_of(start, COLS), COLS)]

    def part(place, top, share=1):
        size = SHARD if top else SHARD // 2
        return (top_out if top else bot_out).at[:, pl.ds(pl.multiple_of(place * size, size), size // share)]

    def weights(route, chunk, rate, top):
        view = piece(places[0], route, chunk, top)

        def body(cols, carry):
            place = (route, chunk, slice(None), cols)
            value = master[place] - rate * mean[place]
            master[place] = value
            view[:, cols] = value.astype(BF16)
            return carry

        strips(body)

    def send(route, chunk, top):
        view = piece(places[0], route, chunk, top)
        kind = int(top)
        for axis in range(2):
            copy_to(view, view, places[1 + axis], side_send.at[axis, kind], side_recv.at[axis, route, chunk])
        copy_to(view, view, partner, partner_send.at[0, kind], partner_recv.at[0, kind])

    def own(chunk, rate, top):
        weights(0, chunk, rate, top)

        @pl.when(chunk > (0 if top else N_TOP))
        def _():
            send(1, chunk - 1, top)

        weights(1, chunk, rate, top)
        send(0, chunk, top)

        @pl.when(chunk == (N_TOP - 1 if top else N_CHUNK - 1))
        def _():
            send(1, chunk, top)

        return rate

    def hand_on(chunk, carry, top):
        kind = int(top)
        for route in range(2):
            for axis in range(2):
                view = piece(places[1 + axis], route, chunk, top)
                drain(view, side_recv.at[axis, route, chunk])
                if axis == route:
                    copy_to(view, view, places[2 - axis], forward_send.at[route, kind], corner_recv.at[route, chunk])
                copy_to(view, view, partner, partner_send.at[1 + axis, kind], partner_recv.at[1 + axis, kind])
        return carry

    def corner(chunk, carry, top):
        for route in range(2):
            view = piece(places[3], route, chunk, top)
            drain(view, corner_recv.at[route, chunk])
            copy_to(view, view, partner, partner_send.at[3, int(top)], partner_recv.at[3, int(top)])
        return carry

    def bottom_first(body, carry=0):
        carry = lax.fori_loop(N_TOP, N_CHUNK, functools.partial(body, top=False), carry)
        return lax.fori_loop(0, N_TOP, functools.partial(body, top=True), carry)

    lax.fori_loop(N_TOP, N_CHUNK, functools.partial(own, top=False), bot_rate())
    lax.fori_loop(0, N_TOP, functools.partial(own, top=True), top_rate())
    bottom_first(hand_on)
    bottom_first(corner)

    for top in (True, False):
        kind = int(top)
        for axis in range(2):
            drain(part(places[0], top), side_send.at[axis, kind])
            drain(part(places[0], top, 2), forward_send.at[axis, kind])
        for chip, (row_pos, col_pos) in enumerate(chips):
            drain(part(places[chip], top), partner_send.at[chip, kind])
            drain(part(data_index(row_pos, col_pos, flip(core)), top), partner_recv.at[chip, kind])
    drain(total_box.at[pl.ds(0, 15)], box_sem.at[0])
    for index in range(2):
        drain(norm_box.at[index, pl.ds(0, 15)], box_sem.at[2 + index])

    def first_sent(chunk, carry, top):
        for route in range(2):
            drain(landing(route, chunk, 2, 6, top), first_send.at[route, chunk])
        return carry

    sweep(first_sent)


def in_hbm(array):
    return pltpu.with_memory_space_constraint(array, pltpu.HBM)


def run_step(local_grads, master, moment_one, moment_two):
    dma = pltpu.SemaphoreType.DMA
    block = pltpu.VMEM((2, N_CHUNK, 8, COLS), F32)
    each = dma((2, N_CHUNK))
    return pl.pallas_call(
        step_kernel,
        out_shape=(pltpu.VMEM((8, 8 * SHARD), BF16), pltpu.VMEM((8, 4 * SHARD), BF16), block, block, block),
        in_specs=[pl.BlockSpec(memory_space=pltpu.HBM)] * 4,
        out_specs=(pl.BlockSpec(memory_space=pltpu.VMEM),) * 5,
        scratch_shapes=[
            block,
            pltpu.VMEM((16, 8, 128), F32),
            pltpu.VMEM((2, 16, 2, 8, 128), F32),
            each, each, each, each, dma((3, 2, N_CHUNK)),
            dma((2, 2)), dma((2, 2, N_CHUNK)), dma((2, 2)), each, dma((4, 2)), dma((4, 2)), dma((6,)),
        ],
        compiler_params=pltpu.CompilerParams(collective_id=0, has_side_effects=True, vmem_limit_bytes=STEP_LIMIT),
        name='lamb_step',
    )(in_hbm(local_grads), in_hbm(master), in_hbm(moment_one), in_hbm(moment_two))


def write_kernel(top, bot, master, one, two, params_out, master_out, one_out, two_out, sem):
    copies = []
    for place in range(8):
        copies.append((top.at[:, pl.ds(place * SHARD, SHARD)], params_out.at[pl.ds(0, 8), pl.ds(place * SHARD, SHARD)]))
        for half in range(2):
            copies.append((bot.at[pl.ds(4 * half, 4), pl.ds(place * TOP_ROUTE, TOP_ROUTE)], params_out.at[pl.ds(8, 4), pl.ds(place * SHARD + half * TOP_ROUTE, TOP_ROUTE)]))
    for block, array in ((master, master_out), (one, one_out), (two, two_out)):
        for route in range(2):
            for chunk in range(N_CHUNK):
                copies += [(src, dst) for dst, src in row_views(array, 0, route, chunk, block.at[route, chunk], chunk < N_TOP)]
    for index, (src, dst) in enumerate(copies):
        pltpu.make_async_copy(src, dst, sem.at[index]).start()
    for index, (src, dst) in enumerate(copies):
        pltpu.make_async_copy(src, dst, sem.at[index]).wait()


def write_out(*blocks):
    state = jax.ShapeDtypeStruct((12, SHARD), F32)
    return pl.pallas_call(
        write_kernel,
        out_shape=(jax.ShapeDtypeStruct((12, 8 * SHARD), BF16), state, state, state),
        in_specs=[pl.BlockSpec(memory_space=pltpu.VMEM)] * 5,
        out_specs=(pl.BlockSpec(memory_space=pltpu.HBM),) * 4,
        scratch_shapes=[pltpu.SemaphoreType.DMA((24 + 6 * (N_TOP + 2 * N_BOT),))],
        compiler_params=pltpu.CompilerParams(vmem_limit_bytes=WRITE_LIMIT),
        name='write_out',
    )(*[pltpu.with_memory_space_constraint(block, pltpu.VMEM) for block in blocks])


def solution(mesh):
    state_spec = P(None, ('model', 'data'))

    def device_step(local_grads, master, moment_one, moment_two):
        return write_out(*run_step(local_grads, master, moment_one, moment_two))

    return jax.shard_map(device_step, mesh=mesh, in_specs=(P('data', None, 'model'), state_spec, state_spec, state_spec), out_specs=(P(None, 'model'), state_spec, state_spec, state_spec), check_vma=False)
```

```python
import functools

import jax
import jax.numpy as jnp
from jax import lax
from jax.experimental import pallas as pl
from jax.experimental.pallas import tpu as pltpu
from jax.sharding import PartitionSpec as P

STEP = 4
LEARN_RATE = 0.08
BETA_ONE = 0.9
BETA_TWO = 0.999
EPSILON = 1e-6
WEIGHT_DECAY = 0.01
MAX_NORM = 1.0
CORR_ONE = 1.0 - BETA_ONE ** STEP
CORR_TWO = 1.0 - BETA_TWO ** STEP

MESH = pl.DeviceIdType.MESH
F32 = jnp.float32
BF16 = jnp.bfloat16

SHARD = 147456
COLS = 12288
TOP_ROUTE = SHARD // 2
BOT_ROUTE = SHARD // 4
N_TOP = TOP_ROUTE // COLS
N_BOT = BOT_ROUTE // COLS
N_CHUNK = N_TOP + N_BOT
N_EARLY = 2 * N_TOP // 3
STRIP = 1024
UPDATE_STRIP = 2048

TINY = 1.2e-38
MIB = 1024 * 1024
STEP_LIMIT = 9 * MIB
WRITE_LIMIT = STEP_LIMIT


def flip(value):
    return 1 - value


def my_place():
    data_pos = lax.axis_index('data')
    return data_pos // 4, lax.rem(data_pos // 2, 2), lax.rem(data_pos, 2)


def data_index(pos_y, pos_x, core):
    return (pos_y * 2 + pos_x) * 2 + core


def others():
    mine = lax.axis_index('model') * 8 + lax.axis_index('data')
    for step in range(1, 16):
        other = lax.rem(mine + step, 16)
        yield other // 8, lax.rem(other, 8)


def drain(ref, sem):
    pltpu.make_async_copy(ref, ref, sem).wait()


def row_views(array, shard, route, chunk, block, top):
    if top:
        start = shard * SHARD + route * TOP_ROUTE + chunk * COLS
        return [(array.at[pl.ds(0, 8), pl.ds(pl.multiple_of(start, COLS), COLS)], block)]
    views = []
    for half in range(2):
        start = shard * SHARD + half * TOP_ROUTE + route * BOT_ROUTE + (chunk - N_TOP) * COLS
        views.append((array.at[pl.ds(8, 4), pl.ds(pl.multiple_of(start, COLS), COLS)], block.at[pl.ds(4 * half, 4)]))
    return views


def sweep(body, carry=0):
    carry = lax.fori_loop(0, N_TOP, functools.partial(body, top=True), carry)
    return lax.fori_loop(N_TOP, N_CHUNK, functools.partial(body, top=False), carry)


def strips(body, carry=0, width=STRIP):
    def step(strip, carry):
        return body(pl.ds(pl.multiple_of(strip * width, width), width), carry)

    return lax.fori_loop(0, COLS // width, step, carry)


def fold(total, values):
    for tile in range(values.shape[1] // 128):
        total = total + values[:, tile * 128:(tile + 1) * 128]
    return total


def step_kernel(
    grads, master_in, one_in, two_in,
    top_out, bot_out, master, one, two,
    mean, total_box, norm_box,
    first_send, first_recv, second_send, second_recv, load_sem,
    side_send, side_recv, forward_send, corner_recv, partner_send, partner_recv, box_sem, seen, known,
):
    pos_y, pos_x, core = my_place()
    model_pos = lax.axis_index('model')
    mine = model_pos * 8 + lax.axis_index('data')
    grad = grads.at[0]
    sent, got = master, two
    chips = ((pos_y, pos_x), (pos_y, flip(pos_x)), (flip(pos_y), pos_x), (flip(pos_y), flip(pos_x)))
    places = [data_index(row, col, core) for row, col in chips]
    partner = data_index(pos_y, pos_x, flip(core))

    def copy_to(src, dst, place, send_sem, recv_sem):
        pltpu.make_async_remote_copy(src_ref=src, dst_ref=dst, send_sem=send_sem, recv_sem=recv_sem, device_id=(model_pos, place), device_id_type=MESH).start()

    def landing(route, chunk, block, count, top):
        if top:
            start = ((route * N_TOP + chunk) * 8 + block) * COLS
        else:
            start = ((route * N_BOT + chunk - N_TOP) * 8 + block) * COLS
        return (top_out if top else bot_out).at[:, pl.ds(pl.multiple_of(start, COLS), count * COLS)]

    def wanted(route, row, col, far):
        return (lax.rem(row + far, 2), col) if route == 0 else (row, lax.rem(col + far, 2))

    def local(chunk, carry, top):
        for route in range(2):
            for far in range(2):
                shard = data_index(*wanted(route, pos_y, pos_x, far), core)
                for src, dst in row_views(grad, shard, route, chunk, landing(route, chunk, far, 1, top), top):
                    pltpu.make_async_copy(src, dst, first_recv.at[route, chunk]).start()
        return carry

    def remote(chunk, carry, top):
        for far in range(2):
            for other in range(2):
                for route in range(2):
                    row, col = chips[1 + route]
                    to_core = lax.rem(core + other, 2)
                    shard = data_index(*wanted(route, row, col, far), to_core)
                    for src, dst in row_views(grad, shard, route, chunk, landing(route, chunk, 4 + 2 * other + far, 1, top), top):
                        copy_to(src, dst, data_index(row, col, to_core), first_send.at[route, chunk], first_recv.at[route, chunk])
            for route in range(2):
                shard = data_index(*wanted(route, pos_y, pos_x, far), flip(core))
                for src, dst in row_views(grad, shard, route, chunk, landing(route, chunk, 2 + far, 1, top), top):
                    copy_to(src, dst, partner, first_send.at[route, chunk], first_recv.at[route, chunk])
        return carry

    def load(which, array, block, route, chunk, top):
        for src, dst in row_views(array, 0, route, chunk, block.at[route, chunk], top):
            pltpu.make_async_copy(src, dst, load_sem.at[which, route, chunk]).start()

    next_to = [(model_pos, place) for chip in (1, 2) for place in (places[chip], data_index(*chips[chip], flip(core)))] + [(model_pos, partner), (flip(model_pos), places[0])]

    def tell(sem, devices):
        for device in devices:
            pl.semaphore_signal(sem, inc=1, device_id=device, device_id_type=MESH)

    sweep(local)
    barrier = pltpu.get_barrier_semaphore()
    tell(barrier, next_to)
    pl.semaphore_wait(barrier, len(next_to))
    sweep(remote)
    tell(seen, next_to)

    def load_one(chunk, carry, top):
        for route in range(2):
            load(1, one_in, one, route, chunk, top)
        return carry

    sweep(load_one)
    pl.semaphore_wait(seen, len(next_to))
    tell(known, next_to[-1:])

    def second(route, chunk):
        copy_to(sent.at[route, chunk], got.at[route, chunk], places[2 - route], second_send.at[route, chunk], second_recv.at[route, chunk])

    def add_four(route, chunk, top):
        drain(landing(route, chunk, 0, 8, top), first_recv.at[route, chunk])

        def body(cols, carry):
            for far, target in ((0, mean), (1, sent)):
                parts = [landing(route, chunk, 2 * source + far, 1, top)[:, cols].astype(F32) for source in range(4)]
                target[route, chunk, :, cols] = (parts[0] + parts[1]) + (parts[2] + parts[3])
            return carry

        strips(body)

    def first_sums(chunk, carry, top):
        add_four(0, chunk, top)

        @pl.when(chunk > 0)
        def _():
            second(1, chunk - 1)

        add_four(1, chunk, top)
        second(0, chunk)
        return carry

    sweep(first_sums)
    second(1, N_CHUNK - 1)

    def finish(chunk, squares, top):
        for route in range(2):
            drain(got.at[route, chunk], second_recv.at[route, chunk])

            def body(cols, total):
                value = (mean[route, chunk, :, cols] + got[route, chunk, :, cols]) * 0.125
                mean[route, chunk, :, cols] = value
                return fold(total, value * value)

            squares = strips(body, squares)
            load(2, two_in, two, route, chunk, top)
            drain(sent.at[route, chunk], second_send.at[route, chunk])
            load(0, master_in, master, route, chunk, top)
        return squares

    def share_all(box, send_sem, recv_sem):
        for device in others():
            pltpu.make_async_remote_copy(src_ref=box.at[mine], dst_ref=box.at[mine], send_sem=send_sem, recv_sem=recv_sem, device_id=device, device_id_type=MESH).start()

    total_box[mine] = sweep(finish, jnp.zeros((8, 128), F32))
    pl.semaphore_wait(known, 1)
    share_all(total_box, box_sem.at[0], box_sem.at[1])
    drain(total_box.at[pl.ds(0, 15)], box_sem.at[1])
    total = jnp.sum(jnp.sum(total_box[...], axis=0), keepdims=True)
    clip = jnp.minimum(1.0, MAX_NORM / jnp.sqrt(total))
    one_scale, two_scale = clip * (1.0 - BETA_ONE), clip * (1.0 - BETA_TWO) ** 0.5

    def update(route, chunk, carry):
        for which, block in enumerate((master, one, two)):
            drain(block.at[route, chunk], load_sem.at[which, route, chunk])

        def body(cols, carry):
            place = (route, chunk, slice(None), cols)
            weight = master[place]
            value = mean[place]
            new_one = BETA_ONE * one[place] + one_scale * value
            change = two_scale * value
            new_two = BETA_TWO * two[place] + change * change
            one[place] = new_one
            two[place] = new_two
            floor = jnp.maximum(new_two, TINY)
            root = floor * lax.rsqrt(floor)
            direction = (new_one * (CORR_TWO ** 0.5 / CORR_ONE)) / (root + EPSILON * CORR_TWO ** 0.5) + WEIGHT_DECAY * weight
            mean[place] = direction
            return fold(carry[0], weight * weight), fold(carry[1], direction * direction)

        return strips(body, carry, UPDATE_STRIP)

    def update_rows(low, high, carry=None):
        zero = jnp.zeros((8, 128), F32)
        return lax.fori_loop(low, high, lambda chunk, carry: update(1, chunk, update(0, chunk, carry)), carry or (zero, zero))

    def share_norms(index, squares):
        box = norm_box.at[index]
        box[mine, 0], box[mine, 1] = squares
        share_all(box, box_sem.at[2 + index], box_sem.at[4 + index])

    def row_sums(index):
        box = norm_box.at[index]
        drain(box.at[pl.ds(0, 15)], box_sem.at[4 + index])
        return jnp.sum(jnp.sum(box[...], axis=0), axis=2, keepdims=True)

    def bot_rate():
        sums = jnp.sqrt(jnp.sum(row_sums(0), axis=1, keepdims=True))
        return LEARN_RATE * (sums[0] / sums[1]) + jnp.zeros((8, 1), F32)

    def top_rate():
        sums = row_sums(1)
        row = lax.broadcasted_iota(jnp.int32, (8, 1), 0)

        def norms(values):
            pieces = [jnp.sum(jnp.where(mask, values, 0.0), axis=0, keepdims=True) for mask in (row < 3, row == 3, row > 3)]
            return jnp.sqrt(jnp.where(row < 3, pieces[0], jnp.where(row == 3, pieces[1], pieces[2])))

        return LEARN_RATE * (norms(sums[0]) / norms(sums[1]))

    share_norms(0, update_rows(N_TOP, N_CHUNK))
    top_squares = update_rows(0, N_EARLY)

    def piece(place, route, chunk, top):
        if top:
            start = place * SHARD + route * TOP_ROUTE + chunk * COLS
        else:
            start = place * (SHARD // 2) + route * BOT_ROUTE + (chunk - N_TOP) * COLS
        return (top_out if top else bot_out).at[:, pl.ds(pl.multiple_of(start, COLS), COLS)]

    def part(place, top, share=1):
        size = SHARD if top else SHARD // 2
        return (top_out if top else bot_out).at[:, pl.ds(pl.multiple_of(place * size, size), size // share)]

    def weights(route, chunk, rate, top):
        view = piece(places[0], route, chunk, top)

        def body(cols, carry):
            place = (route, chunk, slice(None), cols)
            value = master[place] - rate * mean[place]
            master[place] = value
            view[:, cols] = value.astype(BF16)
            return carry

        strips(body)

    def send(route, chunk, top):
        view = piece(places[0], route, chunk, top)
        kind = int(top)
        for axis in range(2):
            copy_to(view, view, places[1 + axis], side_send.at[axis, kind], side_recv.at[axis, route, chunk])
        copy_to(view, view, partner, partner_send.at[0, kind], partner_recv.at[0, kind])

    def own(chunk, rate, top):
        weights(0, chunk, rate, top)

        @pl.when(chunk > (0 if top else N_TOP))
        def _():
            send(1, chunk - 1, top)

        weights(1, chunk, rate, top)
        send(0, chunk, top)

        @pl.when(chunk == (N_TOP - 1 if top else N_CHUNK - 1))
        def _():
            send(1, chunk, top)

        return rate

    def hand_on(chunk, carry, top):
        kind = int(top)
        for route in range(2):
            for axis in range(2):
                view = piece(places[1 + axis], route, chunk, top)
                drain(view, side_recv.at[axis, route, chunk])
                if axis == route:
                    copy_to(view, view, places[2 - axis], forward_send.at[route, kind], corner_recv.at[route, chunk])
                copy_to(view, view, partner, partner_send.at[1 + axis, kind], partner_recv.at[1 + axis, kind])
        return carry

    def corner(chunk, carry, top):
        for route in range(2):
            view = piece(places[3], route, chunk, top)
            drain(view, corner_recv.at[route, chunk])
            copy_to(view, view, partner, partner_send.at[3, int(top)], partner_recv.at[3, int(top)])
        return carry

    def bottom_first(body, carry=0):
        carry = lax.fori_loop(N_TOP, N_CHUNK, functools.partial(body, top=False), carry)
        return lax.fori_loop(0, N_TOP, functools.partial(body, top=True), carry)

    lax.fori_loop(N_TOP, N_CHUNK, functools.partial(own, top=False), bot_rate())
    share_norms(1, update_rows(N_EARLY, N_TOP, top_squares))
    lax.fori_loop(0, N_TOP, functools.partial(own, top=True), top_rate())
    bottom_first(hand_on)
    bottom_first(corner)

    for top in (True, False):
        kind = int(top)
        for axis in range(2):
            drain(part(places[0], top), side_send.at[axis, kind])
            drain(part(places[0], top, 2), forward_send.at[axis, kind])
        for chip, (row_pos, col_pos) in enumerate(chips):
            drain(part(places[chip], top), partner_send.at[chip, kind])
            drain(part(data_index(row_pos, col_pos, flip(core)), top), partner_recv.at[chip, kind])
    drain(total_box.at[pl.ds(0, 15)], box_sem.at[0])
    for index in range(2):
        drain(norm_box.at[index, pl.ds(0, 15)], box_sem.at[2 + index])

    def first_sent(chunk, carry, top):
        for route in range(2):
            drain(landing(route, chunk, 2, 6, top), first_send.at[route, chunk])
        return carry

    sweep(first_sent)


def in_hbm(array):
    return pltpu.with_memory_space_constraint(array, pltpu.HBM)


def run_step(local_grads, master, moment_one, moment_two):
    dma = pltpu.SemaphoreType.DMA
    block = pltpu.VMEM((2, N_CHUNK, 8, COLS), F32)
    each = dma((2, N_CHUNK))
    return pl.pallas_call(
        step_kernel,
        out_shape=(pltpu.VMEM((8, 8 * SHARD), BF16), pltpu.VMEM((8, 4 * SHARD), BF16), block, block, block),
        in_specs=[pl.BlockSpec(memory_space=pltpu.HBM)] * 4,
        out_specs=(pl.BlockSpec(memory_space=pltpu.VMEM),) * 5,
        scratch_shapes=[
            block,
            pltpu.VMEM((16, 8, 128), F32),
            pltpu.VMEM((2, 16, 2, 8, 128), F32),
            each, each, each, each, dma((3, 2, N_CHUNK)),
            dma((2, 2)), dma((2, 2, N_CHUNK)), dma((2, 2)), each, dma((4, 2)), dma((4, 2)), dma((6,)),
            pltpu.SemaphoreType.REGULAR, pltpu.SemaphoreType.REGULAR,
        ],
        compiler_params=pltpu.CompilerParams(collective_id=0, has_side_effects=True, vmem_limit_bytes=STEP_LIMIT),
        name='lamb_step',
    )(in_hbm(local_grads), in_hbm(master), in_hbm(moment_one), in_hbm(moment_two))


def write_kernel(top, bot, master, one, two, params_out, master_out, one_out, two_out, sem):
    copies = []
    for place in range(8):
        copies.append((top.at[:, pl.ds(place * SHARD, SHARD)], params_out.at[pl.ds(0, 8), pl.ds(place * SHARD, SHARD)]))
        for half in range(2):
            copies.append((bot.at[pl.ds(4 * half, 4), pl.ds(place * TOP_ROUTE, TOP_ROUTE)], params_out.at[pl.ds(8, 4), pl.ds(place * SHARD + half * TOP_ROUTE, TOP_ROUTE)]))
    for block, array in ((master, master_out), (one, one_out), (two, two_out)):
        for route in range(2):
            for chunk in range(N_CHUNK):
                copies += [(src, dst) for dst, src in row_views(array, 0, route, chunk, block.at[route, chunk], chunk < N_TOP)]
    for index, (src, dst) in enumerate(copies):
        pltpu.make_async_copy(src, dst, sem.at[index]).start()
    for index, (src, dst) in enumerate(copies):
        pltpu.make_async_copy(src, dst, sem.at[index]).wait()


def write_out(*blocks):
    state = jax.ShapeDtypeStruct((12, SHARD), F32)
    return pl.pallas_call(
        write_kernel,
        out_shape=(jax.ShapeDtypeStruct((12, 8 * SHARD), BF16), state, state, state),
        in_specs=[pl.BlockSpec(memory_space=pltpu.VMEM)] * 5,
        out_specs=(pl.BlockSpec(memory_space=pltpu.HBM),) * 4,
        scratch_shapes=[pltpu.SemaphoreType.DMA((24 + 6 * (N_TOP + 2 * N_BOT),))],
        compiler_params=pltpu.CompilerParams(vmem_limit_bytes=WRITE_LIMIT),
        name='write_out',
    )(*[pltpu.with_memory_space_constraint(block, pltpu.VMEM) for block in blocks])


def solution(mesh):
    state_spec = P(None, ('model', 'data'))

    def device_step(local_grads, master, moment_one, moment_two):
        return write_out(*run_step(local_grads, master, moment_one, moment_two))

    return jax.shard_map(device_step, mesh=mesh, in_specs=(P('data', None, 'model'), state_spec, state_spec, state_spec), out_specs=(P(None, 'model'), state_spec, state_spec, state_spec), check_vma=False)
```

```python
import functools

import jax
import jax.numpy as jnp
from jax import lax
from jax.experimental import pallas as pl
from jax.experimental.pallas import tpu as pltpu
from jax.sharding import PartitionSpec as P

STEP = 4
LEARN_RATE = 0.08
BETA_ONE = 0.9
BETA_TWO = 0.999
EPSILON = 1e-6
WEIGHT_DECAY = 0.01
MAX_NORM = 1.0
CORR_ONE = 1.0 - BETA_ONE ** STEP
CORR_TWO = 1.0 - BETA_TWO ** STEP

MESH = pl.DeviceIdType.MESH
F32 = jnp.float32
BF16 = jnp.bfloat16

SHARD = 147456
COLS = 12288
TOP_ROUTE = SHARD // 2
BOT_ROUTE = SHARD // 4
N_TOP = TOP_ROUTE // COLS
N_BOT = BOT_ROUTE // COLS
N_CHUNK = N_TOP + N_BOT
STRIP = 1024
UPDATE_STRIP = 2048

TINY = 1.2e-38
MIB = 1024 * 1024
STEP_LIMIT = 9 * MIB
WRITE_LIMIT = STEP_LIMIT


def flip(value):
    return 1 - value


def my_place():
    data_pos = lax.axis_index('data')
    return data_pos // 4, lax.rem(data_pos // 2, 2), lax.rem(data_pos, 2)


def data_index(pos_y, pos_x, core):
    return (pos_y * 2 + pos_x) * 2 + core


def others():
    mine = lax.axis_index('model') * 8 + lax.axis_index('data')
    for step in range(1, 16):
        other = lax.rem(mine + step, 16)
        yield other // 8, lax.rem(other, 8)


def drain(ref, sem):
    pltpu.make_async_copy(ref, ref, sem).wait()


def row_views(array, shard, route, chunk, block, top):
    if top:
        start = shard * SHARD + route * TOP_ROUTE + chunk * COLS
        return [(array.at[pl.ds(0, 8), pl.ds(pl.multiple_of(start, COLS), COLS)], block)]
    views = []
    for half in range(2):
        start = shard * SHARD + half * TOP_ROUTE + route * BOT_ROUTE + (chunk - N_TOP) * COLS
        views.append((array.at[pl.ds(8, 4), pl.ds(pl.multiple_of(start, COLS), COLS)], block.at[pl.ds(4 * half, 4)]))
    return views


def sweep(body, carry=0):
    carry = lax.fori_loop(0, N_TOP, functools.partial(body, top=True), carry)
    return lax.fori_loop(N_TOP, N_CHUNK, functools.partial(body, top=False), carry)


def strips(body, carry=0, width=STRIP):
    def step(strip, carry):
        return body(pl.ds(pl.multiple_of(strip * width, width), width), carry)

    return lax.fori_loop(0, COLS // width, step, carry)


def fold(total, values):
    for tile in range(values.shape[1] // 128):
        total = total + values[:, tile * 128:(tile + 1) * 128]
    return total


def step_kernel(
    grads, master_in, one_in, two_in,
    top_out, bot_out, master, one, two,
    mean, total_box, norm_box,
    first_send, first_recv, second_send, second_recv, load_sem,
    side_send, side_recv, forward_send, corner_recv, partner_send, partner_recv, box_sem, seen, known,
):
    pos_y, pos_x, core = my_place()
    model_pos = lax.axis_index('model')
    mine = model_pos * 8 + lax.axis_index('data')
    grad = grads.at[0]
    sent, got = master, two
    chips = ((pos_y, pos_x), (pos_y, flip(pos_x)), (flip(pos_y), pos_x), (flip(pos_y), flip(pos_x)))
    places = [data_index(row, col, core) for row, col in chips]
    partner = data_index(pos_y, pos_x, flip(core))

    def copy_to(src, dst, place, send_sem, recv_sem):
        pltpu.make_async_remote_copy(src_ref=src, dst_ref=dst, send_sem=send_sem, recv_sem=recv_sem, device_id=(model_pos, place), device_id_type=MESH).start()

    def landing(route, chunk, block, count, top):
        if top:
            start = ((route * N_TOP + chunk) * 8 + block) * COLS
        else:
            start = ((route * N_BOT + chunk - N_TOP) * 8 + block) * COLS
        return (top_out if top else bot_out).at[:, pl.ds(pl.multiple_of(start, COLS), count * COLS)]

    def wanted(route, row, col, far):
        return (lax.rem(row + far, 2), col) if route == 0 else (row, lax.rem(col + far, 2))

    def local(chunk, carry, top):
        for route in range(2):
            for far in range(2):
                shard = data_index(*wanted(route, pos_y, pos_x, far), core)
                for src, dst in row_views(grad, shard, route, chunk, landing(route, chunk, far, 1, top), top):
                    pltpu.make_async_copy(src, dst, first_recv.at[route, chunk]).start()
        return carry

    def remote(chunk, carry, top):
        for far in range(2):
            for other in range(2):
                for route in range(2):
                    row, col = chips[1 + route]
                    to_core = lax.rem(core + other, 2)
                    shard = data_index(*wanted(route, row, col, far), to_core)
                    for src, dst in row_views(grad, shard, route, chunk, landing(route, chunk, 4 + 2 * other + far, 1, top), top):
                        copy_to(src, dst, data_index(row, col, to_core), first_send.at[route, chunk], first_recv.at[route, chunk])
            for route in range(2):
                shard = data_index(*wanted(route, pos_y, pos_x, far), flip(core))
                for src, dst in row_views(grad, shard, route, chunk, landing(route, chunk, 2 + far, 1, top), top):
                    copy_to(src, dst, partner, first_send.at[route, chunk], first_recv.at[route, chunk])
        return carry

    def load(which, array, block, route, chunk, top):
        for src, dst in row_views(array, 0, route, chunk, block.at[route, chunk], top):
            pltpu.make_async_copy(src, dst, load_sem.at[which, route, chunk]).start()

    next_to = [(model_pos, place) for chip in (1, 2) for place in (places[chip], data_index(*chips[chip], flip(core)))] + [(model_pos, partner), (flip(model_pos), places[0])]

    def tell(sem, devices):
        for device in devices:
            pl.semaphore_signal(sem, inc=1, device_id=device, device_id_type=MESH)

    sweep(local)
    barrier = pltpu.get_barrier_semaphore()
    tell(barrier, next_to)
    pl.semaphore_wait(barrier, len(next_to))
    sweep(remote)
    tell(seen, next_to)

    def load_one(chunk, carry, top):
        for route in range(2):
            load(1, one_in, one, route, chunk, top)
        return carry

    sweep(load_one)
    pl.semaphore_wait(seen, len(next_to))
    tell(known, next_to[-1:])

    def second(route, chunk):
        copy_to(sent.at[route, chunk], got.at[route, chunk], places[2 - route], second_send.at[route, chunk], second_recv.at[route, chunk])

    def add_four(route, chunk, top):
        drain(landing(route, chunk, 0, 8, top), first_recv.at[route, chunk])

        def body(cols, carry):
            for far, target in ((0, mean), (1, sent)):
                parts = [landing(route, chunk, 2 * source + far, 1, top)[:, cols].astype(F32) for source in range(4)]
                target[route, chunk, :, cols] = (parts[0] + parts[1]) + (parts[2] + parts[3])
            return carry

        strips(body)

    def first_sums(chunk, carry, top):
        add_four(0, chunk, top)

        @pl.when(chunk > 0)
        def _():
            second(1, chunk - 1)

        add_four(1, chunk, top)
        second(0, chunk)
        return carry

    sweep(first_sums)
    second(1, N_CHUNK - 1)

    def finish(chunk, squares, top):
        for route in range(2):
            drain(got.at[route, chunk], second_recv.at[route, chunk])

            def body(cols, total):
                value = (mean[route, chunk, :, cols] + got[route, chunk, :, cols]) * 0.125
                mean[route, chunk, :, cols] = value
                return fold(total, value * value)

            squares = strips(body, squares)
            load(2, two_in, two, route, chunk, top)
            drain(sent.at[route, chunk], second_send.at[route, chunk])
            load(0, master_in, master, route, chunk, top)
        return squares

    def share_all(box, send_sem, recv_sem):
        for device in others():
            pltpu.make_async_remote_copy(src_ref=box.at[mine], dst_ref=box.at[mine], send_sem=send_sem, recv_sem=recv_sem, device_id=device, device_id_type=MESH).start()

    total_box[mine] = sweep(finish, jnp.zeros((8, 128), F32))
    pl.semaphore_wait(known, 1)
    share_all(total_box, box_sem.at[0], box_sem.at[1])
    drain(total_box.at[pl.ds(0, 15)], box_sem.at[1])
    total = jnp.sum(jnp.sum(total_box[...], axis=0), keepdims=True)
    clip = jnp.minimum(1.0, MAX_NORM / jnp.sqrt(total))
    one_scale, two_scale = clip * (1.0 - BETA_ONE), clip * (1.0 - BETA_TWO) ** 0.5

    def update(route, chunk, carry):
        for which, block in enumerate((master, one, two)):
            drain(block.at[route, chunk], load_sem.at[which, route, chunk])

        def body(cols, carry):
            place = (route, chunk, slice(None), cols)
            weight = master[place]
            value = mean[place]
            new_one = BETA_ONE * one[place] + one_scale * value
            change = two_scale * value
            new_two = BETA_TWO * two[place] + change * change
            one[place] = new_one
            two[place] = new_two
            floor = jnp.maximum(new_two, TINY)
            root = floor * lax.rsqrt(floor)
            direction = (new_one * (CORR_TWO ** 0.5 / CORR_ONE)) / (root + EPSILON * CORR_TWO ** 0.5) + WEIGHT_DECAY * weight
            mean[place] = direction
            return fold(carry[0], weight * weight), fold(carry[1], direction * direction)

        return strips(body, carry, UPDATE_STRIP)

    def update_rows(low, high):
        zero = jnp.zeros((8, 128), F32)
        return lax.fori_loop(low, high, lambda chunk, carry: update(1, chunk, update(0, chunk, carry)), (zero, zero))

    def share_norms(index, squares):
        box = norm_box.at[index]
        box[mine, 0], box[mine, 1] = squares
        share_all(box, box_sem.at[2 + index], box_sem.at[4 + index])

    def row_sums(index):
        box = norm_box.at[index]
        drain(box.at[pl.ds(0, 15)], box_sem.at[4 + index])
        return jnp.sum(jnp.sum(box[...], axis=0), axis=2, keepdims=True)

    def bot_rate():
        sums = jnp.sqrt(jnp.sum(row_sums(0), axis=1, keepdims=True))
        return LEARN_RATE * (sums[0] / sums[1]) + jnp.zeros((8, 1), F32)

    def top_rate():
        sums = row_sums(1)
        row = lax.broadcasted_iota(jnp.int32, (8, 1), 0)

        def norms(values):
            pieces = [jnp.sum(jnp.where(mask, values, 0.0), axis=0, keepdims=True) for mask in (row < 3, row == 3, row > 3)]
            return jnp.sqrt(jnp.where(row < 3, pieces[0], jnp.where(row == 3, pieces[1], pieces[2])))

        return LEARN_RATE * (norms(sums[0]) / norms(sums[1]))

    share_norms(0, update_rows(N_TOP, N_CHUNK))
    share_norms(1, update_rows(0, N_TOP))

    def piece(place, route, chunk, top):
        if top:
            start = place * SHARD + route * TOP_ROUTE + chunk * COLS
        else:
            start = place * (SHARD // 2) + route * BOT_ROUTE + (chunk - N_TOP) * COLS
        return (top_out if top else bot_out).at[:, pl.ds(pl.multiple_of(start, COLS), COLS)]

    def part(place, top, share=1):
        size = SHARD if top else SHARD // 2
        return (top_out if top else bot_out).at[:, pl.ds(pl.multiple_of(place * size, size), size // share)]

    def weights(route, chunk, rate, top):
        view = piece(places[0], route, chunk, top)

        def body(cols, carry):
            place = (route, chunk, slice(None), cols)
            value = master[place] - rate * mean[place]
            master[place] = value
            view[:, cols] = value.astype(BF16)
            return carry

        strips(body)

    def send(route, chunk, top):
        view = piece(places[0], route, chunk, top)
        kind = int(top)
        for axis in range(2):
            copy_to(view, view, places[1 + axis], side_send.at[axis, kind], side_recv.at[axis, route, chunk])
        copy_to(view, view, partner, partner_send.at[0, kind], partner_recv.at[0, kind])

    def own(chunk, rate, top):
        weights(0, chunk, rate, top)

        @pl.when(chunk > (0 if top else N_TOP))
        def _():
            send(1, chunk - 1, top)

        weights(1, chunk, rate, top)
        send(0, chunk, top)

        @pl.when(chunk == (N_TOP - 1 if top else N_CHUNK - 1))
        def _():
            send(1, chunk, top)

        return rate

    def hand_on(chunk, carry, top):
        kind = int(top)
        for route in range(2):
            for axis in range(2):
                view = piece(places[1 + axis], route, chunk, top)
                drain(view, side_recv.at[axis, route, chunk])
                if axis == route:
                    copy_to(view, view, places[2 - axis], forward_send.at[route, kind], corner_recv.at[route, chunk])
                copy_to(view, view, partner, partner_send.at[1 + axis, kind], partner_recv.at[1 + axis, kind])
        return carry

    def corner(chunk, carry, top):
        for route in range(2):
            view = piece(places[3], route, chunk, top)
            drain(view, corner_recv.at[route, chunk])
            copy_to(view, view, partner, partner_send.at[3, int(top)], partner_recv.at[3, int(top)])
        return carry

    def bottom_first(body, carry=0):
        carry = lax.fori_loop(N_TOP, N_CHUNK, functools.partial(body, top=False), carry)
        return lax.fori_loop(0, N_TOP, functools.partial(body, top=True), carry)

    lax.fori_loop(N_TOP, N_CHUNK, functools.partial(own, top=False), bot_rate())
    lax.fori_loop(0, N_TOP, functools.partial(own, top=True), top_rate())
    bottom_first(hand_on)
    bottom_first(corner)

    for top in (True, False):
        kind = int(top)
        for axis in range(2):
            drain(part(places[0], top), side_send.at[axis, kind])
            drain(part(places[0], top, 2), forward_send.at[axis, kind])
        for chip, (row_pos, col_pos) in enumerate(chips):
            drain(part(places[chip], top), partner_send.at[chip, kind])
            drain(part(data_index(row_pos, col_pos, flip(core)), top), partner_recv.at[chip, kind])
    drain(total_box.at[pl.ds(0, 15)], box_sem.at[0])
    for index in range(2):
        drain(norm_box.at[index, pl.ds(0, 15)], box_sem.at[2 + index])

    def first_sent(chunk, carry, top):
        for route in range(2):
            drain(landing(route, chunk, 2, 6, top), first_send.at[route, chunk])
        return carry

    sweep(first_sent)


def in_hbm(array):
    return pltpu.with_memory_space_constraint(array, pltpu.HBM)


def run_step(local_grads, master, moment_one, moment_two):
    dma = pltpu.SemaphoreType.DMA
    block = pltpu.VMEM((2, N_CHUNK, 8, COLS), F32)
    each = dma((2, N_CHUNK))
    return pl.pallas_call(
        step_kernel,
        out_shape=(pltpu.VMEM((8, 8 * SHARD), BF16), pltpu.VMEM((8, 4 * SHARD), BF16), block, block, block),
        in_specs=[pl.BlockSpec(memory_space=pltpu.HBM)] * 4,
        out_specs=(pl.BlockSpec(memory_space=pltpu.VMEM),) * 5,
        scratch_shapes=[
            block,
            pltpu.VMEM((16, 8, 128), F32),
            pltpu.VMEM((2, 16, 2, 8, 128), F32),
            each, each, each, each, dma((3, 2, N_CHUNK)),
            dma((2, 2)), dma((2, 2, N_CHUNK)), dma((2, 2)), each, dma((4, 2)), dma((4, 2)), dma((6,)),
            pltpu.SemaphoreType.REGULAR, pltpu.SemaphoreType.REGULAR,
        ],
        compiler_params=pltpu.CompilerParams(collective_id=0, has_side_effects=True, vmem_limit_bytes=STEP_LIMIT),
        name='lamb_step',
    )(in_hbm(local_grads), in_hbm(master), in_hbm(moment_one), in_hbm(moment_two))


def write_kernel(top, bot, master, one, two, params_out, master_out, one_out, two_out, sem):
    copies = []
    for place in range(8):
        copies.append((top.at[:, pl.ds(place * SHARD, SHARD)], params_out.at[pl.ds(0, 8), pl.ds(place * SHARD, SHARD)]))
        for half in range(2):
            copies.append((bot.at[pl.ds(4 * half, 4), pl.ds(place * TOP_ROUTE, TOP_ROUTE)], params_out.at[pl.ds(8, 4), pl.ds(place * SHARD + half * TOP_ROUTE, TOP_ROUTE)]))
    for block, array in ((master, master_out), (one, one_out), (two, two_out)):
        for route in range(2):
            for chunk in range(N_CHUNK):
                copies += [(src, dst) for dst, src in row_views(array, 0, route, chunk, block.at[route, chunk], chunk < N_TOP)]
    for index, (src, dst) in enumerate(copies):
        pltpu.make_async_copy(src, dst, sem.at[index]).start()
    for index, (src, dst) in enumerate(copies):
        pltpu.make_async_copy(src, dst, sem.at[index]).wait()


def write_out(*blocks):
    state = jax.ShapeDtypeStruct((12, SHARD), F32)
    return pl.pallas_call(
        write_kernel,
        out_shape=(jax.ShapeDtypeStruct((12, 8 * SHARD), BF16), state, state, state),
        in_specs=[pl.BlockSpec(memory_space=pltpu.VMEM)] * 5,
        out_specs=(pl.BlockSpec(memory_space=pltpu.HBM),) * 4,
        scratch_shapes=[pltpu.SemaphoreType.DMA((24 + 6 * (N_TOP + 2 * N_BOT),))],
        compiler_params=pltpu.CompilerParams(vmem_limit_bytes=WRITE_LIMIT),
        name='write_out',
    )(*[pltpu.with_memory_space_constraint(block, pltpu.VMEM) for block in blocks])


def solution(mesh):
    state_spec = P(None, ('model', 'data'))

    def device_step(local_grads, master, moment_one, moment_two):
        return write_out(*run_step(local_grads, master, moment_one, moment_two))

    return jax.shard_map(device_step, mesh=mesh, in_specs=(P('data', None, 'model'), state_spec, state_spec, state_spec), out_specs=(P(None, 'model'), state_spec, state_spec, state_spec), check_vma=False)
```

```python
import functools

import jax
import jax.numpy as jnp
from jax import lax
from jax.experimental import pallas as pl
from jax.experimental.pallas import tpu as pltpu
from jax.sharding import PartitionSpec as P

STEP = 4
LEARN_RATE = 0.08
BETA_ONE = 0.9
BETA_TWO = 0.999
EPSILON = 1e-6
WEIGHT_DECAY = 0.01
MAX_NORM = 1.0
CORR_ONE = 1.0 - BETA_ONE ** STEP
CORR_TWO = 1.0 - BETA_TWO ** STEP

MESH = pl.DeviceIdType.MESH
F32 = jnp.float32
BF16 = jnp.bfloat16

SHARD = 147456
COLS = 12288
TOP_ROUTE = SHARD // 2
BOT_ROUTE = SHARD // 4
N_TOP = TOP_ROUTE // COLS
N_BOT = BOT_ROUTE // COLS
N_CHUNK = N_TOP + N_BOT
STRIP = 1024
UPDATE_STRIP = 2048

TINY = 1.2e-38
MIB = 1024 * 1024
STEP_LIMIT = 15 * MIB
WRITE_LIMIT = STEP_LIMIT


def flip(value):
    return 1 - value


def my_place():
    data_pos = lax.axis_index('data')
    return data_pos // 4, lax.rem(data_pos // 2, 2), lax.rem(data_pos, 2)


def data_index(pos_y, pos_x, core):
    return (pos_y * 2 + pos_x) * 2 + core


def others():
    mine = lax.axis_index('model') * 8 + lax.axis_index('data')
    for step in range(1, 16):
        other = lax.rem(mine + step, 16)
        yield other // 8, lax.rem(other, 8)


def drain(ref, sem):
    pltpu.make_async_copy(ref, ref, sem).wait()


def row_views(array, shard, route, chunk, block, top):
    if top:
        start = shard * SHARD + route * TOP_ROUTE + chunk * COLS
        return [(array.at[pl.ds(0, 8), pl.ds(pl.multiple_of(start, COLS), COLS)], block)]
    views = []
    for half in range(2):
        start = shard * SHARD + half * TOP_ROUTE + route * BOT_ROUTE + (chunk - N_TOP) * COLS
        views.append((array.at[pl.ds(8, 4), pl.ds(pl.multiple_of(start, COLS), COLS)], block.at[pl.ds(4 * half, 4)]))
    return views


def sweep(body, carry=0):
    carry = lax.fori_loop(0, N_TOP, functools.partial(body, top=True), carry)
    return lax.fori_loop(N_TOP, N_CHUNK, functools.partial(body, top=False), carry)


def strips(body, carry=0, width=STRIP):
    def step(strip, carry):
        return body(pl.ds(pl.multiple_of(strip * width, width), width), carry)

    return lax.fori_loop(0, COLS // width, step, carry)


def fold(total, values):
    for tile in range(values.shape[1] // 128):
        total = total + values[:, tile * 128:(tile + 1) * 128]
    return total


def step_kernel(
    grads, master_in, one_in, two_in,
    top_out, bot_out, master, one, two,
    mean, sent, total_box, norm_box,
    near_recv, corner_recv, first_send, second_send, load_sem, side_send, forward_send, partner_send, partner_recv, box_sem, seen, known,
):
    pos_y, pos_x, core = my_place()
    model_pos = lax.axis_index('model')
    mine = model_pos * 8 + lax.axis_index('data')
    grad = grads.at[0]
    got = two
    first_recv, second_recv = near_recv.at[0], near_recv.at[1]
    chips = ((pos_y, pos_x), (pos_y, flip(pos_x)), (flip(pos_y), pos_x), (flip(pos_y), flip(pos_x)))
    places = [data_index(row, col, core) for row, col in chips]
    partner = data_index(pos_y, pos_x, flip(core))

    def copy_to(src, dst, place, send_sem, recv_sem):
        pltpu.make_async_remote_copy(src_ref=src, dst_ref=dst, send_sem=send_sem, recv_sem=recv_sem, device_id=(model_pos, place), device_id_type=MESH).start()

    def landing(route, chunk, block, count, top):
        if top:
            start = ((route * N_TOP + chunk) * 8 + block) * COLS
        else:
            start = ((route * N_BOT + chunk - N_TOP) * 8 + block) * COLS
        return (top_out if top else bot_out).at[:, pl.ds(pl.multiple_of(start, COLS), count * COLS)]

    def wanted(route, row, col, far):
        return (lax.rem(row + far, 2), col) if route == 0 else (row, lax.rem(col + far, 2))

    def local(chunk, carry, top):
        for route in range(2):
            for far in range(2):
                shard = data_index(*wanted(route, pos_y, pos_x, far), core)
                for src, dst in row_views(grad, shard, route, chunk, landing(route, chunk, far, 1, top), top):
                    pltpu.make_async_copy(src, dst, first_recv.at[route, chunk]).start()
        return carry

    def remote(chunk, carry, top):
        for far in range(2):
            for other in range(2):
                for route in range(2):
                    row, col = chips[1 + route]
                    to_core = lax.rem(core + other, 2)
                    shard = data_index(*wanted(route, row, col, far), to_core)
                    for src, dst in row_views(grad, shard, route, chunk, landing(route, chunk, 4 + 2 * other + far, 1, top), top):
                        copy_to(src, dst, data_index(row, col, to_core), first_send.at[int(top)], first_recv.at[route, chunk])
            for route in range(2):
                shard = data_index(*wanted(route, pos_y, pos_x, far), flip(core))
                for src, dst in row_views(grad, shard, route, chunk, landing(route, chunk, 2 + far, 1, top), top):
                    copy_to(src, dst, partner, first_send.at[int(top)], first_recv.at[route, chunk])
        return carry

    def load(array, block, sem, route, chunk, top):
        for src, dst in row_views(array, 0, route, chunk, block.at[route, chunk], top):
            pltpu.make_async_copy(src, dst, sem).start()

    next_to = [(model_pos, place) for chip in (1, 2) for place in (places[chip], data_index(*chips[chip], flip(core)))] + [(model_pos, partner), (flip(model_pos), places[0])]

    def tell(sem, devices):
        for device in devices:
            pl.semaphore_signal(sem, inc=1, device_id=device, device_id_type=MESH)

    barrier = pltpu.get_barrier_semaphore()
    tell(barrier, next_to)
    sweep(local)
    pl.semaphore_wait(barrier, len(next_to))
    sweep(remote)
    tell(seen, next_to)

    def load_state(chunk, carry, top):
        for route in range(2):
            load(master_in, master, load_sem.at[0], route, chunk, top)
            load(one_in, one, load_sem.at[1], route, chunk, top)
        return carry

    sweep(load_state)
    pl.semaphore_wait(seen, len(next_to))
    tell(known, next_to[-1:])

    def second(route, chunk):
        copy_to(sent.at[route, chunk], got.at[route, chunk], places[2 - route], second_send, second_recv.at[route, chunk])

    def add_four(route, chunk, squares, top):
        drain(landing(route, chunk, 0, 8, top), first_recv.at[route, chunk])

        def body(cols, total):
            for far, target in ((0, mean), (1, sent)):
                parts = [landing(route, chunk, 2 * source + far, 1, top)[:, cols].astype(F32) for source in range(4)]
                target[route, chunk, :, cols] = (parts[0] + parts[1]) + (parts[2] + parts[3])
            weight = master[route, chunk, :, cols]
            return fold(total, weight * weight)

        return strips(body, squares)

    def first_sums(chunk, squares, top):
        squares = add_four(0, chunk, squares, top)

        @pl.when(chunk > 0)
        def _():
            second(1, chunk - 1)

        squares = add_four(1, chunk, squares, top)
        second(0, chunk)
        return squares

    drain(master, load_sem.at[0])
    zero = jnp.zeros((8, 128), F32)
    top_squares = lax.fori_loop(0, N_TOP, functools.partial(first_sums, top=True), zero)
    bot_squares = lax.fori_loop(N_TOP, N_CHUNK, functools.partial(first_sums, top=False), zero)
    second(1, N_CHUNK - 1)

    def finish(chunk, squares, top):
        for route in range(2):
            drain(got.at[route, chunk], second_recv.at[route, chunk])

            def body(cols, total):
                value = (mean[route, chunk, :, cols] + got[route, chunk, :, cols]) * 0.125
                mean[route, chunk, :, cols] = value
                return fold(total, value * value)

            squares = strips(body, squares)
            load(two_in, two, load_sem.at[2 + int(top)], route, chunk, top)
        return squares

    def share_all(box, send_sem, recv_sem):
        for device in others():
            pltpu.make_async_remote_copy(src_ref=box.at[mine], dst_ref=box.at[mine], send_sem=send_sem, recv_sem=recv_sem, device_id=device, device_id_type=MESH).start()

    total_box[mine] = sweep(finish, zero)
    pl.semaphore_wait(known, 1)
    share_all(total_box, box_sem.at[0], box_sem.at[1])
    drain(total_box.at[pl.ds(0, 15)], box_sem.at[1])
    total = jnp.sum(jnp.sum(total_box[...], axis=0), keepdims=True)
    clip = jnp.minimum(1.0, MAX_NORM / jnp.sqrt(total))
    one_scale, two_scale = clip * (1.0 - BETA_ONE), clip * (1.0 - BETA_TWO) ** 0.5

    def update(route, chunk, carry):
        def body(cols, total):
            place = (route, chunk, slice(None), cols)
            weight = master[place]
            value = mean[place]
            new_one = BETA_ONE * one[place] + one_scale * value
            change = two_scale * value
            new_two = BETA_TWO * two[place] + change * change
            one[place] = new_one
            two[place] = new_two
            floor = jnp.maximum(new_two, TINY)
            root = floor * lax.rsqrt(floor)
            direction = (new_one * (CORR_TWO ** 0.5 / CORR_ONE)) / (root + EPSILON * CORR_TWO ** 0.5) + WEIGHT_DECAY * weight
            mean[place] = direction
            return fold(total, direction * direction)

        return strips(body, carry, UPDATE_STRIP)

    def update_rows(index, low, high, weight_squares):
        drain(two.at[:, pl.ds(low, high - low)], load_sem.at[2 + index])
        box = norm_box.at[index]
        box[mine, 0] = weight_squares
        box[mine, 1] = lax.fori_loop(low, high, lambda chunk, total: update(1, chunk, update(0, chunk, total)), zero)
        share_all(box, box_sem.at[2 + index], box_sem.at[4 + index])

    def row_sums(index):
        box = norm_box.at[index]
        drain(box.at[pl.ds(0, 15)], box_sem.at[4 + index])
        return jnp.sum(jnp.sum(box[...], axis=0), axis=2, keepdims=True)

    def bot_rate():
        sums = jnp.sqrt(jnp.sum(row_sums(0), axis=1, keepdims=True))
        return LEARN_RATE * (sums[0] / sums[1]) + jnp.zeros((8, 1), F32)

    def top_rate():
        sums = row_sums(1)
        row = lax.broadcasted_iota(jnp.int32, (8, 1), 0)

        def norms(values):
            pieces = [jnp.sum(jnp.where(mask, values, 0.0), axis=0, keepdims=True) for mask in (row < 3, row == 3, row > 3)]
            return jnp.sqrt(jnp.where(row < 3, pieces[0], jnp.where(row == 3, pieces[1], pieces[2])))

        return LEARN_RATE * (norms(sums[0]) / norms(sums[1]))

    drain(one, load_sem.at[1])
    update_rows(0, N_TOP, N_CHUNK, bot_squares)
    update_rows(1, 0, N_TOP, top_squares)

    def piece(place, route, chunk, top):
        if top:
            start = place * SHARD + route * TOP_ROUTE + chunk * COLS
        else:
            start = place * (SHARD // 2) + route * BOT_ROUTE + (chunk - N_TOP) * COLS
        return (top_out if top else bot_out).at[:, pl.ds(pl.multiple_of(start, COLS), COLS)]

    def part(place, top, share=1):
        size = SHARD if top else SHARD // 2
        return (top_out if top else bot_out).at[:, pl.ds(pl.multiple_of(place * size, size), size // share)]

    def weights(route, chunk, rate, top):
        view = piece(places[0], route, chunk, top)

        def body(cols, carry):
            place = (route, chunk, slice(None), cols)
            value = master[place] - rate * mean[place]
            master[place] = value
            view[:, cols] = value.astype(BF16)
            return carry

        strips(body)

    def send(route, chunk, top):
        view = piece(places[0], route, chunk, top)
        kind = int(top)
        for axis in range(2):
            copy_to(view, view, places[1 + axis], side_send.at[axis, kind], near_recv.at[axis, route, chunk])
        copy_to(view, view, partner, partner_send.at[0, kind], partner_recv.at[0, kind])

    def own(chunk, rate, top):
        weights(0, chunk, rate, top)

        @pl.when(chunk > (0 if top else N_TOP))
        def _():
            send(1, chunk - 1, top)

        weights(1, chunk, rate, top)
        send(0, chunk, top)

        @pl.when(chunk == (N_TOP - 1 if top else N_CHUNK - 1))
        def _():
            send(1, chunk, top)

        return rate

    def hand_on(chunk, carry, top):
        kind = int(top)
        for route in range(2):
            for axis in range(2):
                view = piece(places[1 + axis], route, chunk, top)
                drain(view, near_recv.at[axis, route, chunk])
                if axis == route:
                    copy_to(view, view, places[2 - axis], forward_send.at[route, kind], corner_recv.at[route, chunk])
                copy_to(view, view, partner, partner_send.at[1 + axis, kind], partner_recv.at[1 + axis, kind])
        return carry

    def corner(chunk, carry, top):
        for route in range(2):
            view = piece(places[3], route, chunk, top)
            drain(view, corner_recv.at[route, chunk])
            copy_to(view, view, partner, partner_send.at[3, int(top)], partner_recv.at[3, int(top)])
        return carry

    def bottom_first(body, carry=0):
        carry = lax.fori_loop(N_TOP, N_CHUNK, functools.partial(body, top=False), carry)
        return lax.fori_loop(0, N_TOP, functools.partial(body, top=True), carry)

    lax.fori_loop(N_TOP, N_CHUNK, functools.partial(own, top=False), bot_rate())
    lax.fori_loop(0, N_TOP, functools.partial(own, top=True), top_rate())
    bottom_first(hand_on)
    bottom_first(corner)

    for top in (True, False):
        kind = int(top)
        for axis in range(2):
            drain(part(places[0], top), side_send.at[axis, kind])
            drain(part(places[0], top, 2), forward_send.at[axis, kind])
        for chip, (row_pos, col_pos) in enumerate(chips):
            drain(part(places[chip], top), partner_send.at[chip, kind])
            drain(part(data_index(row_pos, col_pos, flip(core)), top), partner_recv.at[chip, kind])
    drain(total_box.at[pl.ds(0, 15)], box_sem.at[0])
    for index in range(2):
        drain(norm_box.at[index, pl.ds(0, 15)], box_sem.at[2 + index])

    drain(top_out.at[:, pl.ds(0, 6 * SHARD)], first_send.at[1])
    drain(bot_out.at[:, pl.ds(0, 3 * SHARD)], first_send.at[0])
    drain(sent, second_send)


def in_hbm(array):
    return pltpu.with_memory_space_constraint(array, pltpu.HBM)


def run_step(local_grads, master, moment_one, moment_two):
    dma = pltpu.SemaphoreType.DMA
    block = pltpu.VMEM((2, N_CHUNK, 8, COLS), F32)
    return pl.pallas_call(
        step_kernel,
        out_shape=(pltpu.VMEM((8, 8 * SHARD), BF16), pltpu.VMEM((8, 4 * SHARD), BF16), block, block, block),
        in_specs=[pl.BlockSpec(memory_space=pltpu.HBM)] * 4,
        out_specs=(pl.BlockSpec(memory_space=pltpu.VMEM),) * 5,
        scratch_shapes=[
            block, block,
            pltpu.VMEM((16, 8, 128), F32),
            pltpu.VMEM((2, 16, 2, 8, 128), F32),
            dma((2, 2, N_CHUNK)), dma((2, N_CHUNK)), dma((2,)), dma, dma((4,)), dma((2, 2)), dma((2, 2)), dma((4, 2)), dma((4, 2)), dma((6,)),
            pltpu.SemaphoreType.REGULAR, pltpu.SemaphoreType.REGULAR,
        ],
        compiler_params=pltpu.CompilerParams(collective_id=0, has_side_effects=True, vmem_limit_bytes=STEP_LIMIT),
        name='lamb_step',
    )(in_hbm(local_grads), in_hbm(master), in_hbm(moment_one), in_hbm(moment_two))


def write_kernel(top, bot, master, one, two, params_out, master_out, one_out, two_out, sem):
    copies = []
    for place in range(8):
        copies.append((top.at[:, pl.ds(place * SHARD, SHARD)], params_out.at[pl.ds(0, 8), pl.ds(place * SHARD, SHARD)]))
        for half in range(2):
            copies.append((bot.at[pl.ds(4 * half, 4), pl.ds(place * TOP_ROUTE, TOP_ROUTE)], params_out.at[pl.ds(8, 4), pl.ds(place * SHARD + half * TOP_ROUTE, TOP_ROUTE)]))
    for block, array in ((master, master_out), (one, one_out), (two, two_out)):
        for route in range(2):
            for chunk in range(N_CHUNK):
                copies += [(src, dst) for dst, src in row_views(array, 0, route, chunk, block.at[route, chunk], chunk < N_TOP)]
    for src, dst in copies:
        pltpu.make_async_copy(src, dst, sem).start()
    for src, dst in copies:
        pltpu.make_async_copy(src, dst, sem).wait()


def write_out(*blocks):
    state = jax.ShapeDtypeStruct((12, SHARD), F32)
    return pl.pallas_call(
        write_kernel,
        out_shape=(jax.ShapeDtypeStruct((12, 8 * SHARD), BF16), state, state, state),
        in_specs=[pl.BlockSpec(memory_space=pltpu.VMEM)] * 5,
        out_specs=(pl.BlockSpec(memory_space=pltpu.HBM),) * 4,
        scratch_shapes=[pltpu.SemaphoreType.DMA],
        compiler_params=pltpu.CompilerParams(vmem_limit_bytes=WRITE_LIMIT),
        name='write_out',
    )(*[pltpu.with_memory_space_constraint(block, pltpu.VMEM) for block in blocks])


def solution(mesh):
    state_spec = P(None, ('model', 'data'))

    def device_step(local_grads, master, moment_one, moment_two):
        return write_out(*run_step(local_grads, master, moment_one, moment_two))

    return jax.shard_map(device_step, mesh=mesh, in_specs=(P('data', None, 'model'), state_spec, state_spec, state_spec), out_specs=(P(None, 'model'), state_spec, state_spec, state_spec), check_vma=False)
```

```python
import functools

import jax
import jax.numpy as jnp
from jax import lax
from jax.experimental import pallas as pl
from jax.experimental.pallas import tpu as pltpu
from jax.sharding import PartitionSpec as P

STEP = 4
LEARN_RATE = 0.08
BETA_ONE = 0.9
BETA_TWO = 0.999
EPSILON = 1e-6
WEIGHT_DECAY = 0.01
MAX_NORM = 1.0
CORR_ONE = 1.0 - BETA_ONE ** STEP
CORR_TWO = 1.0 - BETA_TWO ** STEP

MESH = pl.DeviceIdType.MESH
F32 = jnp.float32
BF16 = jnp.bfloat16

SHARD = 147456
COLS = 12288
TOP_ROUTE = SHARD // 2
BOT_ROUTE = SHARD // 4
N_TOP = TOP_ROUTE // COLS
N_BOT = BOT_ROUTE // COLS
N_CHUNK = N_TOP + N_BOT
STRIP = 1024
UPDATE_STRIP = 2048

TINY = 1.2e-38
MIB = 1024 * 1024
STEP_LIMIT = 15 * MIB
WRITE_LIMIT = STEP_LIMIT


def flip(value):
    return 1 - value


def my_place():
    data_pos = lax.axis_index('data')
    return data_pos // 4, lax.rem(data_pos // 2, 2), lax.rem(data_pos, 2)


def data_index(pos_y, pos_x, core):
    return (pos_y * 2 + pos_x) * 2 + core


def drain(ref, sem):
    pltpu.make_async_copy(ref, ref, sem).wait()


def row_views(array, shard, route, chunk, block, top):
    if top:
        start = shard * SHARD + route * TOP_ROUTE + chunk * COLS
        return [(array.at[pl.ds(0, 8), pl.ds(pl.multiple_of(start, COLS), COLS)], block)]
    views = []
    for half in range(2):
        start = shard * SHARD + half * TOP_ROUTE + route * BOT_ROUTE + (chunk - N_TOP) * COLS
        views.append((array.at[pl.ds(8, 4), pl.ds(pl.multiple_of(start, COLS), COLS)], block.at[pl.ds(4 * half, 4)]))
    return views


def sweep(body, carry=0):
    carry = lax.fori_loop(0, N_TOP, functools.partial(body, top=True), carry)
    return lax.fori_loop(N_TOP, N_CHUNK, functools.partial(body, top=False), carry)


def strips(body, carry=0, width=STRIP):
    def step(strip, carry):
        return body(pl.ds(pl.multiple_of(strip * width, width), width), carry)

    return lax.fori_loop(0, COLS // width, step, carry)


def fold(total, values):
    for tile in range(values.shape[1] // 128):
        total = total + values[:, tile * 128:(tile + 1) * 128]
    return total


def step_kernel(
    grads, master_in, one_in, two_in,
    top_out, bot_out, master, one, two,
    mean, sent, total_box, bot_box, top_box,
    near_recv, corner_recv, first_send, second_send, load_sem, side_send, forward_send, partner_send, partner_recv, box_sem, seen, known,
):
    pos_y, pos_x, core = my_place()
    model_pos = lax.axis_index('model')
    mine = model_pos * 8 + lax.axis_index('data')
    grad = grads.at[0]
    got = two
    first_recv, second_recv = near_recv.at[0], near_recv.at[1]
    chips = ((pos_y, pos_x), (pos_y, flip(pos_x)), (flip(pos_y), pos_x), (flip(pos_y), flip(pos_x)))
    places = [data_index(row, col, core) for row, col in chips]
    partner = data_index(pos_y, pos_x, flip(core))

    def copy_to(src, dst, place, send_sem, recv_sem):
        pltpu.make_async_remote_copy(src_ref=src, dst_ref=dst, send_sem=send_sem, recv_sem=recv_sem, device_id=(model_pos, place), device_id_type=MESH).start()

    def landing(route, chunk, block, count, top):
        if top:
            start = ((route * N_TOP + chunk) * 8 + block) * COLS
        else:
            start = ((route * N_BOT + chunk - N_TOP) * 8 + block) * COLS
        return (top_out if top else bot_out).at[:, pl.ds(pl.multiple_of(start, COLS), count * COLS)]

    def wanted(route, row, col, far):
        return (lax.rem(row + far, 2), col) if route == 0 else (row, lax.rem(col + far, 2))

    def local(chunk, carry, top):
        for route in range(2):
            for far in range(2):
                shard = data_index(*wanted(route, pos_y, pos_x, far), core)
                for src, dst in row_views(grad, shard, route, chunk, landing(route, chunk, far, 1, top), top):
                    pltpu.make_async_copy(src, dst, first_recv.at[route, chunk]).start()
        return carry

    def remote(chunk, carry, top):
        for far in range(2):
            for other in range(2):
                for route in range(2):
                    row, col = chips[1 + route]
                    to_core = lax.rem(core + other, 2)
                    shard = data_index(*wanted(route, row, col, far), to_core)
                    for src, dst in row_views(grad, shard, route, chunk, landing(route, chunk, 4 + 2 * other + far, 1, top), top):
                        copy_to(src, dst, data_index(row, col, to_core), first_send.at[int(top)], first_recv.at[route, chunk])
            for route in range(2):
                shard = data_index(*wanted(route, pos_y, pos_x, far), flip(core))
                for src, dst in row_views(grad, shard, route, chunk, landing(route, chunk, 2 + far, 1, top), top):
                    copy_to(src, dst, partner, first_send.at[int(top)], first_recv.at[route, chunk])
        return carry

    def load(array, block, sem, route, chunk, top):
        for src, dst in row_views(array, 0, route, chunk, block.at[route, chunk], top):
            pltpu.make_async_copy(src, dst, sem).start()

    next_to = [(model_pos, place) for chip in (1, 2) for place in (places[chip], data_index(*chips[chip], flip(core)))] + [(model_pos, partner), (flip(model_pos), places[0])]

    def tell(sem, devices):
        for device in devices:
            pl.semaphore_signal(sem, inc=1, device_id=device, device_id_type=MESH)

    barrier = pltpu.get_barrier_semaphore()
    tell(barrier, next_to)
    sweep(local)
    pl.semaphore_wait(barrier, len(next_to))
    sweep(remote)
    tell(seen, next_to)

    def load_state(chunk, carry, top):
        for route in range(2):
            load(master_in, master, load_sem.at[0], route, chunk, top)
            load(one_in, one, load_sem.at[1], route, chunk, top)
        return carry

    sweep(load_state)
    pl.semaphore_wait(seen, len(next_to))
    tell(known, next_to[-1:])

    def second(route, chunk):
        copy_to(sent.at[route, chunk], got.at[route, chunk], places[2 - route], second_send, second_recv.at[route, chunk])

    def add_four(route, chunk, squares, top):
        drain(landing(route, chunk, 0, 8, top), first_recv.at[route, chunk])

        def body(cols, total):
            for far, target in ((0, mean), (1, sent)):
                parts = [landing(route, chunk, 2 * source + far, 1, top)[:, cols].astype(F32) for source in range(4)]
                target[route, chunk, :, cols] = (parts[0] + parts[1]) + (parts[2] + parts[3])
            weight = master[route, chunk, :, cols]
            return fold(total, weight * weight)

        return strips(body, squares)

    def first_sums(chunk, squares, top):
        squares = add_four(0, chunk, squares, top)

        @pl.when(chunk > 0)
        def _():
            second(1, chunk - 1)

        squares = add_four(1, chunk, squares, top)
        second(0, chunk)
        return squares

    drain(master, load_sem.at[0])
    zero = jnp.zeros((8, 128), F32)
    top_squares = lax.fori_loop(0, N_TOP, functools.partial(first_sums, top=True), zero)
    bot_squares = lax.fori_loop(N_TOP, N_CHUNK, functools.partial(first_sums, top=False), zero)
    second(1, N_CHUNK - 1)

    def finish(chunk, squares, top):
        for route in range(2):
            drain(got.at[route, chunk], second_recv.at[route, chunk])

            def body(cols, total):
                value = (mean[route, chunk, :, cols] + got[route, chunk, :, cols]) * 0.125
                mean[route, chunk, :, cols] = value
                return fold(total, value * value)

            squares = strips(body, squares)
            load(two_in, two, load_sem.at[2 + int(top)], route, chunk, top)
        return squares

    everyone = [(row, data_index(*chip, side)) for row, chip in (
        (flip(model_pos), chips[3]), (flip(model_pos), chips[2]), (flip(model_pos), chips[1]), (model_pos, chips[3]),
        (flip(model_pos), chips[0]), (model_pos, chips[2]), (model_pos, chips[1]),
    ) for side in (core, flip(core))] + [(model_pos, partner)]

    def share_all(box, send_sem, recv_sem):
        for device in everyone:
            pltpu.make_async_remote_copy(src_ref=box.at[mine], dst_ref=box.at[mine], send_sem=send_sem, recv_sem=recv_sem, device_id=device, device_id_type=MESH).start()

    total_box[mine] = jnp.sum(sweep(finish, zero), axis=0, keepdims=True)
    pl.semaphore_wait(known, 1)
    share_all(total_box, box_sem.at[0], box_sem.at[1])
    drain(total_box.at[pl.ds(0, 15)], box_sem.at[1])
    total = jnp.sum(jnp.sum(total_box[...], axis=0), keepdims=True)
    clip = jnp.minimum(1.0, MAX_NORM / jnp.sqrt(total))
    one_scale, two_scale = clip * (1.0 - BETA_ONE), clip * (1.0 - BETA_TWO) ** 0.5

    def update(route, chunk, carry):
        def body(cols, total):
            place = (route, chunk, slice(None), cols)
            weight = master[place]
            value = mean[place]
            new_one = BETA_ONE * one[place] + one_scale * value
            change = two_scale * value
            new_two = BETA_TWO * two[place] + change * change
            one[place] = new_one
            two[place] = new_two
            floor = jnp.maximum(new_two, TINY)
            root = floor * lax.rsqrt(floor)
            direction = (new_one * (CORR_TWO ** 0.5 / CORR_ONE)) / (root + EPSILON * CORR_TWO ** 0.5) + WEIGHT_DECAY * weight
            mean[place] = direction
            return fold(total, direction * direction)

        return strips(body, carry, UPDATE_STRIP)

    def update_rows(index, low, high):
        drain(two.at[:, pl.ds(low, high - low)], load_sem.at[2 + index])
        return lax.fori_loop(low, high, lambda chunk, total: update(1, chunk, update(0, chunk, total)), zero)

    def share_norms(index, box, rows):
        for position, value in enumerate(rows):
            box[mine, position:position + 1] = value
        share_all(box, box_sem.at[2 + index], box_sem.at[4 + index])

    def norm_rows(index, box):
        drain(box.at[pl.ds(0, 15)], box_sem.at[4 + index])
        return jnp.sqrt(jnp.sum(jnp.sum(box[...], axis=0), axis=1, keepdims=True))

    def bot_rate():
        norms = norm_rows(0, bot_box)
        return LEARN_RATE * (norms[0:1] / norms[1:2]) + jnp.zeros((8, 1), F32)

    def top_rate():
        norms = norm_rows(1, top_box)
        rates = [LEARN_RATE * (norms[position:position + 1] / norms[position + 3:position + 4]) for position in range(3)]
        row = lax.broadcasted_iota(jnp.int32, (8, 1), 0)
        return jnp.where(row < 3, rates[0], jnp.where(row == 3, rates[1], rates[2]))

    def tensor_rows(squares):
        row = lax.broadcasted_iota(jnp.int32, (8, 128), 0)
        return [jnp.sum(jnp.where(mask, squares, 0.0), axis=0, keepdims=True) for mask in (row < 3, row == 3, row > 3)]

    drain(one, load_sem.at[1])
    share_norms(0, bot_box, [jnp.sum(squares, axis=0, keepdims=True) for squares in (bot_squares, update_rows(0, N_TOP, N_CHUNK))])
    share_norms(1, top_box, tensor_rows(top_squares) + tensor_rows(update_rows(1, 0, N_TOP)))

    def piece(place, route, chunk, top):
        if top:
            start = place * SHARD + route * TOP_ROUTE + chunk * COLS
        else:
            start = place * (SHARD // 2) + route * BOT_ROUTE + (chunk - N_TOP) * COLS
        return (top_out if top else bot_out).at[:, pl.ds(pl.multiple_of(start, COLS), COLS)]

    def part(place, top, share=1):
        size = SHARD if top else SHARD // 2
        return (top_out if top else bot_out).at[:, pl.ds(pl.multiple_of(place * size, size), size // share)]

    def weights(route, chunk, rate, top):
        view = piece(places[0], route, chunk, top)

        def body(cols, carry):
            place = (route, chunk, slice(None), cols)
            value = master[place] - rate * mean[place]
            master[place] = value
            view[:, cols] = value.astype(BF16)
            return carry

        strips(body)

    def send(route, chunk, top):
        view = piece(places[0], route, chunk, top)
        kind = int(top)
        for axis in range(2):
            copy_to(view, view, places[1 + axis], side_send.at[axis, kind], near_recv.at[axis, route, chunk])
        copy_to(view, view, partner, partner_send.at[0, kind], partner_recv.at[0, kind])

    def own(chunk, rate, top):
        weights(0, chunk, rate, top)

        @pl.when(chunk > (0 if top else N_TOP))
        def _():
            send(1, chunk - 1, top)

        weights(1, chunk, rate, top)
        send(0, chunk, top)

        @pl.when(chunk == (N_TOP - 1 if top else N_CHUNK - 1))
        def _():
            send(1, chunk, top)

        return rate

    def hand_on(chunk, carry, top):
        kind = int(top)
        for route in range(2):
            for axis in range(2):
                view = piece(places[1 + axis], route, chunk, top)
                drain(view, near_recv.at[axis, route, chunk])
                if axis == route:
                    copy_to(view, view, places[2 - axis], forward_send.at[route, kind], corner_recv.at[route, chunk])
                copy_to(view, view, partner, partner_send.at[1 + axis, kind], partner_recv.at[1 + axis, kind])
        return carry

    def corner(chunk, carry, top):
        for route in range(2):
            view = piece(places[3], route, chunk, top)
            drain(view, corner_recv.at[route, chunk])
            copy_to(view, view, partner, partner_send.at[3, int(top)], partner_recv.at[3, int(top)])
        return carry

    def bottom_first(body, carry=0):
        carry = lax.fori_loop(N_TOP, N_CHUNK, functools.partial(body, top=False), carry)
        return lax.fori_loop(0, N_TOP, functools.partial(body, top=True), carry)

    lax.fori_loop(N_TOP, N_CHUNK, functools.partial(own, top=False), bot_rate())
    lax.fori_loop(0, N_TOP, functools.partial(own, top=True), top_rate())
    bottom_first(hand_on)
    bottom_first(corner)

    for top in (True, False):
        kind = int(top)
        for axis in range(2):
            drain(part(places[0], top), side_send.at[axis, kind])
            drain(part(places[0], top, 2), forward_send.at[axis, kind])
        for chip, (row_pos, col_pos) in enumerate(chips):
            drain(part(places[chip], top), partner_send.at[chip, kind])
            drain(part(data_index(row_pos, col_pos, flip(core)), top), partner_recv.at[chip, kind])
    drain(total_box.at[pl.ds(0, 15)], box_sem.at[0])
    drain(bot_box.at[pl.ds(0, 15)], box_sem.at[2])
    drain(top_box.at[pl.ds(0, 15)], box_sem.at[3])

    drain(top_out.at[:, pl.ds(0, 6 * SHARD)], first_send.at[1])
    drain(bot_out.at[:, pl.ds(0, 3 * SHARD)], first_send.at[0])
    drain(sent, second_send)


def in_hbm(array):
    return pltpu.with_memory_space_constraint(array, pltpu.HBM)


def run_step(local_grads, master, moment_one, moment_two):
    dma = pltpu.SemaphoreType.DMA
    block = pltpu.VMEM((2, N_CHUNK, 8, COLS), F32)
    return pl.pallas_call(
        step_kernel,
        out_shape=(pltpu.VMEM((8, 8 * SHARD), BF16), pltpu.VMEM((8, 4 * SHARD), BF16), block, block, block),
        in_specs=[pl.BlockSpec(memory_space=pltpu.HBM)] * 4,
        out_specs=(pl.BlockSpec(memory_space=pltpu.VMEM),) * 5,
        scratch_shapes=[
            block, block,
            pltpu.VMEM((16, 1, 128), F32),
            pltpu.VMEM((16, 2, 128), F32),
            pltpu.VMEM((16, 6, 128), F32),
            dma((2, 2, N_CHUNK)), dma((2, N_CHUNK)), dma((2,)), dma, dma((4,)), dma((2, 2)), dma((2, 2)), dma((4, 2)), dma((4, 2)), dma((6,)),
            pltpu.SemaphoreType.REGULAR, pltpu.SemaphoreType.REGULAR,
        ],
        compiler_params=pltpu.CompilerParams(collective_id=0, has_side_effects=True, vmem_limit_bytes=STEP_LIMIT),
        name='lamb_step',
    )(in_hbm(local_grads), in_hbm(master), in_hbm(moment_one), in_hbm(moment_two))


def write_kernel(top, bot, master, one, two, params_out, master_out, one_out, two_out, sem):
    copies = []
    for place in range(8):
        copies.append((top.at[:, pl.ds(place * SHARD, SHARD)], params_out.at[pl.ds(0, 8), pl.ds(place * SHARD, SHARD)]))
        for half in range(2):
            copies.append((bot.at[pl.ds(4 * half, 4), pl.ds(place * TOP_ROUTE, TOP_ROUTE)], params_out.at[pl.ds(8, 4), pl.ds(place * SHARD + half * TOP_ROUTE, TOP_ROUTE)]))
    for block, array in ((master, master_out), (one, one_out), (two, two_out)):
        for route in range(2):
            for chunk in range(N_CHUNK):
                copies += [(src, dst) for dst, src in row_views(array, 0, route, chunk, block.at[route, chunk], chunk < N_TOP)]
    for src, dst in copies:
        pltpu.make_async_copy(src, dst, sem).start()
    for src, dst in copies:
        pltpu.make_async_copy(src, dst, sem).wait()


def write_out(*blocks):
    state = jax.ShapeDtypeStruct((12, SHARD), F32)
    return pl.pallas_call(
        write_kernel,
        out_shape=(jax.ShapeDtypeStruct((12, 8 * SHARD), BF16), state, state, state),
        in_specs=[pl.BlockSpec(memory_space=pltpu.VMEM)] * 5,
        out_specs=(pl.BlockSpec(memory_space=pltpu.HBM),) * 4,
        scratch_shapes=[pltpu.SemaphoreType.DMA],
        compiler_params=pltpu.CompilerParams(vmem_limit_bytes=WRITE_LIMIT),
        name='write_out',
    )(*[pltpu.with_memory_space_constraint(block, pltpu.VMEM) for block in blocks])


def solution(mesh):
    state_spec = P(None, ('model', 'data'))

    def device_step(local_grads, master, moment_one, moment_two):
        return write_out(*run_step(local_grads, master, moment_one, moment_two))

    return jax.shard_map(device_step, mesh=mesh, in_specs=(P('data', None, 'model'), state_spec, state_spec, state_spec), out_specs=(P(None, 'model'), state_spec, state_spec, state_spec), check_vma=False)
```

```python
import functools

import jax
import jax.numpy as jnp
from jax import lax
from jax.experimental import pallas as pl
from jax.experimental.pallas import tpu as pltpu
from jax.sharding import PartitionSpec as P

STEP = 4
LEARN_RATE = 0.08
BETA_ONE = 0.9
BETA_TWO = 0.999
EPSILON = 1e-6
WEIGHT_DECAY = 0.01
MAX_NORM = 1.0
CORR_ONE = 1.0 - BETA_ONE ** STEP
CORR_TWO = 1.0 - BETA_TWO ** STEP

MESH = pl.DeviceIdType.MESH
F32 = jnp.float32
BF16 = jnp.bfloat16

SHARD = 147456
COLS = 12288
TOP_ROUTE = SHARD // 2
BOT_ROUTE = SHARD // 4
N_TOP = TOP_ROUTE // COLS
N_BOT = BOT_ROUTE // COLS
N_CHUNK = N_TOP + N_BOT
STRIP = 1024
UPDATE_STRIP = 2048

TINY = 1.2e-38
MIB = 1024 * 1024
STEP_LIMIT = 15 * MIB
WRITE_LIMIT = STEP_LIMIT


def flip(value):
    return 1 - value


def my_place():
    data_pos = lax.axis_index('data')
    return data_pos // 4, lax.rem(data_pos // 2, 2), lax.rem(data_pos, 2)


def data_index(pos_y, pos_x, core):
    return (pos_y * 2 + pos_x) * 2 + core


def drain(ref, sem):
    pltpu.make_async_copy(ref, ref, sem).wait()


def row_views(array, shard, route, chunk, block, top):
    if top:
        start = shard * SHARD + route * TOP_ROUTE + chunk * COLS
        return [(array.at[pl.ds(0, 8), pl.ds(pl.multiple_of(start, COLS), COLS)], block)]
    views = []
    for half in range(2):
        start = shard * SHARD + half * TOP_ROUTE + route * BOT_ROUTE + (chunk - N_TOP) * COLS
        views.append((array.at[pl.ds(8, 4), pl.ds(pl.multiple_of(start, COLS), COLS)], block.at[pl.ds(4 * half, 4)]))
    return views


def sweep(body, carry=0):
    carry = lax.fori_loop(0, N_TOP, functools.partial(body, top=True), carry)
    return lax.fori_loop(N_TOP, N_CHUNK, functools.partial(body, top=False), carry)


def strips(body, carry=0, width=STRIP):
    def step(strip, carry):
        return body(pl.ds(pl.multiple_of(strip * width, width), width), carry)

    return lax.fori_loop(0, COLS // width, step, carry)


def fold(total, values):
    for tile in range(values.shape[1] // 128):
        total = total + values[:, tile * 128:(tile + 1) * 128]
    return total


def step_kernel(
    grads, master_in, one_in, two_in,
    top_out, bot_out, master, one, two,
    mean, sent, lead, total_box, bot_box, top_box,
    lead_sem, near_recv, corner_recv, first_send, second_send, load_sem, side_send, forward_send, partner_send, partner_recv, box_sem, seen, known,
):
    pos_y, pos_x, core = my_place()
    model_pos = lax.axis_index('model')
    mine = model_pos * 8 + lax.axis_index('data')
    grad = grads.at[0]
    got = two
    first_recv, second_recv = near_recv.at[0], near_recv.at[1]
    chips = ((pos_y, pos_x), (pos_y, flip(pos_x)), (flip(pos_y), pos_x), (flip(pos_y), flip(pos_x)))
    places = [data_index(row, col, core) for row, col in chips]
    partner = data_index(pos_y, pos_x, flip(core))

    def copy_to(src, dst, place, send_sem, recv_sem):
        pltpu.make_async_remote_copy(src_ref=src, dst_ref=dst, send_sem=send_sem, recv_sem=recv_sem, device_id=(model_pos, place), device_id_type=MESH).start()

    def landing(route, chunk, block, count, top):
        if top:
            start = ((route * N_TOP + chunk) * 8 + block) * COLS
        else:
            start = ((route * N_BOT + chunk - N_TOP) * 8 + block) * COLS
        return (top_out if top else bot_out).at[:, pl.ds(pl.multiple_of(start, COLS), count * COLS)]

    def wanted(route, row, col, far):
        return (lax.rem(row + far, 2), col) if route == 0 else (row, lax.rem(col + far, 2))

    def local(chunk, carry, top):
        for route in range(2):
            for far in range(2):
                shard = data_index(*wanted(route, pos_y, pos_x, far), core)
                for src, dst in row_views(grad, shard, route, chunk, landing(route, chunk, far, 1, top), top):
                    pltpu.make_async_copy(src, dst, first_recv.at[route, chunk]).start()
        return carry

    def remote(chunk, carry, top):
        for far in range(2):
            for other in range(2):
                for route in range(2):
                    row, col = chips[1 + route]
                    to_core = lax.rem(core + other, 2)
                    shard = data_index(*wanted(route, row, col, far), to_core)
                    for src, dst in row_views(grad, shard, route, chunk, landing(route, chunk, 4 + 2 * other + far, 1, top), top):
                        if top and far == other == 0:
                            @pl.when(chunk > 0)
                            def _():
                                copy_to(src, dst, data_index(row, col, to_core), first_send.at[1], first_recv.at[route, chunk])
                        else:
                            copy_to(src, dst, data_index(row, col, to_core), first_send.at[int(top)], first_recv.at[route, chunk])
            for route in range(2):
                shard = data_index(*wanted(route, pos_y, pos_x, far), flip(core))
                for src, dst in row_views(grad, shard, route, chunk, landing(route, chunk, 2 + far, 1, top), top):
                    copy_to(src, dst, partner, first_send.at[int(top)], first_recv.at[route, chunk])
        return carry

    def load(array, block, sem, route, chunk, top):
        for src, dst in row_views(array, 0, route, chunk, block.at[route, chunk], top):
            pltpu.make_async_copy(src, dst, sem).start()

    next_to = [(model_pos, place) for chip in (1, 2) for place in (places[chip], data_index(*chips[chip], flip(core)))] + [(model_pos, partner), (flip(model_pos), places[0])]

    def tell(sem, devices):
        for device in devices:
            pl.semaphore_signal(sem, inc=1, device_id=device, device_id_type=MESH)

    barrier = pltpu.get_barrier_semaphore()
    tell(barrier, next_to)
    leads = []
    for route in range(2):
        shard = data_index(*wanted(route, *chips[1 + route], 0), core)
        (src, _), = row_views(grad, shard, route, 0, lead.at[route], True)
        leads.append(pltpu.make_async_copy(src, lead.at[route], lead_sem.at[route]))
        leads[-1].start()
    pl.semaphore_wait(barrier, len(next_to))
    for route, copy in enumerate(leads):
        copy.wait()
        copy_to(lead.at[route], landing(route, 0, 4, 1, True), places[1 + route], first_send.at[1], first_recv.at[route, 0])
    sweep(remote)
    sweep(local)
    tell(seen, next_to)

    def load_state(chunk, carry, top):
        for route in range(2):
            load(master_in, master, load_sem.at[0], route, chunk, top)
            load(one_in, one, load_sem.at[1], route, chunk, top)
        return carry

    sweep(load_state)
    pl.semaphore_wait(seen, len(next_to))
    tell(known, next_to[-1:])

    def second(route, chunk):
        copy_to(sent.at[route, chunk], got.at[route, chunk], places[2 - route], second_send, second_recv.at[route, chunk])

    def add_four(route, chunk, squares, top):
        drain(landing(route, chunk, 0, 8, top), first_recv.at[route, chunk])

        def body(cols, total):
            for far, target in ((0, mean), (1, sent)):
                parts = [landing(route, chunk, 2 * source + far, 1, top)[:, cols].astype(F32) for source in range(4)]
                target[route, chunk, :, cols] = (parts[0] + parts[1]) + (parts[2] + parts[3])
            weight = master[route, chunk, :, cols]
            return fold(total, weight * weight)

        return strips(body, squares)

    def first_sums(chunk, squares, top):
        squares = add_four(0, chunk, squares, top)

        @pl.when(chunk > 0)
        def _():
            second(1, chunk - 1)

        squares = add_four(1, chunk, squares, top)
        second(0, chunk)
        return squares

    drain(master, load_sem.at[0])
    zero = jnp.zeros((8, 128), F32)
    top_squares = lax.fori_loop(0, N_TOP, functools.partial(first_sums, top=True), zero)
    bot_squares = lax.fori_loop(N_TOP, N_CHUNK, functools.partial(first_sums, top=False), zero)
    second(1, N_CHUNK - 1)

    def finish(chunk, squares, top):
        for route in range(2):
            drain(got.at[route, chunk], second_recv.at[route, chunk])

            def body(cols, total):
                value = (mean[route, chunk, :, cols] + got[route, chunk, :, cols]) * 0.125
                mean[route, chunk, :, cols] = value
                return fold(total, value * value)

            squares = strips(body, squares)
            load(two_in, two, load_sem.at[2 + int(top)], route, chunk, top)
        return squares

    everyone = [(row, data_index(*chip, side)) for row, chip in (
        (flip(model_pos), chips[3]), (flip(model_pos), chips[2]), (flip(model_pos), chips[1]), (model_pos, chips[3]),
        (flip(model_pos), chips[0]), (model_pos, chips[2]), (model_pos, chips[1]),
    ) for side in (core, flip(core))] + [(model_pos, partner)]

    def share_all(box, send_sem, recv_sem):
        for device in everyone:
            pltpu.make_async_remote_copy(src_ref=box.at[mine], dst_ref=box.at[mine], send_sem=send_sem, recv_sem=recv_sem, device_id=device, device_id_type=MESH).start()

    total_box[mine] = jnp.sum(sweep(finish, zero), axis=0, keepdims=True)
    pl.semaphore_wait(known, 1)
    share_all(total_box, box_sem.at[0], box_sem.at[1])
    drain(total_box.at[pl.ds(0, 15)], box_sem.at[1])
    total = jnp.sum(jnp.sum(total_box[...], axis=0), keepdims=True)
    clip = jnp.minimum(1.0, MAX_NORM / jnp.sqrt(total))
    one_scale, two_scale = clip * (1.0 - BETA_ONE), clip * (1.0 - BETA_TWO) ** 0.5

    def update(route, chunk, carry):
        def body(cols, total):
            place = (route, chunk, slice(None), cols)
            weight = master[place]
            value = mean[place]
            new_one = BETA_ONE * one[place] + one_scale * value
            change = two_scale * value
            new_two = BETA_TWO * two[place] + change * change
            one[place] = new_one
            two[place] = new_two
            floor = jnp.maximum(new_two, TINY)
            root = floor * lax.rsqrt(floor)
            direction = (new_one * (CORR_TWO ** 0.5 / CORR_ONE)) / (root + EPSILON * CORR_TWO ** 0.5) + WEIGHT_DECAY * weight
            mean[place] = direction
            return fold(total, direction * direction)

        return strips(body, carry, UPDATE_STRIP)

    def update_rows(index, low, high):
        drain(two.at[:, pl.ds(low, high - low)], load_sem.at[2 + index])
        return lax.fori_loop(low, high, lambda chunk, total: update(1, chunk, update(0, chunk, total)), zero)

    def share_norms(index, box, rows):
        for position, value in enumerate(rows):
            box[mine, position:position + 1] = value
        share_all(box, box_sem.at[2 + index], box_sem.at[4 + index])

    def norm_rows(index, box):
        drain(box.at[pl.ds(0, 15)], box_sem.at[4 + index])
        return jnp.sqrt(jnp.sum(jnp.sum(box[...], axis=0), axis=1, keepdims=True))

    def bot_rate():
        norms = norm_rows(0, bot_box)
        return LEARN_RATE * (norms[0:1] / norms[1:2]) + jnp.zeros((8, 1), F32)

    def top_rate():
        norms = norm_rows(1, top_box)
        rates = [LEARN_RATE * (norms[position:position + 1] / norms[position + 3:position + 4]) for position in range(3)]
        row = lax.broadcasted_iota(jnp.int32, (8, 1), 0)
        return jnp.where(row < 3, rates[0], jnp.where(row == 3, rates[1], rates[2]))

    def tensor_rows(squares):
        row = lax.broadcasted_iota(jnp.int32, (8, 128), 0)
        return [jnp.sum(jnp.where(mask, squares, 0.0), axis=0, keepdims=True) for mask in (row < 3, row == 3, row > 3)]

    drain(one, load_sem.at[1])
    share_norms(0, bot_box, [jnp.sum(squares, axis=0, keepdims=True) for squares in (bot_squares, update_rows(0, N_TOP, N_CHUNK))])
    share_norms(1, top_box, tensor_rows(top_squares) + tensor_rows(update_rows(1, 0, N_TOP)))

    def piece(place, route, chunk, top):
        if top:
            start = place * SHARD + route * TOP_ROUTE + chunk * COLS
        else:
            start = place * (SHARD // 2) + route * BOT_ROUTE + (chunk - N_TOP) * COLS
        return (top_out if top else bot_out).at[:, pl.ds(pl.multiple_of(start, COLS), COLS)]

    def part(place, top, share=1):
        size = SHARD if top else SHARD // 2
        return (top_out if top else bot_out).at[:, pl.ds(pl.multiple_of(place * size, size), size // share)]

    def weights(route, chunk, rate, top):
        view = piece(places[0], route, chunk, top)

        def body(cols, carry):
            place = (route, chunk, slice(None), cols)
            value = master[place] - rate * mean[place]
            master[place] = value
            view[:, cols] = value.astype(BF16)
            return carry

        strips(body)

    def send(route, chunk, top):
        view = piece(places[0], route, chunk, top)
        kind = int(top)
        for axis in range(2):
            copy_to(view, view, places[1 + axis], side_send.at[axis, kind], near_recv.at[axis, route, chunk])
        copy_to(view, view, partner, partner_send.at[0, kind], partner_recv.at[0, kind])

    def own(chunk, rate, top):
        weights(0, chunk, rate, top)

        @pl.when(chunk > (0 if top else N_TOP))
        def _():
            send(1, chunk - 1, top)

        weights(1, chunk, rate, top)
        send(0, chunk, top)

        @pl.when(chunk == (N_TOP - 1 if top else N_CHUNK - 1))
        def _():
            send(1, chunk, top)

        return rate

    def hand_on(chunk, carry, top):
        kind = int(top)
        for route in range(2):
            for axis in range(2):
                view = piece(places[1 + axis], route, chunk, top)
                drain(view, near_recv.at[axis, route, chunk])
                if axis == route:
                    copy_to(view, view, places[2 - axis], forward_send.at[route, kind], corner_recv.at[route, chunk])
                copy_to(view, view, partner, partner_send.at[1 + axis, kind], partner_recv.at[1 + axis, kind])
        return carry

    def corner(chunk, carry, top):
        for route in range(2):
            view = piece(places[3], route, chunk, top)
            drain(view, corner_recv.at[route, chunk])
            copy_to(view, view, partner, partner_send.at[3, int(top)], partner_recv.at[3, int(top)])
        return carry

    def bottom_first(body, carry=0):
        carry = lax.fori_loop(N_TOP, N_CHUNK, functools.partial(body, top=False), carry)
        return lax.fori_loop(0, N_TOP, functools.partial(body, top=True), carry)

    lax.fori_loop(N_TOP, N_CHUNK, functools.partial(own, top=False), bot_rate())
    lax.fori_loop(0, N_TOP, functools.partial(own, top=True), top_rate())
    bottom_first(hand_on)
    bottom_first(corner)

    for top in (True, False):
        kind = int(top)
        for axis in range(2):
            drain(part(places[0], top), side_send.at[axis, kind])
            drain(part(places[0], top, 2), forward_send.at[axis, kind])
        for chip, (row_pos, col_pos) in enumerate(chips):
            drain(part(places[chip], top), partner_send.at[chip, kind])
            drain(part(data_index(row_pos, col_pos, flip(core)), top), partner_recv.at[chip, kind])
    drain(total_box.at[pl.ds(0, 15)], box_sem.at[0])
    drain(bot_box.at[pl.ds(0, 15)], box_sem.at[2])
    drain(top_box.at[pl.ds(0, 15)], box_sem.at[3])

    drain(top_out.at[:, pl.ds(0, 6 * SHARD)], first_send.at[1])
    drain(bot_out.at[:, pl.ds(0, 3 * SHARD)], first_send.at[0])
    drain(sent, second_send)


def in_hbm(array):
    return pltpu.with_memory_space_constraint(array, pltpu.HBM)


def run_step(local_grads, master, moment_one, moment_two):
    dma = pltpu.SemaphoreType.DMA
    block = pltpu.VMEM((2, N_CHUNK, 8, COLS), F32)
    return pl.pallas_call(
        step_kernel,
        out_shape=(pltpu.VMEM((8, 8 * SHARD), BF16), pltpu.VMEM((8, 4 * SHARD), BF16), block, block, block),
        in_specs=[pl.BlockSpec(memory_space=pltpu.HBM)] * 4,
        out_specs=(pl.BlockSpec(memory_space=pltpu.VMEM),) * 5,
        scratch_shapes=[
            block, block, pltpu.VMEM((2, 8, COLS), BF16),
            pltpu.VMEM((16, 1, 128), F32),
            pltpu.VMEM((16, 2, 128), F32),
            pltpu.VMEM((16, 6, 128), F32),
            dma((2,)), dma((2, 2, N_CHUNK)), dma((2, N_CHUNK)), dma((2,)), dma, dma((4,)), dma((2, 2)), dma((2, 2)), dma((4, 2)), dma((4, 2)), dma((6,)),
            pltpu.SemaphoreType.REGULAR, pltpu.SemaphoreType.REGULAR,
        ],
        compiler_params=pltpu.CompilerParams(collective_id=0, has_side_effects=True, vmem_limit_bytes=STEP_LIMIT),
        name='lamb_step',
    )(in_hbm(local_grads), in_hbm(master), in_hbm(moment_one), in_hbm(moment_two))


def write_kernel(top, bot, master, one, two, params_out, master_out, one_out, two_out, sem):
    copies = []
    for place in range(8):
        copies.append((top.at[:, pl.ds(place * SHARD, SHARD)], params_out.at[pl.ds(0, 8), pl.ds(place * SHARD, SHARD)]))
        for half in range(2):
            copies.append((bot.at[pl.ds(4 * half, 4), pl.ds(place * TOP_ROUTE, TOP_ROUTE)], params_out.at[pl.ds(8, 4), pl.ds(place * SHARD + half * TOP_ROUTE, TOP_ROUTE)]))
    for block, array in ((master, master_out), (one, one_out), (two, two_out)):
        for route in range(2):
            for chunk in range(N_CHUNK):
                copies += [(src, dst) for dst, src in row_views(array, 0, route, chunk, block.at[route, chunk], chunk < N_TOP)]
    for src, dst in copies:
        pltpu.make_async_copy(src, dst, sem).start()
    for src, dst in copies:
        pltpu.make_async_copy(src, dst, sem).wait()


def write_out(*blocks):
    state = jax.ShapeDtypeStruct((12, SHARD), F32)
    return pl.pallas_call(
        write_kernel,
        out_shape=(jax.ShapeDtypeStruct((12, 8 * SHARD), BF16), state, state, state),
        in_specs=[pl.BlockSpec(memory_space=pltpu.VMEM)] * 5,
        out_specs=(pl.BlockSpec(memory_space=pltpu.HBM),) * 4,
        scratch_shapes=[pltpu.SemaphoreType.DMA],
        compiler_params=pltpu.CompilerParams(vmem_limit_bytes=WRITE_LIMIT),
        name='write_out',
    )(*[pltpu.with_memory_space_constraint(block, pltpu.VMEM) for block in blocks])


def solution(mesh):
    state_spec = P(None, ('model', 'data'))

    def device_step(local_grads, master, moment_one, moment_two):
        return write_out(*run_step(local_grads, master, moment_one, moment_two))

    return jax.shard_map(device_step, mesh=mesh, in_specs=(P('data', None, 'model'), state_spec, state_spec, state_spec), out_specs=(P(None, 'model'), state_spec, state_spec, state_spec), check_vma=False)
```

```python
import functools

import jax
import jax.numpy as jnp
from jax import lax
from jax.experimental import pallas as pl
from jax.experimental.pallas import tpu as pltpu
from jax.sharding import PartitionSpec as P

STEP = 4
LEARN_RATE = 0.08
BETA_ONE = 0.9
BETA_TWO = 0.999
EPSILON = 1e-6
WEIGHT_DECAY = 0.01
MAX_NORM = 1.0
CORR_ONE = 1.0 - BETA_ONE ** STEP
CORR_TWO = 1.0 - BETA_TWO ** STEP

MESH = pl.DeviceIdType.MESH
F32 = jnp.float32
BF16 = jnp.bfloat16

SHARD = 147456
COLS = 18432
TOP_ROUTE = SHARD // 2
BOT_ROUTE = SHARD // 4
N_TOP = TOP_ROUTE // COLS
N_BOT = BOT_ROUTE // COLS
N_CHUNK = N_TOP + N_BOT
STRIP = 1024
UPDATE_STRIP = 2048

TINY = 1.2e-38
MIB = 1024 * 1024
STEP_LIMIT = 15 * MIB
WRITE_LIMIT = STEP_LIMIT


def flip(value):
    return 1 - value


def my_place():
    data_pos = lax.axis_index('data')
    return data_pos // 4, lax.rem(data_pos // 2, 2), lax.rem(data_pos, 2)


def data_index(pos_y, pos_x, core):
    return (pos_y * 2 + pos_x) * 2 + core


def drain(ref, sem):
    pltpu.make_async_copy(ref, ref, sem).wait()


def row_views(array, shard, route, chunk, block, top):
    if top:
        start = shard * SHARD + route * TOP_ROUTE + chunk * COLS
        return [(array.at[pl.ds(0, 8), pl.ds(pl.multiple_of(start, COLS), COLS)], block)]
    views = []
    for half in range(2):
        start = shard * SHARD + half * TOP_ROUTE + route * BOT_ROUTE + (chunk - N_TOP) * COLS
        views.append((array.at[pl.ds(8, 4), pl.ds(pl.multiple_of(start, COLS), COLS)], block.at[pl.ds(4 * half, 4)]))
    return views


def sweep(body, carry=0):
    carry = lax.fori_loop(0, N_TOP, functools.partial(body, top=True), carry)
    return lax.fori_loop(N_TOP, N_CHUNK, functools.partial(body, top=False), carry)


def strips(body, carry=0, width=STRIP):
    def step(strip, carry):
        return body(pl.ds(pl.multiple_of(strip * width, width), width), carry)

    return lax.fori_loop(0, COLS // width, step, carry)


def fold(total, values):
    for tile in range(values.shape[1] // 128):
        total = total + values[:, tile * 128:(tile + 1) * 128]
    return total


def step_kernel(
    grads, master_in, one_in, two_in,
    top_out, bot_out, master, one, two,
    mean, sent, total_box, bot_box, top_box,
    near_recv, corner_recv, first_send, second_send, load_sem, side_send, forward_send, partner_send, partner_recv, box_sem, seen, known,
):
    pos_y, pos_x, core = my_place()
    model_pos = lax.axis_index('model')
    mine = model_pos * 8 + lax.axis_index('data')
    grad = grads.at[0]
    got = two
    first_recv, second_recv = near_recv.at[0], near_recv.at[1]
    chips = ((pos_y, pos_x), (pos_y, flip(pos_x)), (flip(pos_y), pos_x), (flip(pos_y), flip(pos_x)))
    places = [data_index(row, col, core) for row, col in chips]
    partner = data_index(pos_y, pos_x, flip(core))

    def copy_to(src, dst, place, send_sem, recv_sem):
        pltpu.make_async_remote_copy(src_ref=src, dst_ref=dst, send_sem=send_sem, recv_sem=recv_sem, device_id=(model_pos, place), device_id_type=MESH).start()

    def landing(route, chunk, block, count, top):
        if top:
            start = ((route * N_TOP + chunk) * 8 + block) * COLS
        else:
            start = ((route * N_BOT + chunk - N_TOP) * 8 + block) * COLS
        return (top_out if top else bot_out).at[:, pl.ds(pl.multiple_of(start, COLS), count * COLS)]

    def wanted(route, row, col, far):
        return (lax.rem(row + far, 2), col) if route == 0 else (row, lax.rem(col + far, 2))

    def local(chunk, carry, top):
        for route in range(2):
            for far in range(2):
                shard = data_index(*wanted(route, pos_y, pos_x, far), core)
                for src, dst in row_views(grad, shard, route, chunk, landing(route, chunk, far, 1, top), top):
                    pltpu.make_async_copy(src, dst, first_recv.at[route, chunk]).start()
        return carry

    def remote(chunk, carry, top):
        for far in range(2):
            for other in range(2):
                for route in range(2):
                    row, col = chips[1 + route]
                    to_core = lax.rem(core + other, 2)
                    shard = data_index(*wanted(route, row, col, far), to_core)
                    for src, dst in row_views(grad, shard, route, chunk, landing(route, chunk, 4 + 2 * other + far, 1, top), top):
                        copy_to(src, dst, data_index(row, col, to_core), first_send.at[int(top)], first_recv.at[route, chunk])
            for route in range(2):
                shard = data_index(*wanted(route, pos_y, pos_x, far), flip(core))
                for src, dst in row_views(grad, shard, route, chunk, landing(route, chunk, 2 + far, 1, top), top):
                    copy_to(src, dst, partner, first_send.at[int(top)], first_recv.at[route, chunk])
        return carry

    def load(array, block, sem, route, chunk, top):
        for src, dst in row_views(array, 0, route, chunk, block.at[route, chunk], top):
            pltpu.make_async_copy(src, dst, sem).start()

    next_to = [(model_pos, place) for chip in (1, 2) for place in (places[chip], data_index(*chips[chip], flip(core)))] + [(model_pos, partner), (flip(model_pos), places[0])]

    def tell(sem, devices):
        for device in devices:
            pl.semaphore_signal(sem, inc=1, device_id=device, device_id_type=MESH)

    barrier = pltpu.get_barrier_semaphore()
    tell(barrier, next_to)
    sweep(local)
    pl.semaphore_wait(barrier, len(next_to))
    sweep(remote)
    tell(seen, next_to)

    def load_state(chunk, carry, top):
        for route in range(2):
            load(master_in, master, load_sem.at[0], route, chunk, top)
            load(one_in, one, load_sem.at[1], route, chunk, top)
        return carry

    sweep(load_state)
    pl.semaphore_wait(seen, len(next_to))
    tell(known, next_to[-1:])

    def second(route, chunk):
        copy_to(sent.at[route, chunk], got.at[route, chunk], places[2 - route], second_send, second_recv.at[route, chunk])

    def add_four(route, chunk, squares, top):
        drain(landing(route, chunk, 0, 8, top), first_recv.at[route, chunk])

        def body(cols, total):
            for far, target in ((0, mean), (1, sent)):
                parts = [landing(route, chunk, 2 * source + far, 1, top)[:, cols].astype(F32) for source in range(4)]
                target[route, chunk, :, cols] = (parts[0] + parts[1]) + (parts[2] + parts[3])
            weight = master[route, chunk, :, cols]
            return fold(total, weight * weight)

        return strips(body, squares)

    def first_sums(chunk, squares, top):
        squares = add_four(0, chunk, squares, top)

        @pl.when(chunk > 0)
        def _():
            second(1, chunk - 1)

        squares = add_four(1, chunk, squares, top)
        second(0, chunk)
        return squares

    drain(master, load_sem.at[0])
    zero = jnp.zeros((8, 128), F32)
    top_squares = lax.fori_loop(0, N_TOP, functools.partial(first_sums, top=True), zero)
    bot_squares = lax.fori_loop(N_TOP, N_CHUNK, functools.partial(first_sums, top=False), zero)
    second(1, N_CHUNK - 1)

    def finish(chunk, squares, top):
        for route in range(2):
            drain(got.at[route, chunk], second_recv.at[route, chunk])

            def body(cols, total):
                value = (mean[route, chunk, :, cols] + got[route, chunk, :, cols]) * 0.125
                mean[route, chunk, :, cols] = value
                return fold(total, value * value)

            squares = strips(body, squares)
            load(two_in, two, load_sem.at[2 + int(top)], route, chunk, top)
        return squares

    everyone = [(row, data_index(*chip, side)) for row, chip in (
        (flip(model_pos), chips[3]), (flip(model_pos), chips[2]), (flip(model_pos), chips[1]), (model_pos, chips[3]),
        (flip(model_pos), chips[0]), (model_pos, chips[2]), (model_pos, chips[1]),
    ) for side in (core, flip(core))] + [(model_pos, partner)]

    def share_all(box, send_sem, recv_sem):
        for device in everyone:
            pltpu.make_async_remote_copy(src_ref=box.at[mine], dst_ref=box.at[mine], send_sem=send_sem, recv_sem=recv_sem, device_id=device, device_id_type=MESH).start()

    total_box[mine] = jnp.sum(sweep(finish, zero), axis=0, keepdims=True)
    pl.semaphore_wait(known, 1)
    share_all(total_box, box_sem.at[0], box_sem.at[1])
    drain(total_box.at[pl.ds(0, 15)], box_sem.at[1])
    total = jnp.sum(jnp.sum(total_box[...], axis=0), keepdims=True)
    clip = jnp.minimum(1.0, MAX_NORM / jnp.sqrt(total))
    one_scale, two_scale = clip * (1.0 - BETA_ONE), clip * (1.0 - BETA_TWO) ** 0.5

    def update(route, chunk, carry):
        def body(cols, total):
            place = (route, chunk, slice(None), cols)
            weight = master[place]
            value = mean[place]
            new_one = BETA_ONE * one[place] + one_scale * value
            change = two_scale * value
            new_two = BETA_TWO * two[place] + change * change
            one[place] = new_one
            two[place] = new_two
            floor = jnp.maximum(new_two, TINY)
            root = floor * lax.rsqrt(floor)
            direction = (new_one * (CORR_TWO ** 0.5 / CORR_ONE)) / (root + EPSILON * CORR_TWO ** 0.5) + WEIGHT_DECAY * weight
            mean[place] = direction
            return fold(total, direction * direction)

        return strips(body, carry, UPDATE_STRIP)

    def update_rows(index, low, high):
        drain(two.at[:, pl.ds(low, high - low)], load_sem.at[2 + index])
        return lax.fori_loop(low, high, lambda chunk, total: update(1, chunk, update(0, chunk, total)), zero)

    def share_norms(index, box, rows):
        for position, value in enumerate(rows):
            box[mine, position:position + 1] = value
        share_all(box, box_sem.at[2 + index], box_sem.at[4 + index])

    def norm_rows(index, box):
        drain(box.at[pl.ds(0, 15)], box_sem.at[4 + index])
        return jnp.sqrt(jnp.sum(jnp.sum(box[...], axis=0), axis=1, keepdims=True))

    def bot_rate():
        norms = norm_rows(0, bot_box)
        return LEARN_RATE * (norms[0:1] / norms[1:2]) + jnp.zeros((8, 1), F32)

    def top_rate():
        norms = norm_rows(1, top_box)
        rates = [LEARN_RATE * (norms[position:position + 1] / norms[position + 3:position + 4]) for position in range(3)]
        row = lax.broadcasted_iota(jnp.int32, (8, 1), 0)
        return jnp.where(row < 3, rates[0], jnp.where(row == 3, rates[1], rates[2]))

    def tensor_rows(squares):
        row = lax.broadcasted_iota(jnp.int32, (8, 128), 0)
        return [jnp.sum(jnp.where(mask, squares, 0.0), axis=0, keepdims=True) for mask in (row < 3, row == 3, row > 3)]

    drain(one, load_sem.at[1])
    share_norms(0, bot_box, [jnp.sum(squares, axis=0, keepdims=True) for squares in (bot_squares, update_rows(0, N_TOP, N_CHUNK))])
    share_norms(1, top_box, tensor_rows(top_squares) + tensor_rows(update_rows(1, 0, N_TOP)))

    def piece(place, route, chunk, top):
        if top:
            start = place * SHARD + route * TOP_ROUTE + chunk * COLS
        else:
            start = place * (SHARD // 2) + route * BOT_ROUTE + (chunk - N_TOP) * COLS
        return (top_out if top else bot_out).at[:, pl.ds(pl.multiple_of(start, COLS), COLS)]

    def part(place, top, share=1):
        size = SHARD if top else SHARD // 2
        return (top_out if top else bot_out).at[:, pl.ds(pl.multiple_of(place * size, size), size // share)]

    def weights(route, chunk, rate, top):
        view = piece(places[0], route, chunk, top)

        def body(cols, carry):
            place = (route, chunk, slice(None), cols)
            value = master[place] - rate * mean[place]
            master[place] = value
            view[:, cols] = value.astype(BF16)
            return carry

        strips(body)

    def send(route, chunk, top):
        view = piece(places[0], route, chunk, top)
        kind = int(top)
        for axis in range(2):
            copy_to(view, view, places[1 + axis], side_send.at[axis, kind], near_recv.at[axis, route, chunk])
        copy_to(view, view, partner, partner_send.at[0, kind], partner_recv.at[0, kind])

    def own(chunk, rate, top):
        weights(0, chunk, rate, top)

        @pl.when(chunk > (0 if top else N_TOP))
        def _():
            send(1, chunk - 1, top)

        weights(1, chunk, rate, top)
        send(0, chunk, top)

        @pl.when(chunk == (N_TOP - 1 if top else N_CHUNK - 1))
        def _():
            send(1, chunk, top)

        return rate

    def hand_on(chunk, carry, top):
        kind = int(top)
        for route in range(2):
            for axis in range(2):
                view = piece(places[1 + axis], route, chunk, top)
                drain(view, near_recv.at[axis, route, chunk])
                if axis == route:
                    copy_to(view, view, places[2 - axis], forward_send.at[route, kind], corner_recv.at[route, chunk])
                copy_to(view, view, partner, partner_send.at[1 + axis, kind], partner_recv.at[1 + axis, kind])
        return carry

    def corner(chunk, carry, top):
        for route in range(2):
            view = piece(places[3], route, chunk, top)
            drain(view, corner_recv.at[route, chunk])
            copy_to(view, view, partner, partner_send.at[3, int(top)], partner_recv.at[3, int(top)])
        return carry

    def bottom_first(body, carry=0):
        carry = lax.fori_loop(N_TOP, N_CHUNK, functools.partial(body, top=False), carry)
        return lax.fori_loop(0, N_TOP, functools.partial(body, top=True), carry)

    lax.fori_loop(N_TOP, N_CHUNK, functools.partial(own, top=False), bot_rate())
    lax.fori_loop(0, N_TOP, functools.partial(own, top=True), top_rate())
    bottom_first(hand_on)
    bottom_first(corner)

    for top in (True, False):
        kind = int(top)
        for axis in range(2):
            drain(part(places[0], top), side_send.at[axis, kind])
            drain(part(places[0], top, 2), forward_send.at[axis, kind])
        for chip, (row_pos, col_pos) in enumerate(chips):
            drain(part(places[chip], top), partner_send.at[chip, kind])
            drain(part(data_index(row_pos, col_pos, flip(core)), top), partner_recv.at[chip, kind])
    drain(total_box.at[pl.ds(0, 15)], box_sem.at[0])
    drain(bot_box.at[pl.ds(0, 15)], box_sem.at[2])
    drain(top_box.at[pl.ds(0, 15)], box_sem.at[3])

    drain(top_out.at[:, pl.ds(0, 6 * SHARD)], first_send.at[1])
    drain(bot_out.at[:, pl.ds(0, 3 * SHARD)], first_send.at[0])
    drain(sent, second_send)


def in_hbm(array):
    return pltpu.with_memory_space_constraint(array, pltpu.HBM)


def run_step(local_grads, master, moment_one, moment_two):
    dma = pltpu.SemaphoreType.DMA
    block = pltpu.VMEM((2, N_CHUNK, 8, COLS), F32)
    return pl.pallas_call(
        step_kernel,
        out_shape=(pltpu.VMEM((8, 8 * SHARD), BF16), pltpu.VMEM((8, 4 * SHARD), BF16), block, block, block),
        in_specs=[pl.BlockSpec(memory_space=pltpu.HBM)] * 4,
        out_specs=(pl.BlockSpec(memory_space=pltpu.VMEM),) * 5,
        scratch_shapes=[
            block, block,
            pltpu.VMEM((16, 1, 128), F32),
            pltpu.VMEM((16, 2, 128), F32),
            pltpu.VMEM((16, 6, 128), F32),
            dma((2, 2, N_CHUNK)), dma((2, N_CHUNK)), dma((2,)), dma, dma((4,)), dma((2, 2)), dma((2, 2)), dma((4, 2)), dma((4, 2)), dma((6,)),
            pltpu.SemaphoreType.REGULAR, pltpu.SemaphoreType.REGULAR,
        ],
        compiler_params=pltpu.CompilerParams(collective_id=0, has_side_effects=True, vmem_limit_bytes=STEP_LIMIT),
        name='lamb_step',
    )(in_hbm(local_grads), in_hbm(master), in_hbm(moment_one), in_hbm(moment_two))


def write_kernel(top, bot, master, one, two, params_out, master_out, one_out, two_out, sem):
    copies = []
    for place in range(8):
        copies.append((top.at[:, pl.ds(place * SHARD, SHARD)], params_out.at[pl.ds(0, 8), pl.ds(place * SHARD, SHARD)]))
        for half in range(2):
            copies.append((bot.at[pl.ds(4 * half, 4), pl.ds(place * TOP_ROUTE, TOP_ROUTE)], params_out.at[pl.ds(8, 4), pl.ds(place * SHARD + half * TOP_ROUTE, TOP_ROUTE)]))
    for block, array in ((master, master_out), (one, one_out), (two, two_out)):
        for route in range(2):
            for chunk in range(N_CHUNK):
                copies += [(src, dst) for dst, src in row_views(array, 0, route, chunk, block.at[route, chunk], chunk < N_TOP)]
    for src, dst in copies:
        pltpu.make_async_copy(src, dst, sem).start()
    for src, dst in copies:
        pltpu.make_async_copy(src, dst, sem).wait()


def write_out(*blocks):
    state = jax.ShapeDtypeStruct((12, SHARD), F32)
    return pl.pallas_call(
        write_kernel,
        out_shape=(jax.ShapeDtypeStruct((12, 8 * SHARD), BF16), state, state, state),
        in_specs=[pl.BlockSpec(memory_space=pltpu.VMEM)] * 5,
        out_specs=(pl.BlockSpec(memory_space=pltpu.HBM),) * 4,
        scratch_shapes=[pltpu.SemaphoreType.DMA],
        compiler_params=pltpu.CompilerParams(vmem_limit_bytes=WRITE_LIMIT),
        name='write_out',
    )(*[pltpu.with_memory_space_constraint(block, pltpu.VMEM) for block in blocks])


def solution(mesh):
    state_spec = P(None, ('model', 'data'))

    def device_step(local_grads, master, moment_one, moment_two):
        return write_out(*run_step(local_grads, master, moment_one, moment_two))

    return jax.shard_map(device_step, mesh=mesh, in_specs=(P('data', None, 'model'), state_spec, state_spec, state_spec), out_specs=(P(None, 'model'), state_spec, state_spec, state_spec), check_vma=False)
```

```python
import functools

import jax
import jax.numpy as jnp
from jax import lax
from jax.experimental import pallas as pl
from jax.experimental.pallas import tpu as pltpu
from jax.sharding import PartitionSpec as P

STEP = 4
LEARN_RATE = 0.08
BETA_ONE = 0.9
BETA_TWO = 0.999
EPSILON = 1e-6
WEIGHT_DECAY = 0.01
MAX_NORM = 1.0
CORR_ONE = 1.0 - BETA_ONE ** STEP
CORR_TWO = 1.0 - BETA_TWO ** STEP

MESH = pl.DeviceIdType.MESH
F32 = jnp.float32
BF16 = jnp.bfloat16

SHARD = 147456
COLS = 6144
TOP_ROUTE = SHARD // 2
BOT_ROUTE = SHARD // 4
N_TOP = TOP_ROUTE // COLS
N_BOT = BOT_ROUTE // COLS
N_CHUNK = N_TOP + N_BOT
STRIP = 1024
UPDATE_STRIP = 2048

TINY = 1.2e-38
MIB = 1024 * 1024
STEP_LIMIT = 15 * MIB
WRITE_LIMIT = STEP_LIMIT


def flip(value):
    return 1 - value


def my_place():
    data_pos = lax.axis_index('data')
    return data_pos // 4, lax.rem(data_pos // 2, 2), lax.rem(data_pos, 2)


def data_index(pos_y, pos_x, core):
    return (pos_y * 2 + pos_x) * 2 + core


def drain(ref, sem):
    pltpu.make_async_copy(ref, ref, sem).wait()


def row_views(array, shard, route, chunk, block, top):
    if top:
        start = shard * SHARD + route * TOP_ROUTE + chunk * COLS
        return [(array.at[pl.ds(0, 8), pl.ds(pl.multiple_of(start, COLS), COLS)], block)]
    views = []
    for half in range(2):
        start = shard * SHARD + half * TOP_ROUTE + route * BOT_ROUTE + (chunk - N_TOP) * COLS
        views.append((array.at[pl.ds(8, 4), pl.ds(pl.multiple_of(start, COLS), COLS)], block.at[pl.ds(4 * half, 4)]))
    return views


def sweep(body, carry=0):
    carry = lax.fori_loop(0, N_TOP, functools.partial(body, top=True), carry)
    return lax.fori_loop(N_TOP, N_CHUNK, functools.partial(body, top=False), carry)


def strips(body, carry=0, width=STRIP):
    def step(strip, carry):
        return body(pl.ds(pl.multiple_of(strip * width, width), width), carry)

    return lax.fori_loop(0, COLS // width, step, carry)


def fold(total, values):
    for tile in range(values.shape[1] // 128):
        total = total + values[:, tile * 128:(tile + 1) * 128]
    return total


def step_kernel(
    grads, master_in, one_in, two_in,
    top_out, bot_out, master, one, two,
    mean, sent, total_box, bot_box, top_box,
    near_recv, corner_recv, first_send, second_send, load_sem, side_send, forward_send, partner_send, partner_recv, box_sem, seen, known,
):
    pos_y, pos_x, core = my_place()
    model_pos = lax.axis_index('model')
    mine = model_pos * 8 + lax.axis_index('data')
    grad = grads.at[0]
    got = two
    first_recv, second_recv = near_recv.at[0], near_recv.at[1]
    chips = ((pos_y, pos_x), (pos_y, flip(pos_x)), (flip(pos_y), pos_x), (flip(pos_y), flip(pos_x)))
    places = [data_index(row, col, core) for row, col in chips]
    partner = data_index(pos_y, pos_x, flip(core))

    def copy_to(src, dst, place, send_sem, recv_sem):
        pltpu.make_async_remote_copy(src_ref=src, dst_ref=dst, send_sem=send_sem, recv_sem=recv_sem, device_id=(model_pos, place), device_id_type=MESH).start()

    def landing(route, chunk, block, count, top):
        if top:
            start = ((route * N_TOP + chunk) * 8 + block) * COLS
        else:
            start = ((route * N_BOT + chunk - N_TOP) * 8 + block) * COLS
        return (top_out if top else bot_out).at[:, pl.ds(pl.multiple_of(start, COLS), count * COLS)]

    def wanted(route, row, col, far):
        return (lax.rem(row + far, 2), col) if route == 0 else (row, lax.rem(col + far, 2))

    def local(chunk, carry, top):
        for route in range(2):
            for far in range(2):
                shard = data_index(*wanted(route, pos_y, pos_x, far), core)
                for src, dst in row_views(grad, shard, route, chunk, landing(route, chunk, far, 1, top), top):
                    pltpu.make_async_copy(src, dst, first_recv.at[route, chunk]).start()
        return carry

    def remote(chunk, carry, top):
        for far in range(2):
            for other in range(2):
                for route in range(2):
                    row, col = chips[1 + route]
                    to_core = lax.rem(core + other, 2)
                    shard = data_index(*wanted(route, row, col, far), to_core)
                    for src, dst in row_views(grad, shard, route, chunk, landing(route, chunk, 4 + 2 * other + far, 1, top), top):
                        copy_to(src, dst, data_index(row, col, to_core), first_send.at[int(top)], first_recv.at[route, chunk])
            for route in range(2):
                shard = data_index(*wanted(route, pos_y, pos_x, far), flip(core))
                for src, dst in row_views(grad, shard, route, chunk, landing(route, chunk, 2 + far, 1, top), top):
                    copy_to(src, dst, partner, first_send.at[int(top)], first_recv.at[route, chunk])
        return carry

    def load(array, block, sem, route, chunk, top):
        for src, dst in row_views(array, 0, route, chunk, block.at[route, chunk], top):
            pltpu.make_async_copy(src, dst, sem).start()

    next_to = [(model_pos, place) for chip in (1, 2) for place in (places[chip], data_index(*chips[chip], flip(core)))] + [(model_pos, partner), (flip(model_pos), places[0])]

    def tell(sem, devices):
        for device in devices:
            pl.semaphore_signal(sem, inc=1, device_id=device, device_id_type=MESH)

    barrier = pltpu.get_barrier_semaphore()
    tell(barrier, next_to)
    sweep(local)
    pl.semaphore_wait(barrier, len(next_to))
    sweep(remote)
    tell(seen, next_to)

    def load_state(chunk, carry, top):
        for route in range(2):
            load(master_in, master, load_sem.at[0], route, chunk, top)
            load(one_in, one, load_sem.at[1], route, chunk, top)
        return carry

    sweep(load_state)
    pl.semaphore_wait(seen, len(next_to))
    tell(known, next_to[-1:])

    def second(route, chunk):
        copy_to(sent.at[route, chunk], got.at[route, chunk], places[2 - route], second_send, second_recv.at[route, chunk])

    def add_four(route, chunk, squares, top):
        drain(landing(route, chunk, 0, 8, top), first_recv.at[route, chunk])

        def body(cols, total):
            for far, target in ((0, mean), (1, sent)):
                parts = [landing(route, chunk, 2 * source + far, 1, top)[:, cols].astype(F32) for source in range(4)]
                target[route, chunk, :, cols] = (parts[0] + parts[1]) + (parts[2] + parts[3])
            weight = master[route, chunk, :, cols]
            return fold(total, weight * weight)

        return strips(body, squares)

    def first_sums(chunk, squares, top):
        squares = add_four(0, chunk, squares, top)

        @pl.when(chunk > 0)
        def _():
            second(1, chunk - 1)

        squares = add_four(1, chunk, squares, top)
        second(0, chunk)
        return squares

    drain(master, load_sem.at[0])
    zero = jnp.zeros((8, 128), F32)
    top_squares = lax.fori_loop(0, N_TOP, functools.partial(first_sums, top=True), zero)
    bot_squares = lax.fori_loop(N_TOP, N_CHUNK, functools.partial(first_sums, top=False), zero)
    second(1, N_CHUNK - 1)

    def finish(chunk, squares, top):
        for route in range(2):
            drain(got.at[route, chunk], second_recv.at[route, chunk])

            def body(cols, total):
                value = (mean[route, chunk, :, cols] + got[route, chunk, :, cols]) * 0.125
                mean[route, chunk, :, cols] = value
                return fold(total, value * value)

            squares = strips(body, squares)
            load(two_in, two, load_sem.at[2 + int(top)], route, chunk, top)
        return squares

    everyone = [(row, data_index(*chip, side)) for row, chip in (
        (flip(model_pos), chips[3]), (flip(model_pos), chips[2]), (flip(model_pos), chips[1]), (model_pos, chips[3]),
        (flip(model_pos), chips[0]), (model_pos, chips[2]), (model_pos, chips[1]),
    ) for side in (core, flip(core))] + [(model_pos, partner)]

    def share_all(box, send_sem, recv_sem):
        for device in everyone:
            pltpu.make_async_remote_copy(src_ref=box.at[mine], dst_ref=box.at[mine], send_sem=send_sem, recv_sem=recv_sem, device_id=device, device_id_type=MESH).start()

    total_box[mine] = jnp.sum(sweep(finish, zero), axis=0, keepdims=True)
    pl.semaphore_wait(known, 1)
    share_all(total_box, box_sem.at[0], box_sem.at[1])
    drain(total_box.at[pl.ds(0, 15)], box_sem.at[1])
    total = jnp.sum(jnp.sum(total_box[...], axis=0), keepdims=True)
    clip = jnp.minimum(1.0, MAX_NORM / jnp.sqrt(total))
    one_scale, two_scale = clip * (1.0 - BETA_ONE), clip * (1.0 - BETA_TWO) ** 0.5

    def update(route, chunk, carry):
        def body(cols, total):
            place = (route, chunk, slice(None), cols)
            weight = master[place]
            value = mean[place]
            new_one = BETA_ONE * one[place] + one_scale * value
            change = two_scale * value
            new_two = BETA_TWO * two[place] + change * change
            one[place] = new_one
            two[place] = new_two
            floor = jnp.maximum(new_two, TINY)
            root = floor * lax.rsqrt(floor)
            direction = (new_one * (CORR_TWO ** 0.5 / CORR_ONE)) / (root + EPSILON * CORR_TWO ** 0.5) + WEIGHT_DECAY * weight
            mean[place] = direction
            return fold(total, direction * direction)

        return strips(body, carry, UPDATE_STRIP)

    def update_rows(index, low, high):
        drain(two.at[:, pl.ds(low, high - low)], load_sem.at[2 + index])
        return lax.fori_loop(low, high, lambda chunk, total: update(1, chunk, update(0, chunk, total)), zero)

    def share_norms(index, box, rows):
        for position, value in enumerate(rows):
            box[mine, position:position + 1] = value
        share_all(box, box_sem.at[2 + index], box_sem.at[4 + index])

    def norm_rows(index, box):
        drain(box.at[pl.ds(0, 15)], box_sem.at[4 + index])
        return jnp.sqrt(jnp.sum(jnp.sum(box[...], axis=0), axis=1, keepdims=True))

    def bot_rate():
        norms = norm_rows(0, bot_box)
        return LEARN_RATE * (norms[0:1] / norms[1:2]) + jnp.zeros((8, 1), F32)

    def top_rate():
        norms = norm_rows(1, top_box)
        rates = [LEARN_RATE * (norms[position:position + 1] / norms[position + 3:position + 4]) for position in range(3)]
        row = lax.broadcasted_iota(jnp.int32, (8, 1), 0)
        return jnp.where(row < 3, rates[0], jnp.where(row == 3, rates[1], rates[2]))

    def tensor_rows(squares):
        row = lax.broadcasted_iota(jnp.int32, (8, 128), 0)
        return [jnp.sum(jnp.where(mask, squares, 0.0), axis=0, keepdims=True) for mask in (row < 3, row == 3, row > 3)]

    drain(one, load_sem.at[1])
    share_norms(0, bot_box, [jnp.sum(squares, axis=0, keepdims=True) for squares in (bot_squares, update_rows(0, N_TOP, N_CHUNK))])
    share_norms(1, top_box, tensor_rows(top_squares) + tensor_rows(update_rows(1, 0, N_TOP)))

    def piece(place, route, chunk, top):
        if top:
            start = place * SHARD + route * TOP_ROUTE + chunk * COLS
        else:
            start = place * (SHARD // 2) + route * BOT_ROUTE + (chunk - N_TOP) * COLS
        return (top_out if top else bot_out).at[:, pl.ds(pl.multiple_of(start, COLS), COLS)]

    def part(place, top, share=1):
        size = SHARD if top else SHARD // 2
        return (top_out if top else bot_out).at[:, pl.ds(pl.multiple_of(place * size, size), size // share)]

    def weights(route, chunk, rate, top):
        view = piece(places[0], route, chunk, top)

        def body(cols, carry):
            place = (route, chunk, slice(None), cols)
            value = master[place] - rate * mean[place]
            master[place] = value
            view[:, cols] = value.astype(BF16)
            return carry

        strips(body)

    def send(route, chunk, top):
        view = piece(places[0], route, chunk, top)
        kind = int(top)
        for axis in range(2):
            copy_to(view, view, places[1 + axis], side_send.at[axis, kind], near_recv.at[axis, route, chunk])
        copy_to(view, view, partner, partner_send.at[0, kind], partner_recv.at[0, kind])

    def own(chunk, rate, top):
        weights(0, chunk, rate, top)

        @pl.when(chunk > (0 if top else N_TOP))
        def _():
            send(1, chunk - 1, top)

        weights(1, chunk, rate, top)
        send(0, chunk, top)

        @pl.when(chunk == (N_TOP - 1 if top else N_CHUNK - 1))
        def _():
            send(1, chunk, top)

        return rate

    def hand_on(chunk, carry, top):
        kind = int(top)
        for route in range(2):
            for axis in range(2):
                view = piece(places[1 + axis], route, chunk, top)
                drain(view, near_recv.at[axis, route, chunk])
                if axis == route:
                    copy_to(view, view, places[2 - axis], forward_send.at[route, kind], corner_recv.at[route, chunk])
                copy_to(view, view, partner, partner_send.at[1 + axis, kind], partner_recv.at[1 + axis, kind])
        return carry

    def corner(chunk, carry, top):
        for route in range(2):
            view = piece(places[3], route, chunk, top)
            drain(view, corner_recv.at[route, chunk])
            copy_to(view, view, partner, partner_send.at[3, int(top)], partner_recv.at[3, int(top)])
        return carry

    def bottom_first(body, carry=0):
        carry = lax.fori_loop(N_TOP, N_CHUNK, functools.partial(body, top=False), carry)
        return lax.fori_loop(0, N_TOP, functools.partial(body, top=True), carry)

    lax.fori_loop(N_TOP, N_CHUNK, functools.partial(own, top=False), bot_rate())
    lax.fori_loop(0, N_TOP, functools.partial(own, top=True), top_rate())
    bottom_first(hand_on)
    bottom_first(corner)

    for top in (True, False):
        kind = int(top)
        for axis in range(2):
            drain(part(places[0], top), side_send.at[axis, kind])
            drain(part(places[0], top, 2), forward_send.at[axis, kind])
        for chip, (row_pos, col_pos) in enumerate(chips):
            drain(part(places[chip], top), partner_send.at[chip, kind])
            drain(part(data_index(row_pos, col_pos, flip(core)), top), partner_recv.at[chip, kind])
    drain(total_box.at[pl.ds(0, 15)], box_sem.at[0])
    drain(bot_box.at[pl.ds(0, 15)], box_sem.at[2])
    drain(top_box.at[pl.ds(0, 15)], box_sem.at[3])

    drain(top_out.at[:, pl.ds(0, 6 * SHARD)], first_send.at[1])
    drain(bot_out.at[:, pl.ds(0, 3 * SHARD)], first_send.at[0])
    drain(sent, second_send)


def in_hbm(array):
    return pltpu.with_memory_space_constraint(array, pltpu.HBM)


def run_step(local_grads, master, moment_one, moment_two):
    dma = pltpu.SemaphoreType.DMA
    block = pltpu.VMEM((2, N_CHUNK, 8, COLS), F32)
    return pl.pallas_call(
        step_kernel,
        out_shape=(pltpu.VMEM((8, 8 * SHARD), BF16), pltpu.VMEM((8, 4 * SHARD), BF16), block, block, block),
        in_specs=[pl.BlockSpec(memory_space=pltpu.HBM)] * 4,
        out_specs=(pl.BlockSpec(memory_space=pltpu.VMEM),) * 5,
        scratch_shapes=[
            block, block,
            pltpu.VMEM((16, 1, 128), F32),
            pltpu.VMEM((16, 2, 128), F32),
            pltpu.VMEM((16, 6, 128), F32),
            dma((2, 2, N_CHUNK)), dma((2, N_CHUNK)), dma((2,)), dma, dma((4,)), dma((2, 2)), dma((2, 2)), dma((4, 2)), dma((4, 2)), dma((6,)),
            pltpu.SemaphoreType.REGULAR, pltpu.SemaphoreType.REGULAR,
        ],
        compiler_params=pltpu.CompilerParams(collective_id=0, has_side_effects=True, vmem_limit_bytes=STEP_LIMIT),
        name='lamb_step',
    )(in_hbm(local_grads), in_hbm(master), in_hbm(moment_one), in_hbm(moment_two))


def write_kernel(top, bot, master, one, two, params_out, master_out, one_out, two_out, sem):
    copies = []
    for place in range(8):
        copies.append((top.at[:, pl.ds(place * SHARD, SHARD)], params_out.at[pl.ds(0, 8), pl.ds(place * SHARD, SHARD)]))
        for half in range(2):
            copies.append((bot.at[pl.ds(4 * half, 4), pl.ds(place * TOP_ROUTE, TOP_ROUTE)], params_out.at[pl.ds(8, 4), pl.ds(place * SHARD + half * TOP_ROUTE, TOP_ROUTE)]))
    for block, array in ((master, master_out), (one, one_out), (two, two_out)):
        for route in range(2):
            for chunk in range(N_CHUNK):
                copies += [(src, dst) for dst, src in row_views(array, 0, route, chunk, block.at[route, chunk], chunk < N_TOP)]
    for src, dst in copies:
        pltpu.make_async_copy(src, dst, sem).start()
    for src, dst in copies:
        pltpu.make_async_copy(src, dst, sem).wait()


def write_out(*blocks):
    state = jax.ShapeDtypeStruct((12, SHARD), F32)
    return pl.pallas_call(
        write_kernel,
        out_shape=(jax.ShapeDtypeStruct((12, 8 * SHARD), BF16), state, state, state),
        in_specs=[pl.BlockSpec(memory_space=pltpu.VMEM)] * 5,
        out_specs=(pl.BlockSpec(memory_space=pltpu.HBM),) * 4,
        scratch_shapes=[pltpu.SemaphoreType.DMA],
        compiler_params=pltpu.CompilerParams(vmem_limit_bytes=WRITE_LIMIT),
        name='write_out',
    )(*[pltpu.with_memory_space_constraint(block, pltpu.VMEM) for block in blocks])


def solution(mesh):
    state_spec = P(None, ('model', 'data'))

    def device_step(local_grads, master, moment_one, moment_two):
        return write_out(*run_step(local_grads, master, moment_one, moment_two))

    return jax.shard_map(device_step, mesh=mesh, in_specs=(P('data', None, 'model'), state_spec, state_spec, state_spec), out_specs=(P(None, 'model'), state_spec, state_spec, state_spec), check_vma=False)
```

```python
import functools

import jax
import jax.numpy as jnp
from jax import lax
from jax.experimental import pallas as pl
from jax.experimental.pallas import tpu as pltpu
from jax.sharding import PartitionSpec as P

STEP = 4
LEARN_RATE = 0.08
BETA_ONE = 0.9
BETA_TWO = 0.999
EPSILON = 1e-6
WEIGHT_DECAY = 0.01
MAX_NORM = 1.0
CORR_ONE = 1.0 - BETA_ONE ** STEP
CORR_TWO = 1.0 - BETA_TWO ** STEP

MESH = pl.DeviceIdType.MESH
F32 = jnp.float32
BF16 = jnp.bfloat16

SHARD = 147456
COLS = 6144
TOP_ROUTE = SHARD // 2
BOT_ROUTE = SHARD // 4
N_TOP = TOP_ROUTE // COLS
N_BOT = BOT_ROUTE // COLS
N_CHUNK = N_TOP + N_BOT
HOLD = N_CHUNK - 2
STRIP = 1024
UPDATE_STRIP = 2048

TINY = 1.2e-38
MIB = 1024 * 1024
STEP_LIMIT = 15 * MIB
WRITE_LIMIT = STEP_LIMIT


def flip(value):
    return 1 - value


def my_place():
    data_pos = lax.axis_index('data')
    return data_pos // 4, lax.rem(data_pos // 2, 2), lax.rem(data_pos, 2)


def data_index(pos_y, pos_x, core):
    return (pos_y * 2 + pos_x) * 2 + core


def drain(ref, sem):
    pltpu.make_async_copy(ref, ref, sem).wait()


def row_views(array, shard, route, chunk, block, top):
    if top:
        start = shard * SHARD + route * TOP_ROUTE + chunk * COLS
        return [(array.at[pl.ds(0, 8), pl.ds(pl.multiple_of(start, COLS), COLS)], block)]
    views = []
    for half in range(2):
        start = shard * SHARD + half * TOP_ROUTE + route * BOT_ROUTE + (chunk - N_TOP) * COLS
        views.append((array.at[pl.ds(8, 4), pl.ds(pl.multiple_of(start, COLS), COLS)], block.at[pl.ds(4 * half, 4)]))
    return views


def sweep(body, carry=0):
    carry = lax.fori_loop(0, N_TOP, functools.partial(body, top=True), carry)
    return lax.fori_loop(N_TOP, N_CHUNK, functools.partial(body, top=False), carry)


def strips(body, carry=0, width=STRIP):
    def step(strip, carry):
        return body(pl.ds(pl.multiple_of(strip * width, width), width), carry)

    return lax.fori_loop(0, COLS // width, step, carry)


def fold(total, values):
    for tile in range(values.shape[1] // 128):
        total = total + values[:, tile * 128:(tile + 1) * 128]
    return total


def step_kernel(
    grads, master_in, one_in, two_in,
    top_out, bot_out, master, one, two,
    mean, sent, total_box, bot_box, top_box,
    near_recv, corner_recv, first_send, second_send, load_sem, side_send, forward_send, partner_send, partner_recv, box_sem, seen, known,
):
    pos_y, pos_x, core = my_place()
    model_pos = lax.axis_index('model')
    mine = model_pos * 8 + lax.axis_index('data')
    grad = grads.at[0]
    got = two
    first_recv, second_recv = near_recv.at[0], near_recv.at[1]
    chips = ((pos_y, pos_x), (pos_y, flip(pos_x)), (flip(pos_y), pos_x), (flip(pos_y), flip(pos_x)))
    places = [data_index(row, col, core) for row, col in chips]
    partner = data_index(pos_y, pos_x, flip(core))

    def copy_to(src, dst, place, send_sem, recv_sem):
        pltpu.make_async_remote_copy(src_ref=src, dst_ref=dst, send_sem=send_sem, recv_sem=recv_sem, device_id=(model_pos, place), device_id_type=MESH).start()

    def landing(route, chunk, block, count, top):
        if top:
            start = ((route * N_TOP + chunk) * 8 + block) * COLS
        else:
            start = ((route * N_BOT + chunk - N_TOP) * 8 + block) * COLS
        return (top_out if top else bot_out).at[:, pl.ds(pl.multiple_of(start, COLS), count * COLS)]

    def wanted(route, row, col, far):
        return (lax.rem(row + far, 2), col) if route == 0 else (row, lax.rem(col + far, 2))

    def local(chunk, carry, top):
        for route in range(2):
            for far in range(2):
                shard = data_index(*wanted(route, pos_y, pos_x, far), core)
                for src, dst in row_views(grad, shard, route, chunk, landing(route, chunk, far, 1, top), top):
                    pltpu.make_async_copy(src, dst, first_recv.at[route, chunk]).start()
        return carry

    def remote(chunk, carry, top):
        for far in range(2):
            for other in range(2):
                for route in range(2):
                    row, col = chips[1 + route]
                    to_core = lax.rem(core + other, 2)
                    shard = data_index(*wanted(route, row, col, far), to_core)
                    for src, dst in row_views(grad, shard, route, chunk, landing(route, chunk, 4 + 2 * other + far, 1, top), top):
                        copy_to(src, dst, data_index(row, col, to_core), first_send.at[int(top)], first_recv.at[route, chunk])
            for route in range(2):
                shard = data_index(*wanted(route, pos_y, pos_x, far), flip(core))
                for src, dst in row_views(grad, shard, route, chunk, landing(route, chunk, 2 + far, 1, top), top):
                    copy_to(src, dst, partner, first_send.at[int(top)], first_recv.at[route, chunk])
        return carry

    def load(array, block, sem, route, chunk, top):
        for src, dst in row_views(array, 0, route, chunk, block.at[route, chunk], top):
            pltpu.make_async_copy(src, dst, sem).start()

    next_to = [(model_pos, place) for chip in (1, 2) for place in (places[chip], data_index(*chips[chip], flip(core)))] + [(model_pos, partner), (flip(model_pos), places[0])]

    def tell(sem, devices):
        for device in devices:
            pl.semaphore_signal(sem, inc=1, device_id=device, device_id_type=MESH)

    barrier = pltpu.get_barrier_semaphore()
    tell(barrier, next_to)
    sweep(local)
    pl.semaphore_wait(barrier, len(next_to))
    sweep(remote)
    tell(seen, next_to)

    def load_state(chunk, carry, top):
        for route in range(2):
            load(master_in, master, load_sem.at[0], route, chunk, top)
            load(one_in, one, load_sem.at[1], route, chunk, top)
        return carry

    sweep(load_state)
    pl.semaphore_wait(seen, len(next_to))
    tell(known, next_to[-1:])

    def second(route, chunk):
        copy_to(sent.at[route, chunk], got.at[route, chunk], places[2 - route], second_send, second_recv.at[route, chunk])

    def add_four(route, chunk, squares, top):
        drain(landing(route, chunk, 0, 8, top), first_recv.at[route, chunk])

        def body(cols, total):
            for far, target in ((0, mean), (1, sent)):
                parts = [landing(route, chunk, 2 * source + far, 1, top)[:, cols].astype(F32) for source in range(4)]
                target[route, chunk, :, cols] = (parts[0] + parts[1]) + (parts[2] + parts[3])
            weight = master[route, chunk, :, cols]
            return fold(total, weight * weight)

        return strips(body, squares)

    def first_sums(chunk, squares, top):
        squares = add_four(1, chunk, add_four(0, chunk, squares, top), top)

        @pl.when(chunk >= HOLD)
        def _():
            second(0, chunk - HOLD)
            second(1, chunk - HOLD)

        return squares

    drain(master, load_sem.at[0])
    zero = jnp.zeros((8, 128), F32)
    top_squares = lax.fori_loop(0, N_TOP, functools.partial(first_sums, top=True), zero)
    bot_squares = lax.fori_loop(N_TOP, N_CHUNK, functools.partial(first_sums, top=False), zero)

    @pl.loop(N_CHUNK - HOLD, N_CHUNK)
    def _(chunk):
        second(0, chunk)
        second(1, chunk)

    def finish(chunk, squares, top):
        for route in range(2):
            drain(got.at[route, chunk], second_recv.at[route, chunk])

            def body(cols, total):
                value = (mean[route, chunk, :, cols] + got[route, chunk, :, cols]) * 0.125
                mean[route, chunk, :, cols] = value
                return fold(total, value * value)

            squares = strips(body, squares)
            load(two_in, two, load_sem.at[2 + int(top)], route, chunk, top)
        return squares

    everyone = [(row, data_index(*chip, side)) for row, chip in (
        (flip(model_pos), chips[3]), (flip(model_pos), chips[2]), (flip(model_pos), chips[1]), (model_pos, chips[3]),
        (flip(model_pos), chips[0]), (model_pos, chips[2]), (model_pos, chips[1]),
    ) for side in (core, flip(core))] + [(model_pos, partner)]

    def share_all(box, send_sem, recv_sem):
        for device in everyone:
            pltpu.make_async_remote_copy(src_ref=box.at[mine], dst_ref=box.at[mine], send_sem=send_sem, recv_sem=recv_sem, device_id=device, device_id_type=MESH).start()

    total_box[mine] = jnp.sum(sweep(finish, zero), axis=0, keepdims=True)
    pl.semaphore_wait(known, 1)
    share_all(total_box, box_sem.at[0], box_sem.at[1])
    drain(total_box.at[pl.ds(0, 15)], box_sem.at[1])
    total = jnp.sum(jnp.sum(total_box[...], axis=0), keepdims=True)
    clip = jnp.minimum(1.0, MAX_NORM / jnp.sqrt(total))
    one_scale, two_scale = clip * (1.0 - BETA_ONE), clip * (1.0 - BETA_TWO) ** 0.5

    def update(route, chunk, carry):
        def body(cols, total):
            place = (route, chunk, slice(None), cols)
            weight = master[place]
            value = mean[place]
            new_one = BETA_ONE * one[place] + one_scale * value
            change = two_scale * value
            new_two = BETA_TWO * two[place] + change * change
            one[place] = new_one
            two[place] = new_two
            floor = jnp.maximum(new_two, TINY)
            root = floor * lax.rsqrt(floor)
            direction = (new_one * (CORR_TWO ** 0.5 / CORR_ONE)) / (root + EPSILON * CORR_TWO ** 0.5) + WEIGHT_DECAY * weight
            mean[place] = direction
            return fold(total, direction * direction)

        return strips(body, carry, UPDATE_STRIP)

    def update_rows(index, low, high):
        drain(two.at[:, pl.ds(low, high - low)], load_sem.at[2 + index])
        return lax.fori_loop(low, high, lambda chunk, total: update(1, chunk, update(0, chunk, total)), zero)

    def share_norms(index, box, rows):
        for position, value in enumerate(rows):
            box[mine, position:position + 1] = value
        share_all(box, box_sem.at[2 + index], box_sem.at[4 + index])

    def norm_rows(index, box):
        drain(box.at[pl.ds(0, 15)], box_sem.at[4 + index])
        return jnp.sqrt(jnp.sum(jnp.sum(box[...], axis=0), axis=1, keepdims=True))

    def bot_rate():
        norms = norm_rows(0, bot_box)
        return LEARN_RATE * (norms[0:1] / norms[1:2]) + jnp.zeros((8, 1), F32)

    def top_rate():
        norms = norm_rows(1, top_box)
        rates = [LEARN_RATE * (norms[position:position + 1] / norms[position + 3:position + 4]) for position in range(3)]
        row = lax.broadcasted_iota(jnp.int32, (8, 1), 0)
        return jnp.where(row < 3, rates[0], jnp.where(row == 3, rates[1], rates[2]))

    def tensor_rows(squares):
        row = lax.broadcasted_iota(jnp.int32, (8, 128), 0)
        return [jnp.sum(jnp.where(mask, squares, 0.0), axis=0, keepdims=True) for mask in (row < 3, row == 3, row > 3)]

    drain(one, load_sem.at[1])
    share_norms(0, bot_box, [jnp.sum(squares, axis=0, keepdims=True) for squares in (bot_squares, update_rows(0, N_TOP, N_CHUNK))])
    share_norms(1, top_box, tensor_rows(top_squares) + tensor_rows(update_rows(1, 0, N_TOP)))

    def piece(place, route, chunk, top):
        if top:
            start = place * SHARD + route * TOP_ROUTE + chunk * COLS
        else:
            start = place * (SHARD // 2) + route * BOT_ROUTE + (chunk - N_TOP) * COLS
        return (top_out if top else bot_out).at[:, pl.ds(pl.multiple_of(start, COLS), COLS)]

    def part(place, top, share=1):
        size = SHARD if top else SHARD // 2
        return (top_out if top else bot_out).at[:, pl.ds(pl.multiple_of(place * size, size), size // share)]

    def weights(route, chunk, rate, top):
        view = piece(places[0], route, chunk, top)

        def body(cols, carry):
            place = (route, chunk, slice(None), cols)
            value = master[place] - rate * mean[place]
            master[place] = value
            view[:, cols] = value.astype(BF16)
            return carry

        strips(body)

    def send(route, chunk, top):
        view = piece(places[0], route, chunk, top)
        kind = int(top)
        for axis in range(2):
            copy_to(view, view, places[1 + axis], side_send.at[axis, kind], near_recv.at[axis, route, chunk])
        copy_to(view, view, partner, partner_send.at[0, kind], partner_recv.at[0, kind])

    def own(chunk, rate, top):
        weights(0, chunk, rate, top)

        @pl.when(chunk > (0 if top else N_TOP))
        def _():
            send(1, chunk - 1, top)

        weights(1, chunk, rate, top)
        send(0, chunk, top)

        @pl.when(chunk == (N_TOP - 1 if top else N_CHUNK - 1))
        def _():
            send(1, chunk, top)

        return rate

    def hand_on(chunk, carry, top):
        kind = int(top)
        for route in range(2):
            for axis in range(2):
                view = piece(places[1 + axis], route, chunk, top)
                drain(view, near_recv.at[axis, route, chunk])
                copy_to(view, view, partner, partner_send.at[1 + axis, kind], partner_recv.at[1 + axis, kind])
        return carry

    def corner(chunk, carry, top):
        for route in range(2):
            view = piece(places[3], route, chunk, top)
            drain(view, corner_recv.at[route, chunk])
            copy_to(view, view, partner, partner_send.at[3, int(top)], partner_recv.at[3, int(top)])
        return carry

    def bottom_first(body, carry=0):
        carry = lax.fori_loop(N_TOP, N_CHUNK, functools.partial(body, top=False), carry)
        return lax.fori_loop(0, N_TOP, functools.partial(body, top=True), carry)

    lax.fori_loop(N_TOP, N_CHUNK, functools.partial(own, top=False), bot_rate())
    lax.fori_loop(0, N_TOP, functools.partial(own, top=True), top_rate())
    def hand_to_corner(chunk, carry, top):
        for route in range(2):
            view = piece(places[1 + route], route, chunk, top)
            copy_to(view, view, places[2 - route], forward_send.at[route, int(top)], corner_recv.at[route, chunk])
        return carry

    lax.fori_loop(N_TOP, N_CHUNK, functools.partial(hand_on, top=False), 0)
    lax.fori_loop(0, N_TOP - 2, functools.partial(hand_on, top=True), 0)
    lax.fori_loop(N_TOP, N_CHUNK, functools.partial(hand_to_corner, top=False), 0)
    lax.fori_loop(0, N_TOP - 2, functools.partial(hand_to_corner, top=True), 0)
    lax.fori_loop(N_TOP - 2, N_TOP, lambda chunk, carry: hand_to_corner(chunk, hand_on(chunk, carry, True), True), 0)
    bottom_first(corner)

    for top in (True, False):
        kind = int(top)
        for axis in range(2):
            drain(part(places[0], top), side_send.at[axis, kind])
            drain(part(places[0], top, 2), forward_send.at[axis, kind])
        for chip, (row_pos, col_pos) in enumerate(chips):
            drain(part(places[chip], top), partner_send.at[chip, kind])
            drain(part(data_index(row_pos, col_pos, flip(core)), top), partner_recv.at[chip, kind])
    drain(total_box.at[pl.ds(0, 15)], box_sem.at[0])
    drain(bot_box.at[pl.ds(0, 15)], box_sem.at[2])
    drain(top_box.at[pl.ds(0, 15)], box_sem.at[3])

    drain(top_out.at[:, pl.ds(0, 6 * SHARD)], first_send.at[1])
    drain(bot_out.at[:, pl.ds(0, 3 * SHARD)], first_send.at[0])
    drain(sent, second_send)


def in_hbm(array):
    return pltpu.with_memory_space_constraint(array, pltpu.HBM)


def run_step(local_grads, master, moment_one, moment_two):
    dma = pltpu.SemaphoreType.DMA
    block = pltpu.VMEM((2, N_CHUNK, 8, COLS), F32)
    return pl.pallas_call(
        step_kernel,
        out_shape=(pltpu.VMEM((8, 8 * SHARD), BF16), pltpu.VMEM((8, 4 * SHARD), BF16), block, block, block),
        in_specs=[pl.BlockSpec(memory_space=pltpu.HBM)] * 4,
        out_specs=(pl.BlockSpec(memory_space=pltpu.VMEM),) * 5,
        scratch_shapes=[
            block, block,
            pltpu.VMEM((16, 1, 128), F32),
            pltpu.VMEM((16, 2, 128), F32),
            pltpu.VMEM((16, 6, 128), F32),
            dma((2, 2, N_CHUNK)), dma((2, N_CHUNK)), dma((2,)), dma, dma((4,)), dma((2, 2)), dma((2, 2)), dma((4, 2)), dma((4, 2)), dma((6,)),
            pltpu.SemaphoreType.REGULAR, pltpu.SemaphoreType.REGULAR,
        ],
        compiler_params=pltpu.CompilerParams(collective_id=0, has_side_effects=True, vmem_limit_bytes=STEP_LIMIT),
        name='lamb_step',
    )(in_hbm(local_grads), in_hbm(master), in_hbm(moment_one), in_hbm(moment_two))


def write_kernel(top, bot, master, one, two, params_out, master_out, one_out, two_out, sem):
    copies = []
    for place in range(8):
        copies.append((top.at[:, pl.ds(place * SHARD, SHARD)], params_out.at[pl.ds(0, 8), pl.ds(place * SHARD, SHARD)]))
        for half in range(2):
            copies.append((bot.at[pl.ds(4 * half, 4), pl.ds(place * TOP_ROUTE, TOP_ROUTE)], params_out.at[pl.ds(8, 4), pl.ds(place * SHARD + half * TOP_ROUTE, TOP_ROUTE)]))
    for block, array in ((master, master_out), (one, one_out), (two, two_out)):
        for route in range(2):
            for chunk in range(N_CHUNK):
                copies += [(src, dst) for dst, src in row_views(array, 0, route, chunk, block.at[route, chunk], chunk < N_TOP)]
    for src, dst in copies:
        pltpu.make_async_copy(src, dst, sem).start()
    for src, dst in copies:
        pltpu.make_async_copy(src, dst, sem).wait()


def write_out(*blocks):
    state = jax.ShapeDtypeStruct((12, SHARD), F32)
    return pl.pallas_call(
        write_kernel,
        out_shape=(jax.ShapeDtypeStruct((12, 8 * SHARD), BF16), state, state, state),
        in_specs=[pl.BlockSpec(memory_space=pltpu.VMEM)] * 5,
        out_specs=(pl.BlockSpec(memory_space=pltpu.HBM),) * 4,
        scratch_shapes=[pltpu.SemaphoreType.DMA],
        compiler_params=pltpu.CompilerParams(vmem_limit_bytes=WRITE_LIMIT),
        name='write_out',
    )(*[pltpu.with_memory_space_constraint(block, pltpu.VMEM) for block in blocks])


def solution(mesh):
    state_spec = P(None, ('model', 'data'))

    def device_step(local_grads, master, moment_one, moment_two):
        return write_out(*run_step(local_grads, master, moment_one, moment_two))

    return jax.shard_map(device_step, mesh=mesh, in_specs=(P('data', None, 'model'), state_spec, state_spec, state_spec), out_specs=(P(None, 'model'), state_spec, state_spec, state_spec), check_vma=False)
```

```python
import functools

import jax
import jax.numpy as jnp
from jax import lax
from jax.experimental import pallas as pl
from jax.experimental.pallas import tpu as pltpu
from jax.sharding import PartitionSpec as P

STEP = 4
LEARN_RATE = 0.08
BETA_ONE = 0.9
BETA_TWO = 0.999
EPSILON = 1e-6
WEIGHT_DECAY = 0.01
MAX_NORM = 1.0
CORR_ONE = 1.0 - BETA_ONE ** STEP
CORR_TWO = 1.0 - BETA_TWO ** STEP

MESH = pl.DeviceIdType.MESH
F32 = jnp.float32
BF16 = jnp.bfloat16

SHARD = 147456
COLS = 6144
TOP_ROUTE = SHARD // 2
BOT_ROUTE = SHARD // 4
N_TOP = TOP_ROUTE // COLS
N_BOT = BOT_ROUTE // COLS
N_CHUNK = N_TOP + N_BOT
REDUCE_GROUPS = (
    (0, N_TOP // 2, True), (N_TOP // 2, N_TOP, True),
    (N_TOP, N_TOP + N_BOT // 2, False), (N_TOP + N_BOT // 2, N_CHUNK - 1, False), (N_CHUNK - 1, N_CHUNK, False),
)
GATHER_GROUPS = (
    (N_TOP, N_TOP + N_BOT // 2, False), (N_TOP + N_BOT // 2, N_CHUNK, False),
    (0, N_TOP // 2, True), (N_TOP // 2, N_TOP - 2, True), (N_TOP - 2, N_TOP - 1, True), (N_TOP - 1, N_TOP, True),
)
STRIP = 1024
UPDATE_STRIP = 2048

TINY = 1.2e-38
MIB = 1024 * 1024
STEP_LIMIT = 15 * MIB
WRITE_LIMIT = STEP_LIMIT


def flip(value):
    return 1 - value


def my_place():
    data_pos = lax.axis_index('data')
    return data_pos // 4, lax.rem(data_pos // 2, 2), lax.rem(data_pos, 2)


def data_index(pos_y, pos_x, core):
    return (pos_y * 2 + pos_x) * 2 + core


def drain(ref, sem):
    pltpu.make_async_copy(ref, ref, sem).wait()


def row_views(array, shard, route, chunk, block, top):
    if top:
        start = shard * SHARD + route * TOP_ROUTE + chunk * COLS
        return [(array.at[pl.ds(0, 8), pl.ds(pl.multiple_of(start, COLS), COLS)], block)]
    views = []
    for half in range(2):
        start = shard * SHARD + half * TOP_ROUTE + route * BOT_ROUTE + (chunk - N_TOP) * COLS
        views.append((array.at[pl.ds(8, 4), pl.ds(pl.multiple_of(start, COLS), COLS)], block.at[pl.ds(4 * half, 4)]))
    return views


def sweep(body, carry=0):
    for index, (low, high, top) in enumerate(REDUCE_GROUPS):
        carry = lax.fori_loop(low, high, functools.partial(body, index=index, top=top), carry)
    return carry


def strips(body, carry=0, width=STRIP):
    def step(strip, carry):
        return body(pl.ds(pl.multiple_of(strip * width, width), width), carry)

    return lax.fori_loop(0, COLS // width, step, carry)


def fold(total, values):
    for tile in range(values.shape[1] // 128):
        total = total + values[:, tile * 128:(tile + 1) * 128]
    return total


def step_kernel(
    grads, master_in, one_in, two_in,
    top_out, bot_out, master, one, two,
    mean, sent, total_box, bot_box, top_box,
    near_recv, corner_recv, first_send, second_send, load_sem, side_send, forward_send, partner_send, partner_recv, box_sem, seen, known,
):
    pos_y, pos_x, core = my_place()
    model_pos = lax.axis_index('model')
    mine = model_pos * 8 + lax.axis_index('data')
    grad = grads.at[0]
    got = two
    first_recv, second_recv = near_recv.at[0], near_recv.at[1]
    chips = ((pos_y, pos_x), (pos_y, flip(pos_x)), (flip(pos_y), pos_x), (flip(pos_y), flip(pos_x)))
    places = [data_index(row, col, core) for row, col in chips]
    partner = data_index(pos_y, pos_x, flip(core))

    def copy_to(src, dst, place, send_sem, recv_sem):
        pltpu.make_async_remote_copy(src_ref=src, dst_ref=dst, send_sem=send_sem, recv_sem=recv_sem, device_id=(model_pos, place), device_id_type=MESH).start()

    def landing(route, chunk, block, count, top):
        if top:
            start = ((route * N_TOP + chunk) * 8 + block) * COLS
        else:
            start = ((route * N_BOT + chunk - N_TOP) * 8 + block) * COLS
        return (top_out if top else bot_out).at[:, pl.ds(pl.multiple_of(start, COLS), count * COLS)]

    def wanted(route, row, col, far):
        return (lax.rem(row + far, 2), col) if route == 0 else (row, lax.rem(col + far, 2))

    def local(chunk, carry, index, top):
        for route in range(2):
            for far in range(2):
                shard = data_index(*wanted(route, pos_y, pos_x, far), core)
                for src, dst in row_views(grad, shard, route, chunk, landing(route, chunk, far, 1, top), top):
                    pltpu.make_async_copy(src, dst, first_recv.at[route, index]).start()
        return carry

    def remote(chunk, carry, index, top):
        for far in range(2):
            for other in range(2):
                for route in range(2):
                    row, col = chips[1 + route]
                    to_core = lax.rem(core + other, 2)
                    shard = data_index(*wanted(route, row, col, far), to_core)
                    for src, dst in row_views(grad, shard, route, chunk, landing(route, chunk, 4 + 2 * other + far, 1, top), top):
                        copy_to(src, dst, data_index(row, col, to_core), first_send.at[int(top)], first_recv.at[route, index])
            for route in range(2):
                shard = data_index(*wanted(route, pos_y, pos_x, far), flip(core))
                for src, dst in row_views(grad, shard, route, chunk, landing(route, chunk, 2 + far, 1, top), top):
                    copy_to(src, dst, partner, first_send.at[int(top)], first_recv.at[route, index])
        return carry

    def load(array, block, sem, route, chunk, top):
        for src, dst in row_views(array, 0, route, chunk, block.at[route, chunk], top):
            pltpu.make_async_copy(src, dst, sem).start()

    next_to = [(model_pos, place) for chip in (1, 2) for place in (places[chip], data_index(*chips[chip], flip(core)))] + [(model_pos, partner), (flip(model_pos), places[0])]

    def tell(sem, devices):
        for device in devices:
            pl.semaphore_signal(sem, inc=1, device_id=device, device_id_type=MESH)

    barrier = pltpu.get_barrier_semaphore()
    tell(barrier, next_to)
    sweep(local)
    pl.semaphore_wait(barrier, len(next_to))
    sweep(remote)
    tell(seen, next_to)

    def load_state(chunk, carry, index, top):
        for route in range(2):
            load(master_in, master, load_sem.at[0], route, chunk, top)
            load(one_in, one, load_sem.at[1], route, chunk, top)
        return carry

    sweep(load_state)
    pl.semaphore_wait(seen, len(next_to))
    tell(known, next_to[-1:])

    def second(route, chunk, index):
        copy_to(sent.at[route, chunk], got.at[route, chunk], places[2 - route], second_send, second_recv.at[route, index])

    def add_four(chunk, squares, top):
        for route in range(2):
            def body(cols, total):
                for far, target in ((0, mean), (1, sent)):
                    parts = [landing(route, chunk, 2 * source + far, 1, top)[:, cols].astype(F32) for source in range(4)]
                    target[route, chunk, :, cols] = (parts[0] + parts[1]) + (parts[2] + parts[3])
                weight = master[route, chunk, :, cols]
                return fold(total, weight * weight)

            squares = strips(body, squares)
        return squares

    drain(master, load_sem.at[0])
    zero = jnp.zeros((8, 128), F32)
    top_squares = bot_squares = zero
    for index, (low, high, top) in enumerate(REDUCE_GROUPS):
        for route in range(2):
            drain(landing(route, low, 0, 8 * (high - low), top), first_recv.at[route, index])
        squares = lax.fori_loop(low, high, functools.partial(add_four, top=top), top_squares if top else bot_squares)
        top_squares, bot_squares = (squares, bot_squares) if top else (top_squares, squares)

        @pl.loop(low, high)
        def _(chunk):
            second(0, chunk, index)
            second(1, chunk, index)

    def finish(chunk, squares, top):
        for route in range(2):
            def body(cols, total):
                value = (mean[route, chunk, :, cols] + got[route, chunk, :, cols]) * 0.125
                mean[route, chunk, :, cols] = value
                return fold(total, value * value)

            squares = strips(body, squares)
            load(two_in, two, load_sem.at[2 + int(top)], route, chunk, top)
        return squares

    def finish_all():
        squares = zero
        for index, (low, high, top) in enumerate(REDUCE_GROUPS):
            for route in range(2):
                drain(got.at[route, pl.ds(low, high - low)], second_recv.at[route, index])
            squares = lax.fori_loop(low, high, functools.partial(finish, top=top), squares)
        return squares

    everyone = [(row, data_index(*chip, side)) for row, chip in (
        (flip(model_pos), chips[3]), (flip(model_pos), chips[2]), (flip(model_pos), chips[1]), (model_pos, chips[3]),
        (flip(model_pos), chips[0]), (model_pos, chips[2]), (model_pos, chips[1]),
    ) for side in (core, flip(core))] + [(model_pos, partner)]

    def share_all(box, send_sem, recv_sem):
        for device in everyone:
            pltpu.make_async_remote_copy(src_ref=box.at[mine], dst_ref=box.at[mine], send_sem=send_sem, recv_sem=recv_sem, device_id=device, device_id_type=MESH).start()

    total_box[mine] = jnp.sum(finish_all(), axis=0, keepdims=True)
    pl.semaphore_wait(known, 1)
    share_all(total_box, box_sem.at[0], box_sem.at[1])
    drain(total_box.at[pl.ds(0, 15)], box_sem.at[1])
    total = jnp.sum(jnp.sum(total_box[...], axis=0), keepdims=True)
    clip = jnp.minimum(1.0, MAX_NORM / jnp.sqrt(total))
    one_scale, two_scale = clip * (1.0 - BETA_ONE), clip * (1.0 - BETA_TWO) ** 0.5

    def update(route, chunk, carry):
        def body(cols, total):
            place = (route, chunk, slice(None), cols)
            weight = master[place]
            value = mean[place]
            new_one = BETA_ONE * one[place] + one_scale * value
            change = two_scale * value
            new_two = BETA_TWO * two[place] + change * change
            one[place] = new_one
            two[place] = new_two
            floor = jnp.maximum(new_two, TINY)
            root = floor * lax.rsqrt(floor)
            direction = (new_one * (CORR_TWO ** 0.5 / CORR_ONE)) / (root + EPSILON * CORR_TWO ** 0.5) + WEIGHT_DECAY * weight
            mean[place] = direction
            return fold(total, direction * direction)

        return strips(body, carry, UPDATE_STRIP)

    def update_rows(index, low, high):
        drain(two.at[:, pl.ds(low, high - low)], load_sem.at[2 + index])
        return lax.fori_loop(low, high, lambda chunk, total: update(1, chunk, update(0, chunk, total)), zero)

    def share_norms(index, box, rows):
        for position, value in enumerate(rows):
            box[mine, position:position + 1] = value
        share_all(box, box_sem.at[2 + index], box_sem.at[4 + index])

    def norm_rows(index, box):
        drain(box.at[pl.ds(0, 15)], box_sem.at[4 + index])
        return jnp.sqrt(jnp.sum(jnp.sum(box[...], axis=0), axis=1, keepdims=True))

    def bot_rate():
        norms = norm_rows(0, bot_box)
        return LEARN_RATE * (norms[0:1] / norms[1:2]) + jnp.zeros((8, 1), F32)

    def top_rate():
        norms = norm_rows(1, top_box)
        rates = [LEARN_RATE * (norms[position:position + 1] / norms[position + 3:position + 4]) for position in range(3)]
        row = lax.broadcasted_iota(jnp.int32, (8, 1), 0)
        return jnp.where(row < 3, rates[0], jnp.where(row == 3, rates[1], rates[2]))

    def tensor_rows(squares):
        row = lax.broadcasted_iota(jnp.int32, (8, 128), 0)
        return [jnp.sum(jnp.where(mask, squares, 0.0), axis=0, keepdims=True) for mask in (row < 3, row == 3, row > 3)]

    drain(one, load_sem.at[1])
    share_norms(0, bot_box, [jnp.sum(squares, axis=0, keepdims=True) for squares in (bot_squares, update_rows(0, N_TOP, N_CHUNK))])
    share_norms(1, top_box, tensor_rows(top_squares) + tensor_rows(update_rows(1, 0, N_TOP)))

    def piece(place, route, chunk, top, count=1):
        if top:
            start = place * SHARD + route * TOP_ROUTE + chunk * COLS
        else:
            start = place * (SHARD // 2) + route * BOT_ROUTE + (chunk - N_TOP) * COLS
        return (top_out if top else bot_out).at[:, pl.ds(pl.multiple_of(start, COLS), count * COLS)]

    def part(place, top, share=1):
        size = SHARD if top else SHARD // 2
        return (top_out if top else bot_out).at[:, pl.ds(pl.multiple_of(place * size, size), size // share)]

    def weights(route, chunk, rate, top):
        view = piece(places[0], route, chunk, top)

        def body(cols, carry):
            place = (route, chunk, slice(None), cols)
            value = master[place] - rate * mean[place]
            master[place] = value
            view[:, cols] = value.astype(BF16)
            return carry

        strips(body)

    def send(route, chunk, index, top):
        view = piece(places[0], route, chunk, top)
        kind = int(top)
        for axis in range(2):
            copy_to(view, view, places[1 + axis], side_send.at[axis, kind], near_recv.at[axis, route, index])
        copy_to(view, view, partner, partner_send.at[0, kind], partner_recv.at[0, kind])

    def own(chunk, rate, index, low, high, top):
        weights(0, chunk, rate, top)

        @pl.when(chunk > low)
        def _():
            send(1, chunk - 1, index, top)

        weights(1, chunk, rate, top)
        send(0, chunk, index, top)

        @pl.when(chunk == high - 1)
        def _():
            send(1, chunk, index, top)

        return rate

    for index, (low, high, top) in enumerate(GATHER_GROUPS):
        if index == 0:
            rate = bot_rate()
        elif top and not GATHER_GROUPS[index - 1][2]:
            rate = top_rate()
        lax.fori_loop(low, high, functools.partial(own, index=index, low=low, high=high, top=top), rate)

    for index, (low, high, top) in enumerate(GATHER_GROUPS):
        kind = int(top)
        for axis in range(2):
            for route in range(2):
                view = piece(places[1 + axis], route, low, top, high - low)
                drain(view, near_recv.at[axis, route, index])
                if axis == route:
                    copy_to(view, view, places[2 - route], forward_send.at[route, kind], corner_recv.at[route, index])
                copy_to(view, view, partner, partner_send.at[1 + axis, kind], partner_recv.at[1 + axis, kind])

    for index, (low, high, top) in enumerate(GATHER_GROUPS):
        for route in range(2):
            view = piece(places[3], route, low, top, high - low)
            drain(view, corner_recv.at[route, index])
            copy_to(view, view, partner, partner_send.at[3, int(top)], partner_recv.at[3, int(top)])

    for top in (True, False):
        kind = int(top)
        for axis in range(2):
            drain(part(places[0], top), side_send.at[axis, kind])
            drain(part(places[0], top, 2), forward_send.at[axis, kind])
        for chip, (row_pos, col_pos) in enumerate(chips):
            drain(part(places[chip], top), partner_send.at[chip, kind])
            drain(part(data_index(row_pos, col_pos, flip(core)), top), partner_recv.at[chip, kind])
    drain(total_box.at[pl.ds(0, 15)], box_sem.at[0])
    drain(bot_box.at[pl.ds(0, 15)], box_sem.at[2])
    drain(top_box.at[pl.ds(0, 15)], box_sem.at[3])

    drain(top_out.at[:, pl.ds(0, 6 * SHARD)], first_send.at[1])
    drain(bot_out.at[:, pl.ds(0, 3 * SHARD)], first_send.at[0])
    drain(sent, second_send)


def in_hbm(array):
    return pltpu.with_memory_space_constraint(array, pltpu.HBM)


def run_step(local_grads, master, moment_one, moment_two):
    dma = pltpu.SemaphoreType.DMA
    block = pltpu.VMEM((2, N_CHUNK, 8, COLS), F32)
    return pl.pallas_call(
        step_kernel,
        out_shape=(pltpu.VMEM((8, 8 * SHARD), BF16), pltpu.VMEM((8, 4 * SHARD), BF16), block, block, block),
        in_specs=[pl.BlockSpec(memory_space=pltpu.HBM)] * 4,
        out_specs=(pl.BlockSpec(memory_space=pltpu.VMEM),) * 5,
        scratch_shapes=[
            block, block,
            pltpu.VMEM((16, 1, 128), F32),
            pltpu.VMEM((16, 2, 128), F32),
            pltpu.VMEM((16, 6, 128), F32),
            dma((2, 2, len(GATHER_GROUPS))), dma((2, len(GATHER_GROUPS))), dma((2,)), dma, dma((4,)), dma((2, 2)), dma((2, 2)), dma((4, 2)), dma((4, 2)), dma((6,)),
            pltpu.SemaphoreType.REGULAR, pltpu.SemaphoreType.REGULAR,
        ],
        compiler_params=pltpu.CompilerParams(collective_id=0, has_side_effects=True, vmem_limit_bytes=STEP_LIMIT),
        name='lamb_step',
    )(in_hbm(local_grads), in_hbm(master), in_hbm(moment_one), in_hbm(moment_two))


def write_kernel(top, bot, master, one, two, params_out, master_out, one_out, two_out, sem):
    copies = []
    for place in range(8):
        copies.append((top.at[:, pl.ds(place * SHARD, SHARD)], params_out.at[pl.ds(0, 8), pl.ds(place * SHARD, SHARD)]))
        for half in range(2):
            copies.append((bot.at[pl.ds(4 * half, 4), pl.ds(place * TOP_ROUTE, TOP_ROUTE)], params_out.at[pl.ds(8, 4), pl.ds(place * SHARD + half * TOP_ROUTE, TOP_ROUTE)]))
    for block, array in ((master, master_out), (one, one_out), (two, two_out)):
        for route in range(2):
            for chunk in range(N_CHUNK):
                copies += [(src, dst) for dst, src in row_views(array, 0, route, chunk, block.at[route, chunk], chunk < N_TOP)]
    for src, dst in copies:
        pltpu.make_async_copy(src, dst, sem).start()
    for src, dst in copies:
        pltpu.make_async_copy(src, dst, sem).wait()


def write_out(*blocks):
    state = jax.ShapeDtypeStruct((12, SHARD), F32)
    return pl.pallas_call(
        write_kernel,
        out_shape=(jax.ShapeDtypeStruct((12, 8 * SHARD), BF16), state, state, state),
        in_specs=[pl.BlockSpec(memory_space=pltpu.VMEM)] * 5,
        out_specs=(pl.BlockSpec(memory_space=pltpu.HBM),) * 4,
        scratch_shapes=[pltpu.SemaphoreType.DMA],
        compiler_params=pltpu.CompilerParams(vmem_limit_bytes=WRITE_LIMIT),
        name='write_out',
    )(*[pltpu.with_memory_space_constraint(block, pltpu.VMEM) for block in blocks])


def solution(mesh):
    state_spec = P(None, ('model', 'data'))

    def device_step(local_grads, master, moment_one, moment_two):
        return write_out(*run_step(local_grads, master, moment_one, moment_two))

    return jax.shard_map(device_step, mesh=mesh, in_specs=(P('data', None, 'model'), state_spec, state_spec, state_spec), out_specs=(P(None, 'model'), state_spec, state_spec, state_spec), check_vma=False)
```

```python
import functools

import jax
import jax.numpy as jnp
from jax import lax
from jax.experimental import pallas as pl
from jax.experimental.pallas import tpu as pltpu
from jax.sharding import PartitionSpec as P

STEP = 4
LEARN_RATE = 0.08
BETA_ONE = 0.9
BETA_TWO = 0.999
EPSILON = 1e-6
WEIGHT_DECAY = 0.01
MAX_NORM = 1.0
CORR_ONE = 1.0 - BETA_ONE ** STEP
CORR_TWO = 1.0 - BETA_TWO ** STEP

MESH = pl.DeviceIdType.MESH
F32 = jnp.float32
BF16 = jnp.bfloat16

SHARD = 147456
COLS = 3072
TOP_ROUTE = SHARD // 2
BOT_ROUTE = SHARD // 4
N_TOP = TOP_ROUTE // COLS
N_BOT = BOT_ROUTE // COLS
N_CHUNK = N_TOP + N_BOT
REDUCE_GROUPS = (
    (0, N_TOP // 2, True), (N_TOP // 2, N_TOP, True),
    (N_TOP, N_TOP + N_BOT // 2, False), (N_TOP + N_BOT // 2, N_CHUNK - 1, False), (N_CHUNK - 1, N_CHUNK, False),
)
GATHER_GROUPS = (
    (N_TOP, N_TOP + N_BOT // 2, False), (N_TOP + N_BOT // 2, N_CHUNK, False),
    (0, N_TOP // 2, True), (N_TOP // 2, N_TOP - 2, True), (N_TOP - 2, N_TOP - 1, True), (N_TOP - 1, N_TOP, True),
)
STRIP = 1024
UPDATE_STRIP = 3072

TINY = 1.2e-38
MIB = 1024 * 1024
STEP_LIMIT = 15 * MIB
WRITE_LIMIT = STEP_LIMIT


def flip(value):
    return 1 - value


def my_place():
    data_pos = lax.axis_index('data')
    return data_pos // 4, lax.rem(data_pos // 2, 2), lax.rem(data_pos, 2)


def data_index(pos_y, pos_x, core):
    return (pos_y * 2 + pos_x) * 2 + core


def drain(ref, sem):
    pltpu.make_async_copy(ref, ref, sem).wait()


def row_views(array, shard, route, chunk, block, top):
    if top:
        start = shard * SHARD + route * TOP_ROUTE + chunk * COLS
        return [(array.at[pl.ds(0, 8), pl.ds(pl.multiple_of(start, COLS), COLS)], block)]
    views = []
    for half in range(2):
        start = shard * SHARD + half * TOP_ROUTE + route * BOT_ROUTE + (chunk - N_TOP) * COLS
        views.append((array.at[pl.ds(8, 4), pl.ds(pl.multiple_of(start, COLS), COLS)], block.at[pl.ds(4 * half, 4)]))
    return views


def sweep(body, carry=0):
    for index, (low, high, top) in enumerate(REDUCE_GROUPS):
        carry = lax.fori_loop(low, high, functools.partial(body, index=index, top=top), carry)
    return carry


def strips(body, carry=0, width=STRIP):
    def step(strip, carry):
        return body(pl.ds(pl.multiple_of(strip * width, width), width), carry)

    return lax.fori_loop(0, COLS // width, step, carry)


def fold(total, values):
    for tile in range(values.shape[1] // 128):
        total = total + values[:, tile * 128:(tile + 1) * 128]
    return total


def step_kernel(
    grads, master_in, one_in, two_in,
    top_out, bot_out, master, one, two,
    mean, sent, total_box, bot_box, top_box,
    near_recv, corner_recv, first_send, second_send, load_sem, side_send, forward_send, partner_send, partner_recv, box_sem, seen, known,
):
    pos_y, pos_x, core = my_place()
    model_pos = lax.axis_index('model')
    mine = model_pos * 8 + lax.axis_index('data')
    grad = grads.at[0]
    got = two
    first_recv, second_recv = near_recv.at[0], near_recv.at[1]
    chips = ((pos_y, pos_x), (pos_y, flip(pos_x)), (flip(pos_y), pos_x), (flip(pos_y), flip(pos_x)))
    places = [data_index(row, col, core) for row, col in chips]
    partner = data_index(pos_y, pos_x, flip(core))

    def copy_to(src, dst, place, send_sem, recv_sem):
        pltpu.make_async_remote_copy(src_ref=src, dst_ref=dst, send_sem=send_sem, recv_sem=recv_sem, device_id=(model_pos, place), device_id_type=MESH).start()

    def landing(route, chunk, block, count, top):
        if top:
            start = ((route * N_TOP + chunk) * 8 + block) * COLS
        else:
            start = ((route * N_BOT + chunk - N_TOP) * 8 + block) * COLS
        return (top_out if top else bot_out).at[:, pl.ds(pl.multiple_of(start, COLS), count * COLS)]

    def wanted(route, row, col, far):
        return (lax.rem(row + far, 2), col) if route == 0 else (row, lax.rem(col + far, 2))

    def local(chunk, carry, index, top):
        for route in range(2):
            for far in range(2):
                shard = data_index(*wanted(route, pos_y, pos_x, far), core)
                for src, dst in row_views(grad, shard, route, chunk, landing(route, chunk, far, 1, top), top):
                    pltpu.make_async_copy(src, dst, first_recv.at[route, index]).start()
        return carry

    def remote(chunk, carry, index, top):
        for far in range(2):
            for other in range(2):
                for route in range(2):
                    row, col = chips[1 + route]
                    to_core = lax.rem(core + other, 2)
                    shard = data_index(*wanted(route, row, col, far), to_core)
                    for src, dst in row_views(grad, shard, route, chunk, landing(route, chunk, 4 + 2 * other + far, 1, top), top):
                        copy_to(src, dst, data_index(row, col, to_core), first_send.at[int(top)], first_recv.at[route, index])
            for route in range(2):
                shard = data_index(*wanted(route, pos_y, pos_x, far), flip(core))
                for src, dst in row_views(grad, shard, route, chunk, landing(route, chunk, 2 + far, 1, top), top):
                    copy_to(src, dst, partner, first_send.at[int(top)], first_recv.at[route, index])
        return carry

    def load(array, block, sem, route, chunk, top):
        for src, dst in row_views(array, 0, route, chunk, block.at[route, chunk], top):
            pltpu.make_async_copy(src, dst, sem).start()

    next_to = [(model_pos, place) for chip in (1, 2) for place in (places[chip], data_index(*chips[chip], flip(core)))] + [(model_pos, partner), (flip(model_pos), places[0])]

    def tell(sem, devices):
        for device in devices:
            pl.semaphore_signal(sem, inc=1, device_id=device, device_id_type=MESH)

    barrier = pltpu.get_barrier_semaphore()
    tell(barrier, next_to)
    sweep(local)
    pl.semaphore_wait(barrier, len(next_to))
    sweep(remote)
    tell(seen, next_to)

    def load_state(chunk, carry, index, top):
        for route in range(2):
            load(master_in, master, load_sem.at[0], route, chunk, top)
            load(one_in, one, load_sem.at[1], route, chunk, top)
        return carry

    sweep(load_state)
    pl.semaphore_wait(seen, len(next_to))
    tell(known, next_to[-1:])

    def second(route, chunk, index):
        copy_to(sent.at[route, chunk], got.at[route, chunk], places[2 - route], second_send, second_recv.at[route, index])

    def add_four(chunk, squares, top):
        for route in range(2):
            def body(cols, total):
                for far, target in ((0, mean), (1, sent)):
                    parts = [landing(route, chunk, 2 * source + far, 1, top)[:, cols].astype(F32) for source in range(4)]
                    target[route, chunk, :, cols] = (parts[0] + parts[1]) + (parts[2] + parts[3])
                weight = master[route, chunk, :, cols]
                return fold(total, weight * weight)

            squares = strips(body, squares)
        return squares

    drain(master, load_sem.at[0])
    zero = jnp.zeros((8, 128), F32)
    top_squares = bot_squares = zero
    for index, (low, high, top) in enumerate(REDUCE_GROUPS):
        for route in range(2):
            drain(landing(route, low, 0, 8 * (high - low), top), first_recv.at[route, index])
        squares = lax.fori_loop(low, high, functools.partial(add_four, top=top), top_squares if top else bot_squares)
        top_squares, bot_squares = (squares, bot_squares) if top else (top_squares, squares)

        @pl.loop(low, high)
        def _(chunk):
            second(0, chunk, index)
            second(1, chunk, index)

    def finish(chunk, squares, top):
        for route in range(2):
            def body(cols, total):
                value = (mean[route, chunk, :, cols] + got[route, chunk, :, cols]) * 0.125
                mean[route, chunk, :, cols] = value
                return fold(total, value * value)

            squares = strips(body, squares)
            load(two_in, two, load_sem.at[2 + int(top)], route, chunk, top)
        return squares

    def finish_all():
        squares = zero
        for index, (low, high, top) in enumerate(REDUCE_GROUPS):
            for route in range(2):
                drain(got.at[route, pl.ds(low, high - low)], second_recv.at[route, index])
            squares = lax.fori_loop(low, high, functools.partial(finish, top=top), squares)
        return squares

    everyone = [(row, data_index(*chip, side)) for row, chip in (
        (flip(model_pos), chips[3]), (flip(model_pos), chips[2]), (flip(model_pos), chips[1]), (model_pos, chips[3]),
        (flip(model_pos), chips[0]), (model_pos, chips[2]), (model_pos, chips[1]),
    ) for side in (core, flip(core))] + [(model_pos, partner)]

    def share_all(box, send_sem, recv_sem):
        for device in everyone:
            pltpu.make_async_remote_copy(src_ref=box.at[mine], dst_ref=box.at[mine], send_sem=send_sem, recv_sem=recv_sem, device_id=device, device_id_type=MESH).start()

    total_box[mine] = jnp.sum(finish_all(), axis=0, keepdims=True)
    pl.semaphore_wait(known, 1)
    share_all(total_box, box_sem.at[0], box_sem.at[1])
    drain(total_box.at[pl.ds(0, 15)], box_sem.at[1])
    total = jnp.sum(jnp.sum(total_box[...], axis=0), keepdims=True)
    clip = jnp.minimum(1.0, MAX_NORM / jnp.sqrt(total))
    one_scale, two_scale = clip * (1.0 - BETA_ONE), clip * (1.0 - BETA_TWO) ** 0.5

    def update(route, chunk, carry):
        def body(cols, total):
            place = (route, chunk, slice(None), cols)
            weight = master[place]
            value = mean[place]
            new_one = BETA_ONE * one[place] + one_scale * value
            change = two_scale * value
            new_two = BETA_TWO * two[place] + change * change
            one[place] = new_one
            two[place] = new_two
            floor = jnp.maximum(new_two, TINY)
            root = floor * lax.rsqrt(floor)
            direction = (new_one * (CORR_TWO ** 0.5 / CORR_ONE)) / (root + EPSILON * CORR_TWO ** 0.5) + WEIGHT_DECAY * weight
            mean[place] = direction
            return fold(total, direction * direction)

        return strips(body, carry, UPDATE_STRIP)

    def update_rows(index, low, high):
        drain(two.at[:, pl.ds(low, high - low)], load_sem.at[2 + index])
        return lax.fori_loop(low, high, lambda chunk, total: update(1, chunk, update(0, chunk, total)), zero)

    def share_norms(index, box, rows):
        for position, value in enumerate(rows):
            box[mine, position:position + 1] = value
        share_all(box, box_sem.at[2 + index], box_sem.at[4 + index])

    def norm_rows(index, box):
        drain(box.at[pl.ds(0, 15)], box_sem.at[4 + index])
        return jnp.sqrt(jnp.sum(jnp.sum(box[...], axis=0), axis=1, keepdims=True))

    def bot_rate():
        norms = norm_rows(0, bot_box)
        return LEARN_RATE * (norms[0:1] / norms[1:2]) + jnp.zeros((8, 1), F32)

    def top_rate():
        norms = norm_rows(1, top_box)
        rates = [LEARN_RATE * (norms[position:position + 1] / norms[position + 3:position + 4]) for position in range(3)]
        row = lax.broadcasted_iota(jnp.int32, (8, 1), 0)
        return jnp.where(row < 3, rates[0], jnp.where(row == 3, rates[1], rates[2]))

    def tensor_rows(squares):
        row = lax.broadcasted_iota(jnp.int32, (8, 128), 0)
        return [jnp.sum(jnp.where(mask, squares, 0.0), axis=0, keepdims=True) for mask in (row < 3, row == 3, row > 3)]

    drain(one, load_sem.at[1])
    share_norms(0, bot_box, [jnp.sum(squares, axis=0, keepdims=True) for squares in (bot_squares, update_rows(0, N_TOP, N_CHUNK))])
    share_norms(1, top_box, tensor_rows(top_squares) + tensor_rows(update_rows(1, 0, N_TOP)))

    def piece(place, route, chunk, top, count=1):
        if top:
            start = place * SHARD + route * TOP_ROUTE + chunk * COLS
        else:
            start = place * (SHARD // 2) + route * BOT_ROUTE + (chunk - N_TOP) * COLS
        return (top_out if top else bot_out).at[:, pl.ds(pl.multiple_of(start, COLS), count * COLS)]

    def part(place, top, share=1):
        size = SHARD if top else SHARD // 2
        return (top_out if top else bot_out).at[:, pl.ds(pl.multiple_of(place * size, size), size // share)]

    def weights(route, chunk, rate, top):
        view = piece(places[0], route, chunk, top)

        def body(cols, carry):
            place = (route, chunk, slice(None), cols)
            value = master[place] - rate * mean[place]
            master[place] = value
            view[:, cols] = value.astype(BF16)
            return carry

        strips(body)

    def send(route, chunk, index, top):
        view = piece(places[0], route, chunk, top)
        kind = int(top)
        for axis in range(2):
            copy_to(view, view, places[1 + axis], side_send.at[axis, kind], near_recv.at[axis, route, index])
        copy_to(view, view, partner, partner_send.at[0, kind], partner_recv.at[0, kind])

    def own(chunk, rate, index, low, high, top):
        weights(0, chunk, rate, top)

        @pl.when(chunk > low)
        def _():
            send(1, chunk - 1, index, top)

        weights(1, chunk, rate, top)
        send(0, chunk, index, top)

        @pl.when(chunk == high - 1)
        def _():
            send(1, chunk, index, top)

        return rate

    for index, (low, high, top) in enumerate(GATHER_GROUPS):
        if index == 0:
            rate = bot_rate()
        elif top and not GATHER_GROUPS[index - 1][2]:
            rate = top_rate()
        lax.fori_loop(low, high, functools.partial(own, index=index, low=low, high=high, top=top), rate)

    for index, (low, high, top) in enumerate(GATHER_GROUPS):
        kind = int(top)
        for axis in range(2):
            for route in range(2):
                view = piece(places[1 + axis], route, low, top, high - low)
                drain(view, near_recv.at[axis, route, index])
                if axis == route:
                    copy_to(view, view, places[2 - route], forward_send.at[route, kind], corner_recv.at[route, index])
                copy_to(view, view, partner, partner_send.at[1 + axis, kind], partner_recv.at[1 + axis, kind])

    for index, (low, high, top) in enumerate(GATHER_GROUPS):
        for route in range(2):
            view = piece(places[3], route, low, top, high - low)
            drain(view, corner_recv.at[route, index])
            copy_to(view, view, partner, partner_send.at[3, int(top)], partner_recv.at[3, int(top)])

    for top in (True, False):
        kind = int(top)
        for axis in range(2):
            drain(part(places[0], top), side_send.at[axis, kind])
            drain(part(places[0], top, 2), forward_send.at[axis, kind])
        for chip, (row_pos, col_pos) in enumerate(chips):
            drain(part(places[chip], top), partner_send.at[chip, kind])
            drain(part(data_index(row_pos, col_pos, flip(core)), top), partner_recv.at[chip, kind])
    drain(total_box.at[pl.ds(0, 15)], box_sem.at[0])
    drain(bot_box.at[pl.ds(0, 15)], box_sem.at[2])
    drain(top_box.at[pl.ds(0, 15)], box_sem.at[3])

    drain(top_out.at[:, pl.ds(0, 6 * SHARD)], first_send.at[1])
    drain(bot_out.at[:, pl.ds(0, 3 * SHARD)], first_send.at[0])
    drain(sent, second_send)


def in_hbm(array):
    return pltpu.with_memory_space_constraint(array, pltpu.HBM)


def run_step(local_grads, master, moment_one, moment_two):
    dma = pltpu.SemaphoreType.DMA
    block = pltpu.VMEM((2, N_CHUNK, 8, COLS), F32)
    return pl.pallas_call(
        step_kernel,
        out_shape=(pltpu.VMEM((8, 8 * SHARD), BF16), pltpu.VMEM((8, 4 * SHARD), BF16), block, block, block),
        in_specs=[pl.BlockSpec(memory_space=pltpu.HBM)] * 4,
        out_specs=(pl.BlockSpec(memory_space=pltpu.VMEM),) * 5,
        scratch_shapes=[
            block, block,
            pltpu.VMEM((16, 1, 128), F32),
            pltpu.VMEM((16, 2, 128), F32),
            pltpu.VMEM((16, 6, 128), F32),
            dma((2, 2, len(GATHER_GROUPS))), dma((2, len(GATHER_GROUPS))), dma((2,)), dma, dma((4,)), dma((2, 2)), dma((2, 2)), dma((4, 2)), dma((4, 2)), dma((6,)),
            pltpu.SemaphoreType.REGULAR, pltpu.SemaphoreType.REGULAR,
        ],
        compiler_params=pltpu.CompilerParams(collective_id=0, has_side_effects=True, vmem_limit_bytes=STEP_LIMIT),
        name='lamb_step',
    )(in_hbm(local_grads), in_hbm(master), in_hbm(moment_one), in_hbm(moment_two))


def write_kernel(top, bot, master, one, two, params_out, master_out, one_out, two_out, sem):
    copies = []
    for place in range(8):
        copies.append((top.at[:, pl.ds(place * SHARD, SHARD)], params_out.at[pl.ds(0, 8), pl.ds(place * SHARD, SHARD)]))
        for half in range(2):
            copies.append((bot.at[pl.ds(4 * half, 4), pl.ds(place * TOP_ROUTE, TOP_ROUTE)], params_out.at[pl.ds(8, 4), pl.ds(place * SHARD + half * TOP_ROUTE, TOP_ROUTE)]))
    for block, array in ((master, master_out), (one, one_out), (two, two_out)):
        for route in range(2):
            for chunk in range(N_CHUNK):
                copies += [(src, dst) for dst, src in row_views(array, 0, route, chunk, block.at[route, chunk], chunk < N_TOP)]
    for src, dst in copies:
        pltpu.make_async_copy(src, dst, sem).start()
    for src, dst in copies:
        pltpu.make_async_copy(src, dst, sem).wait()


def write_out(*blocks):
    state = jax.ShapeDtypeStruct((12, SHARD), F32)
    return pl.pallas_call(
        write_kernel,
        out_shape=(jax.ShapeDtypeStruct((12, 8 * SHARD), BF16), state, state, state),
        in_specs=[pl.BlockSpec(memory_space=pltpu.VMEM)] * 5,
        out_specs=(pl.BlockSpec(memory_space=pltpu.HBM),) * 4,
        scratch_shapes=[pltpu.SemaphoreType.DMA],
        compiler_params=pltpu.CompilerParams(vmem_limit_bytes=WRITE_LIMIT),
        name='write_out',
    )(*[pltpu.with_memory_space_constraint(block, pltpu.VMEM) for block in blocks])


def solution(mesh):
    state_spec = P(None, ('model', 'data'))

    def device_step(local_grads, master, moment_one, moment_two):
        return write_out(*run_step(local_grads, master, moment_one, moment_two))

    return jax.shard_map(device_step, mesh=mesh, in_specs=(P('data', None, 'model'), state_spec, state_spec, state_spec), out_specs=(P(None, 'model'), state_spec, state_spec, state_spec), check_vma=False)
```

```python
import functools

import jax
import jax.numpy as jnp
from jax import lax
from jax.experimental import pallas as pl
from jax.experimental.pallas import tpu as pltpu
from jax.sharding import PartitionSpec as P

STEP = 4
LEARN_RATE = 0.08
BETA_ONE = 0.9
BETA_TWO = 0.999
EPSILON = 1e-6
WEIGHT_DECAY = 0.01
MAX_NORM = 1.0
CORR_ONE = 1.0 - BETA_ONE ** STEP
CORR_TWO = 1.0 - BETA_TWO ** STEP

MESH = pl.DeviceIdType.MESH
F32 = jnp.float32
BF16 = jnp.bfloat16

SHARD = 147456
COLS = 3072
TOP_ROUTE = SHARD // 2
BOT_ROUTE = SHARD // 4
N_TOP = TOP_ROUTE // COLS
N_BOT = BOT_ROUTE // COLS
N_CHUNK = N_TOP + N_BOT
REDUCE_GROUPS = (
    (0, N_TOP // 2, True), (N_TOP // 2, N_TOP, True),
    (N_TOP, N_TOP + N_BOT // 2, False), (N_TOP + N_BOT // 2, N_CHUNK - 1, False), (N_CHUNK - 1, N_CHUNK, False),
)
GATHER_GROUPS = (
    (N_TOP, N_TOP + N_BOT // 2, False), (N_TOP + N_BOT // 2, N_CHUNK, False),
    (0, N_TOP // 2, True), (N_TOP // 2, N_TOP - 2, True), (N_TOP - 2, N_TOP - 1, True), (N_TOP - 1, N_TOP, True),
)
STRIP = 1024
UPDATE_STRIP = 2048

TINY = 1.2e-38
MIB = 1024 * 1024
STEP_LIMIT = 15 * MIB
WRITE_LIMIT = STEP_LIMIT


def flip(value):
    return 1 - value


def my_place():
    data_pos = lax.axis_index('data')
    return data_pos // 4, lax.rem(data_pos // 2, 2), lax.rem(data_pos, 2)


def data_index(pos_y, pos_x, core):
    return (pos_y * 2 + pos_x) * 2 + core


def drain(ref, sem):
    pltpu.make_async_copy(ref, ref, sem).wait()


def slot(block, route, chunk, count=1):
    return block.at[route, :, pl.ds(pl.multiple_of(chunk * COLS, COLS), count * COLS)]


def row_views(array, shard, route, chunk, block, top, count=1):
    if top:
        start = shard * SHARD + route * TOP_ROUTE + chunk * COLS
        return [(array.at[pl.ds(0, 8), pl.ds(pl.multiple_of(start, COLS), count * COLS)], block)]
    views = []
    for half in range(2):
        start = shard * SHARD + half * TOP_ROUTE + route * BOT_ROUTE + (chunk - N_TOP) * COLS
        views.append((array.at[pl.ds(8, 4), pl.ds(pl.multiple_of(start, COLS), count * COLS)], block.at[pl.ds(4 * half, 4)]))
    return views


def sweep(body, carry=0):
    for index, (low, high, top) in enumerate(REDUCE_GROUPS):
        carry = lax.fori_loop(low, high, functools.partial(body, index=index, top=top), carry)
    return carry


def strips(body, low, high, carry=0, width=STRIP):
    def step(strip, carry):
        return body(pl.ds(pl.multiple_of(low + strip * width, width), width), carry)

    return lax.fori_loop(0, (high - low) // width, step, carry)


def fold(total, values):
    for tile in range(values.shape[1] // 128):
        total = total + values[:, tile * 128:(tile + 1) * 128]
    return total


def step_kernel(
    grads, master_in, one_in, two_in,
    top_out, bot_out, master, one, two,
    mean, sent, total_box, bot_box, top_box,
    near_recv, corner_recv, first_send, second_send, load_sem, side_send, forward_send, partner_send, partner_recv, box_sem, seen, known,
):
    pos_y, pos_x, core = my_place()
    model_pos = lax.axis_index('model')
    mine = model_pos * 8 + lax.axis_index('data')
    grad = grads.at[0]
    got = two
    first_recv, second_recv = near_recv.at[0], near_recv.at[1]
    chips = ((pos_y, pos_x), (pos_y, flip(pos_x)), (flip(pos_y), pos_x), (flip(pos_y), flip(pos_x)))
    places = [data_index(row, col, core) for row, col in chips]
    partner = data_index(pos_y, pos_x, flip(core))

    def copy_to(src, dst, place, send_sem, recv_sem):
        pltpu.make_async_remote_copy(src_ref=src, dst_ref=dst, send_sem=send_sem, recv_sem=recv_sem, device_id=(model_pos, place), device_id_type=MESH).start()

    def landing(route, chunk, block, count, top):
        if top:
            start = ((route * N_TOP + chunk) * 8 + block) * COLS
        else:
            start = ((route * N_BOT + chunk - N_TOP) * 8 + block) * COLS
        return (top_out if top else bot_out).at[:, pl.ds(pl.multiple_of(start, COLS), count * COLS)]

    def wanted(route, row, col, far):
        return (lax.rem(row + far, 2), col) if route == 0 else (row, lax.rem(col + far, 2))

    def local(chunk, carry, index, top):
        for route in range(2):
            for far in range(2):
                shard = data_index(*wanted(route, pos_y, pos_x, far), core)
                for src, dst in row_views(grad, shard, route, chunk, landing(route, chunk, far, 1, top), top):
                    pltpu.make_async_copy(src, dst, first_recv.at[route, index]).start()
        return carry

    def remote(chunk, carry, index, top):
        for far in range(2):
            for other in range(2):
                for route in range(2):
                    row, col = chips[1 + route]
                    to_core = lax.rem(core + other, 2)
                    shard = data_index(*wanted(route, row, col, far), to_core)
                    for src, dst in row_views(grad, shard, route, chunk, landing(route, chunk, 4 + 2 * other + far, 1, top), top):
                        copy_to(src, dst, data_index(row, col, to_core), first_send.at[int(top)], first_recv.at[route, index])
            for route in range(2):
                shard = data_index(*wanted(route, pos_y, pos_x, far), flip(core))
                for src, dst in row_views(grad, shard, route, chunk, landing(route, chunk, 2 + far, 1, top), top):
                    copy_to(src, dst, partner, first_send.at[int(top)], first_recv.at[route, index])
        return carry

    def load(array, block, sem, route, chunk, top, count=1):
        for src, dst in row_views(array, 0, route, chunk, slot(block, route, chunk, count), top, count):
            pltpu.make_async_copy(src, dst, sem).start()

    next_to = [(model_pos, place) for chip in (1, 2) for place in (places[chip], data_index(*chips[chip], flip(core)))] + [(model_pos, partner), (flip(model_pos), places[0])]

    def tell(sem, devices):
        for device in devices:
            pl.semaphore_signal(sem, inc=1, device_id=device, device_id_type=MESH)

    barrier = pltpu.get_barrier_semaphore()
    tell(barrier, next_to)
    sweep(local)
    pl.semaphore_wait(barrier, len(next_to))
    sweep(remote)
    tell(seen, next_to)

    for index, (low, high, top) in enumerate(REDUCE_GROUPS):
        for route in range(2):
            load(master_in, master, load_sem.at[0], route, low, top, high - low)
            load(one_in, one, load_sem.at[1], route, low, top, high - low)
    pl.semaphore_wait(seen, len(next_to))
    tell(known, next_to[-1:])

    def second(route, chunk, index):
        copy_to(slot(sent, route, chunk), slot(got, route, chunk), places[2 - route], second_send, second_recv.at[route, index])

    def add_four(chunk, squares, top):
        for route in range(2):
            targets = [slot(block, route, chunk) for block in (mean, sent)]
            weights_view = slot(master, route, chunk)

            def body(cols, total):
                for far, target in enumerate(targets):
                    parts = [landing(route, chunk, 2 * source + far, 1, top)[:, cols].astype(F32) for source in range(4)]
                    target[:, cols] = (parts[0] + parts[1]) + (parts[2] + parts[3])
                weight = weights_view[:, cols]
                return fold(total, weight * weight)

            squares = strips(body, 0, COLS, squares)
        return squares

    drain(master, load_sem.at[0])
    zero = jnp.zeros((8, 128), F32)
    top_squares = bot_squares = zero
    for index, (low, high, top) in enumerate(REDUCE_GROUPS):
        for route in range(2):
            drain(landing(route, low, 0, 8 * (high - low), top), first_recv.at[route, index])
        squares = lax.fori_loop(low, high, functools.partial(add_four, top=top), top_squares if top else bot_squares)
        top_squares, bot_squares = (squares, bot_squares) if top else (top_squares, squares)

        @pl.loop(low, high)
        def _(chunk):
            second(0, chunk, index)
            second(1, chunk, index)

    def finish():
        squares = zero
        for index, (low, high, top) in enumerate(REDUCE_GROUPS):
            for route in range(2):
                drain(slot(got, route, low, high - low), second_recv.at[route, index])

                def body(cols, total):
                    value = (mean[route, :, cols] + got[route, :, cols]) * 0.125
                    mean[route, :, cols] = value
                    return fold(total, value * value)

                squares = strips(body, low * COLS, high * COLS, squares)
                load(two_in, two, load_sem.at[2 + int(top)], route, low, top, high - low)
        return squares

    everyone = [(row, data_index(*chip, side)) for row, chip in (
        (flip(model_pos), chips[3]), (flip(model_pos), chips[2]), (flip(model_pos), chips[1]), (model_pos, chips[3]),
        (flip(model_pos), chips[0]), (model_pos, chips[2]), (model_pos, chips[1]),
    ) for side in (core, flip(core))] + [(model_pos, partner)]

    def share_all(box, send_sem, recv_sem):
        for device in everyone:
            pltpu.make_async_remote_copy(src_ref=box.at[mine], dst_ref=box.at[mine], send_sem=send_sem, recv_sem=recv_sem, device_id=device, device_id_type=MESH).start()

    total_box[mine] = jnp.sum(finish(), axis=0, keepdims=True)
    pl.semaphore_wait(known, 1)
    share_all(total_box, box_sem.at[0], box_sem.at[1])
    drain(total_box.at[pl.ds(0, 15)], box_sem.at[1])
    total = jnp.sum(jnp.sum(total_box[...], axis=0), keepdims=True)
    clip = jnp.minimum(1.0, MAX_NORM / jnp.sqrt(total))
    one_scale, two_scale = clip * (1.0 - BETA_ONE), clip * (1.0 - BETA_TWO) ** 0.5

    def update(route, low, high, carry):
        def body(cols, total):
            place = (route, slice(None), cols)
            weight = master[place]
            value = mean[place]
            new_one = BETA_ONE * one[place] + one_scale * value
            change = two_scale * value
            new_two = BETA_TWO * two[place] + change * change
            one[place] = new_one
            two[place] = new_two
            floor = jnp.maximum(new_two, TINY)
            root = floor * lax.rsqrt(floor)
            direction = (new_one * (CORR_TWO ** 0.5 / CORR_ONE)) / (root + EPSILON * CORR_TWO ** 0.5) + WEIGHT_DECAY * weight
            mean[place] = direction
            return fold(total, direction * direction)

        return strips(body, low * COLS, high * COLS, carry, UPDATE_STRIP)

    def update_rows(index, low, high):
        drain(two.at[:, :, pl.ds(low * COLS, (high - low) * COLS)], load_sem.at[2 + index])
        return update(1, low, high, update(0, low, high, zero))

    def share_norms(index, box, rows):
        for position, value in enumerate(rows):
            box[mine, position:position + 1] = value
        share_all(box, box_sem.at[2 + index], box_sem.at[4 + index])

    def norm_rows(index, box):
        drain(box.at[pl.ds(0, 15)], box_sem.at[4 + index])
        return jnp.sqrt(jnp.sum(jnp.sum(box[...], axis=0), axis=1, keepdims=True))

    def bot_rate():
        norms = norm_rows(0, bot_box)
        return LEARN_RATE * (norms[0:1] / norms[1:2]) + jnp.zeros((8, 1), F32)

    def top_rate():
        norms = norm_rows(1, top_box)
        rates = [LEARN_RATE * (norms[position:position + 1] / norms[position + 3:position + 4]) for position in range(3)]
        row = lax.broadcasted_iota(jnp.int32, (8, 1), 0)
        return jnp.where(row < 3, rates[0], jnp.where(row == 3, rates[1], rates[2]))

    def tensor_rows(squares):
        row = lax.broadcasted_iota(jnp.int32, (8, 128), 0)
        return [jnp.sum(jnp.where(mask, squares, 0.0), axis=0, keepdims=True) for mask in (row < 3, row == 3, row > 3)]

    drain(one, load_sem.at[1])
    share_norms(0, bot_box, [jnp.sum(squares, axis=0, keepdims=True) for squares in (bot_squares, update_rows(0, N_TOP, N_CHUNK))])
    share_norms(1, top_box, tensor_rows(top_squares) + tensor_rows(update_rows(1, 0, N_TOP)))

    def piece(place, route, chunk, top, count=1):
        if top:
            start = place * SHARD + route * TOP_ROUTE + chunk * COLS
        else:
            start = place * (SHARD // 2) + route * BOT_ROUTE + (chunk - N_TOP) * COLS
        return (top_out if top else bot_out).at[:, pl.ds(pl.multiple_of(start, COLS), count * COLS)]

    def part(place, top, share=1):
        size = SHARD if top else SHARD // 2
        return (top_out if top else bot_out).at[:, pl.ds(pl.multiple_of(place * size, size), size // share)]

    def weights(route, chunk, rate, top):
        view = piece(places[0], route, chunk, top)
        masters, directions = slot(master, route, chunk), slot(mean, route, chunk)

        def body(cols, carry):
            value = masters[:, cols] - rate * directions[:, cols]
            masters[:, cols] = value
            view[:, cols] = value.astype(BF16)
            return carry

        strips(body, 0, COLS)

    def send(route, chunk, index, top):
        view = piece(places[0], route, chunk, top)
        kind = int(top)
        for axis in range(2):
            copy_to(view, view, places[1 + axis], side_send.at[axis, kind], near_recv.at[axis, route, index])
        copy_to(view, view, partner, partner_send.at[0, kind], partner_recv.at[0, kind])

    def own(chunk, rate, index, low, high, top):
        weights(0, chunk, rate, top)

        @pl.when(chunk > low)
        def _():
            send(1, chunk - 1, index, top)

        weights(1, chunk, rate, top)
        send(0, chunk, index, top)

        @pl.when(chunk == high - 1)
        def _():
            send(1, chunk, index, top)

        return rate

    for index, (low, high, top) in enumerate(GATHER_GROUPS):
        if index == 0:
            rate = bot_rate()
        elif top and not GATHER_GROUPS[index - 1][2]:
            rate = top_rate()
        lax.fori_loop(low, high, functools.partial(own, index=index, low=low, high=high, top=top), rate)

    for index, (low, high, top) in enumerate(GATHER_GROUPS):
        kind = int(top)
        for axis in range(2):
            for route in range(2):
                view = piece(places[1 + axis], route, low, top, high - low)
                drain(view, near_recv.at[axis, route, index])
                if axis == route:
                    copy_to(view, view, places[2 - route], forward_send.at[route, kind], corner_recv.at[route, index])
                copy_to(view, view, partner, partner_send.at[1 + axis, kind], partner_recv.at[1 + axis, kind])

    for index, (low, high, top) in enumerate(GATHER_GROUPS):
        for route in range(2):
            view = piece(places[3], route, low, top, high - low)
            drain(view, corner_recv.at[route, index])
            copy_to(view, view, partner, partner_send.at[3, int(top)], partner_recv.at[3, int(top)])

    for top in (True, False):
        kind = int(top)
        for axis in range(2):
            drain(part(places[0], top), side_send.at[axis, kind])
            drain(part(places[0], top, 2), forward_send.at[axis, kind])
        for chip, (row_pos, col_pos) in enumerate(chips):
            drain(part(places[chip], top), partner_send.at[chip, kind])
            drain(part(data_index(row_pos, col_pos, flip(core)), top), partner_recv.at[chip, kind])
    drain(total_box.at[pl.ds(0, 15)], box_sem.at[0])
    drain(bot_box.at[pl.ds(0, 15)], box_sem.at[2])
    drain(top_box.at[pl.ds(0, 15)], box_sem.at[3])

    drain(top_out.at[:, pl.ds(0, 6 * SHARD)], first_send.at[1])
    drain(bot_out.at[:, pl.ds(0, 3 * SHARD)], first_send.at[0])
    drain(sent, second_send)


def in_hbm(array):
    return pltpu.with_memory_space_constraint(array, pltpu.HBM)


def run_step(local_grads, master, moment_one, moment_two):
    dma = pltpu.SemaphoreType.DMA
    block = pltpu.VMEM((2, 8, N_CHUNK * COLS), F32)
    return pl.pallas_call(
        step_kernel,
        out_shape=(pltpu.VMEM((8, 8 * SHARD), BF16), pltpu.VMEM((8, 4 * SHARD), BF16), block, block, block),
        in_specs=[pl.BlockSpec(memory_space=pltpu.HBM)] * 4,
        out_specs=(pl.BlockSpec(memory_space=pltpu.VMEM),) * 5,
        scratch_shapes=[
            block, block,
            pltpu.VMEM((16, 1, 128), F32),
            pltpu.VMEM((16, 2, 128), F32),
            pltpu.VMEM((16, 6, 128), F32),
            dma((2, 2, len(GATHER_GROUPS))), dma((2, len(GATHER_GROUPS))), dma((2,)), dma, dma((4,)), dma((2, 2)), dma((2, 2)), dma((4, 2)), dma((4, 2)), dma((6,)),
            pltpu.SemaphoreType.REGULAR, pltpu.SemaphoreType.REGULAR,
        ],
        compiler_params=pltpu.CompilerParams(collective_id=0, has_side_effects=True, vmem_limit_bytes=STEP_LIMIT),
        name='lamb_step',
    )(in_hbm(local_grads), in_hbm(master), in_hbm(moment_one), in_hbm(moment_two))


def write_kernel(top, bot, master, one, two, params_out, master_out, one_out, two_out, sem):
    copies = []
    for place in range(8):
        copies.append((top.at[:, pl.ds(place * SHARD, SHARD)], params_out.at[pl.ds(0, 8), pl.ds(place * SHARD, SHARD)]))
        for half in range(2):
            copies.append((bot.at[pl.ds(4 * half, 4), pl.ds(place * TOP_ROUTE, TOP_ROUTE)], params_out.at[pl.ds(8, 4), pl.ds(place * SHARD + half * TOP_ROUTE, TOP_ROUTE)]))
    for block, array in ((master, master_out), (one, one_out), (two, two_out)):
        for route in range(2):
            for first, count, top in ((0, N_TOP, True), (N_TOP, N_BOT, False)):
                copies += [(src, dst) for dst, src in row_views(array, 0, route, first, slot(block, route, first, count), top, count)]
    for src, dst in copies:
        pltpu.make_async_copy(src, dst, sem).start()
    for src, dst in copies:
        pltpu.make_async_copy(src, dst, sem).wait()


def write_out(*blocks):
    state = jax.ShapeDtypeStruct((12, SHARD), F32)
    return pl.pallas_call(
        write_kernel,
        out_shape=(jax.ShapeDtypeStruct((12, 8 * SHARD), BF16), state, state, state),
        in_specs=[pl.BlockSpec(memory_space=pltpu.VMEM)] * 5,
        out_specs=(pl.BlockSpec(memory_space=pltpu.HBM),) * 4,
        scratch_shapes=[pltpu.SemaphoreType.DMA],
        compiler_params=pltpu.CompilerParams(vmem_limit_bytes=WRITE_LIMIT),
        name='write_out',
    )(*[pltpu.with_memory_space_constraint(block, pltpu.VMEM) for block in blocks])


def solution(mesh):
    state_spec = P(None, ('model', 'data'))

    def device_step(local_grads, master, moment_one, moment_two):
        return write_out(*run_step(local_grads, master, moment_one, moment_two))

    return jax.shard_map(device_step, mesh=mesh, in_specs=(P('data', None, 'model'), state_spec, state_spec, state_spec), out_specs=(P(None, 'model'), state_spec, state_spec, state_spec), check_vma=False)
```

```python
import functools

import jax
import jax.numpy as jnp
from jax import lax
from jax.experimental import pallas as pl
from jax.experimental.pallas import tpu as pltpu
from jax.sharding import PartitionSpec as P

STEP = 4
LEARN_RATE = 0.08
BETA_ONE = 0.9
BETA_TWO = 0.999
EPSILON = 1e-6
WEIGHT_DECAY = 0.01
MAX_NORM = 1.0
CORR_ONE = 1.0 - BETA_ONE ** STEP
CORR_TWO = 1.0 - BETA_TWO ** STEP

MESH = pl.DeviceIdType.MESH
F32 = jnp.float32
BF16 = jnp.bfloat16

SHARD = 147456
COLS = 3072
TOP_ROUTE = SHARD // 2
BOT_ROUTE = SHARD // 4
N_TOP = TOP_ROUTE // COLS
N_BOT = BOT_ROUTE // COLS
N_CHUNK = N_TOP + N_BOT
REDUCE_GROUPS = (
    (0, N_TOP // 2, True), (N_TOP // 2, N_TOP, True),
    (N_TOP, N_TOP + N_BOT // 2, False), (N_TOP + N_BOT // 2, N_CHUNK - 1, False), (N_CHUNK - 1, N_CHUNK, False),
)
GATHER_GROUPS = (
    (N_TOP, N_TOP + N_BOT // 2, False), (N_TOP + N_BOT // 2, N_CHUNK, False),
    (0, N_TOP // 2, True), (N_TOP // 2, N_TOP - 2, True), (N_TOP - 2, N_TOP - 1, True), (N_TOP - 1, N_TOP, True),
)
STRIP = 1024
UPDATE_STRIP = 3072

TINY = 1.2e-38
MIB = 1024 * 1024
STEP_LIMIT = 15 * MIB
WRITE_LIMIT = STEP_LIMIT


def flip(value):
    return 1 - value


def my_place():
    data_pos = lax.axis_index('data')
    return data_pos // 4, lax.rem(data_pos // 2, 2), lax.rem(data_pos, 2)


def data_index(pos_y, pos_x, core):
    return (pos_y * 2 + pos_x) * 2 + core


def drain(ref, sem):
    pltpu.make_async_copy(ref, ref, sem).wait()


def row_views(array, shard, route, chunk, block, top):
    if top:
        start = shard * SHARD + route * TOP_ROUTE + chunk * COLS
        return [(array.at[pl.ds(0, 8), pl.ds(pl.multiple_of(start, COLS), COLS)], block)]
    views = []
    for half in range(2):
        start = shard * SHARD + half * TOP_ROUTE + route * BOT_ROUTE + (chunk - N_TOP) * COLS
        views.append((array.at[pl.ds(8, 4), pl.ds(pl.multiple_of(start, COLS), COLS)], block.at[pl.ds(4 * half, 4)]))
    return views


def sweep(body, carry=0):
    for index, (low, high, top) in enumerate(REDUCE_GROUPS):
        carry = lax.fori_loop(low, high, functools.partial(body, index=index, top=top), carry)
    return carry


def strips(body, carry=0, width=STRIP):
    def step(strip, carry):
        return body(pl.ds(pl.multiple_of(strip * width, width), width), carry)

    return lax.fori_loop(0, COLS // width, step, carry)


def fold(total, values):
    for tile in range(values.shape[1] // 128):
        total = total + values[:, tile * 128:(tile + 1) * 128]
    return total


def step_kernel(
    grads, master_in, one_in, two_in,
    top_out, bot_out, master, one, two,
    mean, sent, total_box, bot_box, top_box,
    near_recv, corner_recv, first_send, second_send, load_sem, side_send, forward_send, partner_send, partner_recv, box_sem, seen, known,
):
    pos_y, pos_x, core = my_place()
    model_pos = lax.axis_index('model')
    mine = model_pos * 8 + lax.axis_index('data')
    grad = grads.at[0]
    got = two
    first_recv, second_recv = near_recv.at[0], near_recv.at[1]
    chips = ((pos_y, pos_x), (pos_y, flip(pos_x)), (flip(pos_y), pos_x), (flip(pos_y), flip(pos_x)))
    places = [data_index(row, col, core) for row, col in chips]
    partner = data_index(pos_y, pos_x, flip(core))

    def copy_to(src, dst, place, send_sem, recv_sem):
        pltpu.make_async_remote_copy(src_ref=src, dst_ref=dst, send_sem=send_sem, recv_sem=recv_sem, device_id=(model_pos, place), device_id_type=MESH).start()

    def landing(route, chunk, block, count, top):
        if top:
            start = ((route * N_TOP + chunk) * 8 + block) * COLS
        else:
            start = ((route * N_BOT + chunk - N_TOP) * 8 + block) * COLS
        return (top_out if top else bot_out).at[:, pl.ds(pl.multiple_of(start, COLS), count * COLS)]

    def wanted(route, row, col, far):
        return (lax.rem(row + far, 2), col) if route == 0 else (row, lax.rem(col + far, 2))

    def local(chunk, carry, index, top):
        for route in range(2):
            for far in range(2):
                shard = data_index(*wanted(route, pos_y, pos_x, far), core)
                for src, dst in row_views(grad, shard, route, chunk, landing(route, chunk, far, 1, top), top):
                    pltpu.make_async_copy(src, dst, first_recv.at[route, index]).start()
        return carry

    def remote(chunk, carry, index, top):
        for far in range(2):
            for other in range(2):
                for route in range(2):
                    row, col = chips[1 + route]
                    to_core = lax.rem(core + other, 2)
                    shard = data_index(*wanted(route, row, col, far), to_core)
                    for src, dst in row_views(grad, shard, route, chunk, landing(route, chunk, 4 + 2 * other + far, 1, top), top):
                        copy_to(src, dst, data_index(row, col, to_core), first_send.at[int(top)], first_recv.at[route, index])
            for route in range(2):
                shard = data_index(*wanted(route, pos_y, pos_x, far), flip(core))
                for src, dst in row_views(grad, shard, route, chunk, landing(route, chunk, 2 + far, 1, top), top):
                    copy_to(src, dst, partner, first_send.at[int(top)], first_recv.at[route, index])
        return carry

    def load(array, block, sem, route, chunk, top):
        for src, dst in row_views(array, 0, route, chunk, block.at[route, chunk], top):
            pltpu.make_async_copy(src, dst, sem).start()

    next_to = [(model_pos, place) for chip in (1, 2) for place in (places[chip], data_index(*chips[chip], flip(core)))] + [(model_pos, partner), (flip(model_pos), places[0])]

    def tell(sem, devices):
        for device in devices:
            pl.semaphore_signal(sem, inc=1, device_id=device, device_id_type=MESH)

    barrier = pltpu.get_barrier_semaphore()
    tell(barrier, next_to)
    sweep(local)
    pl.semaphore_wait(barrier, len(next_to))
    sweep(remote)
    tell(seen, next_to)

    def load_state(chunk, carry, index, top):
        for route in range(2):
            load(master_in, master, load_sem.at[0], route, chunk, top)
            load(one_in, one, load_sem.at[1], route, chunk, top)
        return carry

    sweep(load_state)
    pl.semaphore_wait(seen, len(next_to))
    tell(known, next_to[-1:])

    def second(route, chunk, index):
        copy_to(sent.at[route, chunk], got.at[route, chunk], places[2 - route], second_send, second_recv.at[route, index])

    def add_four(chunk, squares, top):
        for route in range(2):
            def body(cols, total):
                for far, target in ((0, mean), (1, sent)):
                    parts = [landing(route, chunk, 2 * source + far, 1, top)[:, cols].astype(F32) for source in range(4)]
                    target[route, chunk, :, cols] = (parts[0] + parts[1]) + (parts[2] + parts[3])
                weight = master[route, chunk, :, cols]
                return fold(total, weight * weight)

            squares = strips(body, squares)
        return squares

    drain(master, load_sem.at[0])
    zero = jnp.zeros((8, 128), F32)
    top_squares = bot_squares = zero
    for index, (low, high, top) in enumerate(REDUCE_GROUPS):
        for route in range(2):
            drain(landing(route, low, 0, 8 * (high - low), top), first_recv.at[route, index])
        squares = lax.fori_loop(low, high, functools.partial(add_four, top=top), top_squares if top else bot_squares)
        top_squares, bot_squares = (squares, bot_squares) if top else (top_squares, squares)

        @pl.loop(low, high)
        def _(chunk):
            second(0, chunk, index)
            second(1, chunk, index)

    def finish(chunk, squares, top):
        for route in range(2):
            def body(cols, total):
                value = (mean[route, chunk, :, cols] + got[route, chunk, :, cols]) * 0.125
                mean[route, chunk, :, cols] = value
                return fold(total, value * value)

            squares = strips(body, squares)
            load(two_in, two, load_sem.at[2 + int(top)], route, chunk, top)
        return squares

    def finish_all():
        squares = zero
        for index, (low, high, top) in enumerate(REDUCE_GROUPS):
            for route in range(2):
                drain(got.at[route, pl.ds(low, high - low)], second_recv.at[route, index])
            squares = lax.fori_loop(low, high, functools.partial(finish, top=top), squares)
        return squares

    everyone = [(row, data_index(*chip, side)) for row, chip in (
        (flip(model_pos), chips[3]), (flip(model_pos), chips[2]), (flip(model_pos), chips[1]), (model_pos, chips[3]),
        (flip(model_pos), chips[0]), (model_pos, chips[2]), (model_pos, chips[1]),
    ) for side in (core, flip(core))] + [(model_pos, partner)]

    def share_all(box, send_sem, recv_sem):
        for device in everyone:
            pltpu.make_async_remote_copy(src_ref=box.at[mine], dst_ref=box.at[mine], send_sem=send_sem, recv_sem=recv_sem, device_id=device, device_id_type=MESH).start()

    total_box[mine] = jnp.sum(finish_all(), axis=0, keepdims=True)
    pl.semaphore_wait(known, 1)
    share_all(total_box, box_sem.at[0], box_sem.at[1])

    drain(one, load_sem.at[1])
    drain(two.at[:, pl.ds(N_TOP, N_BOT)], load_sem.at[2])

    @pl.loop(N_TOP, N_CHUNK)
    def _(chunk):
        for route in range(2):
            for block, rate in ((one, BETA_ONE), (two, BETA_TWO)):
                block[route, chunk] = rate * block[route, chunk]

    drain(total_box.at[pl.ds(0, 15)], box_sem.at[1])
    total = jnp.sum(jnp.sum(total_box[...], axis=0), keepdims=True)
    clip = jnp.minimum(1.0, MAX_NORM / jnp.sqrt(total))
    one_scale, two_scale = clip * (1.0 - BETA_ONE), clip * (1.0 - BETA_TWO) ** 0.5

    def update(route, chunk, carry, decayed):
        def body(cols, total):
            place = (route, chunk, slice(None), cols)
            weight = master[place]
            value = mean[place]
            old_one, old_two = (one[place], two[place]) if decayed else (BETA_ONE * one[place], BETA_TWO * two[place])
            new_one = old_one + one_scale * value
            change = two_scale * value
            new_two = old_two + change * change
            one[place] = new_one
            two[place] = new_two
            floor = jnp.maximum(new_two, TINY)
            root = floor * lax.rsqrt(floor)
            direction = (new_one * (CORR_TWO ** 0.5 / CORR_ONE)) / (root + EPSILON * CORR_TWO ** 0.5) + WEIGHT_DECAY * weight
            mean[place] = direction
            return fold(total, direction * direction)

        return strips(body, carry, UPDATE_STRIP)

    def update_rows(index, low, high):
        return lax.fori_loop(low, high, lambda chunk, total: update(1, chunk, update(0, chunk, total, index == 0), index == 0), zero)

    def share_norms(index, box, rows):
        for position, value in enumerate(rows):
            box[mine, position:position + 1] = value
        share_all(box, box_sem.at[2 + index], box_sem.at[4 + index])

    def norm_rows(index, box):
        drain(box.at[pl.ds(0, 15)], box_sem.at[4 + index])
        return jnp.sqrt(jnp.sum(jnp.sum(box[...], axis=0), axis=1, keepdims=True))

    def bot_rate():
        norms = norm_rows(0, bot_box)
        return LEARN_RATE * (norms[0:1] / norms[1:2]) + jnp.zeros((8, 1), F32)

    def top_rate():
        norms = norm_rows(1, top_box)
        rates = [LEARN_RATE * (norms[position:position + 1] / norms[position + 3:position + 4]) for position in range(3)]
        row = lax.broadcasted_iota(jnp.int32, (8, 1), 0)
        return jnp.where(row < 3, rates[0], jnp.where(row == 3, rates[1], rates[2]))

    def tensor_rows(squares):
        row = lax.broadcasted_iota(jnp.int32, (8, 128), 0)
        return [jnp.sum(jnp.where(mask, squares, 0.0), axis=0, keepdims=True) for mask in (row < 3, row == 3, row > 3)]

    share_norms(0, bot_box, [jnp.sum(squares, axis=0, keepdims=True) for squares in (bot_squares, update_rows(0, N_TOP, N_CHUNK))])
    drain(two.at[:, pl.ds(0, N_TOP)], load_sem.at[3])
    share_norms(1, top_box, tensor_rows(top_squares) + tensor_rows(update_rows(1, 0, N_TOP)))

    def piece(place, route, chunk, top, count=1):
        if top:
            start = place * SHARD + route * TOP_ROUTE + chunk * COLS
        else:
            start = place * (SHARD // 2) + route * BOT_ROUTE + (chunk - N_TOP) * COLS
        return (top_out if top else bot_out).at[:, pl.ds(pl.multiple_of(start, COLS), count * COLS)]

    def part(place, top, share=1):
        size = SHARD if top else SHARD // 2
        return (top_out if top else bot_out).at[:, pl.ds(pl.multiple_of(place * size, size), size // share)]

    def weights(route, chunk, rate, top):
        view = piece(places[0], route, chunk, top)

        def body(cols, carry):
            place = (route, chunk, slice(None), cols)
            value = master[place] - rate * mean[place]
            master[place] = value
            view[:, cols] = value.astype(BF16)
            return carry

        strips(body)

    def send(route, chunk, index, top):
        view = piece(places[0], route, chunk, top)
        kind = int(top)
        for axis in range(2):
            copy_to(view, view, places[1 + axis], side_send.at[axis, kind], near_recv.at[axis, route, index])
        copy_to(view, view, partner, partner_send.at[0, kind], partner_recv.at[0, kind])

    def own(chunk, rate, index, low, high, top):
        weights(0, chunk, rate, top)

        @pl.when(chunk > low)
        def _():
            send(1, chunk - 1, index, top)

        weights(1, chunk, rate, top)
        send(0, chunk, index, top)

        @pl.when(chunk == high - 1)
        def _():
            send(1, chunk, index, top)

        return rate

    for index, (low, high, top) in enumerate(GATHER_GROUPS):
        if index == 0:
            rate = bot_rate()
        elif top and not GATHER_GROUPS[index - 1][2]:
            rate = top_rate()
        lax.fori_loop(low, high, functools.partial(own, index=index, low=low, high=high, top=top), rate)

    for index, (low, high, top) in enumerate(GATHER_GROUPS):
        kind = int(top)
        for axis in range(2):
            for route in range(2):
                view = piece(places[1 + axis], route, low, top, high - low)
                drain(view, near_recv.at[axis, route, index])
                if axis == route:
                    copy_to(view, view, places[2 - route], forward_send.at[route, kind], corner_recv.at[route, index])
                copy_to(view, view, partner, partner_send.at[1 + axis, kind], partner_recv.at[1 + axis, kind])

    for index, (low, high, top) in enumerate(GATHER_GROUPS):
        for route in range(2):
            view = piece(places[3], route, low, top, high - low)
            drain(view, corner_recv.at[route, index])
            copy_to(view, view, partner, partner_send.at[3, int(top)], partner_recv.at[3, int(top)])

    for top in (True, False):
        kind = int(top)
        for axis in range(2):
            drain(part(places[0], top), side_send.at[axis, kind])
            drain(part(places[0], top, 2), forward_send.at[axis, kind])
        for chip, (row_pos, col_pos) in enumerate(chips):
            drain(part(places[chip], top), partner_send.at[chip, kind])
            drain(part(data_index(row_pos, col_pos, flip(core)), top), partner_recv.at[chip, kind])
    drain(total_box.at[pl.ds(0, 15)], box_sem.at[0])
    drain(bot_box.at[pl.ds(0, 15)], box_sem.at[2])
    drain(top_box.at[pl.ds(0, 15)], box_sem.at[3])

    drain(top_out.at[:, pl.ds(0, 6 * SHARD)], first_send.at[1])
    drain(bot_out.at[:, pl.ds(0, 3 * SHARD)], first_send.at[0])
    drain(sent, second_send)


def in_hbm(array):
    return pltpu.with_memory_space_constraint(array, pltpu.HBM)


def run_step(local_grads, master, moment_one, moment_two):
    dma = pltpu.SemaphoreType.DMA
    block = pltpu.VMEM((2, N_CHUNK, 8, COLS), F32)
    return pl.pallas_call(
        step_kernel,
        out_shape=(pltpu.VMEM((8, 8 * SHARD), BF16), pltpu.VMEM((8, 4 * SHARD), BF16), block, block, block),
        in_specs=[pl.BlockSpec(memory_space=pltpu.HBM)] * 4,
        out_specs=(pl.BlockSpec(memory_space=pltpu.VMEM),) * 5,
        scratch_shapes=[
            block, block,
            pltpu.VMEM((16, 1, 128), F32),
            pltpu.VMEM((16, 2, 128), F32),
            pltpu.VMEM((16, 6, 128), F32),
            dma((2, 2, len(GATHER_GROUPS))), dma((2, len(GATHER_GROUPS))), dma((2,)), dma, dma((4,)), dma((2, 2)), dma((2, 2)), dma((4, 2)), dma((4, 2)), dma((6,)),
            pltpu.SemaphoreType.REGULAR, pltpu.SemaphoreType.REGULAR,
        ],
        compiler_params=pltpu.CompilerParams(collective_id=0, has_side_effects=True, vmem_limit_bytes=STEP_LIMIT),
        name='lamb_step',
    )(in_hbm(local_grads), in_hbm(master), in_hbm(moment_one), in_hbm(moment_two))


def write_kernel(top, bot, master, one, two, params_out, master_out, one_out, two_out, sem):
    copies = []
    for place in range(8):
        copies.append((top.at[:, pl.ds(place * SHARD, SHARD)], params_out.at[pl.ds(0, 8), pl.ds(place * SHARD, SHARD)]))
        for half in range(2):
            copies.append((bot.at[pl.ds(4 * half, 4), pl.ds(place * TOP_ROUTE, TOP_ROUTE)], params_out.at[pl.ds(8, 4), pl.ds(place * SHARD + half * TOP_ROUTE, TOP_ROUTE)]))
    for block, array in ((master, master_out), (one, one_out), (two, two_out)):
        for route in range(2):
            for chunk in range(N_CHUNK):
                copies += [(src, dst) for dst, src in row_views(array, 0, route, chunk, block.at[route, chunk], chunk < N_TOP)]
    for src, dst in copies:
        pltpu.make_async_copy(src, dst, sem).start()
    for src, dst in copies:
        pltpu.make_async_copy(src, dst, sem).wait()


def write_out(*blocks):
    state = jax.ShapeDtypeStruct((12, SHARD), F32)
    return pl.pallas_call(
        write_kernel,
        out_shape=(jax.ShapeDtypeStruct((12, 8 * SHARD), BF16), state, state, state),
        in_specs=[pl.BlockSpec(memory_space=pltpu.VMEM)] * 5,
        out_specs=(pl.BlockSpec(memory_space=pltpu.HBM),) * 4,
        scratch_shapes=[pltpu.SemaphoreType.DMA],
        compiler_params=pltpu.CompilerParams(vmem_limit_bytes=WRITE_LIMIT),
        name='write_out',
    )(*[pltpu.with_memory_space_constraint(block, pltpu.VMEM) for block in blocks])


def solution(mesh):
    state_spec = P(None, ('model', 'data'))

    def device_step(local_grads, master, moment_one, moment_two):
        return write_out(*run_step(local_grads, master, moment_one, moment_two))

    return jax.shard_map(device_step, mesh=mesh, in_specs=(P('data', None, 'model'), state_spec, state_spec, state_spec), out_specs=(P(None, 'model'), state_spec, state_spec, state_spec), check_vma=False)
```
